32 devices in a mesh: layer: 2 (over x), col: 4 (over z), row: 4 (over y, core).
Axes of the slice: x: 2, y: 2, z: 4, core: 2. Of those that a mesh axis runs over, the one named last changes fastest.
Arguments:
- weight: float32 [2048, 4096], P(('layer', 'row'), 'col'), parts along dimension 0
- grad_in: float32 [2048, 4096], P(('layer', 'row'), 'col'), parts along dimension 0
- mom_first: float32 [2048, 4096], P(('layer', 'row'), 'col'), parts along dimension 0
- mom_second: float32 [2048, 4096], P(('layer', 'row'), 'col'), parts along dimension 0
- stat_left: float32 [2048, 1024], P(('layer', 'row'), 'col'), parts along dimension 0
- stat_right: float32 [8192, 4096], P(('layer', 'row'), 'col'), parts along dimension 0
- basis_left: float32 [2048, 1024], P(('layer', 'row'), 'col'), parts along dimension 0
- basis_right: float32 [8192, 4096], P(('layer', 'row'), 'col'), parts along dimension 0
Outputs:
- output 1: float32 [2048, 4096], P(('layer', 'row'), 'col'), parts along dimension 0
- output 2: float32 [2048, 4096], P(('layer', 'row'), 'col'), parts along dimension 0
- output 3: float32 [2048, 4096], P(('layer', 'row'), 'col'), parts along dimension 0
- output 4: float32 [2048, 1024], P(('layer', 'row'), 'col'), parts along dimension 0
- output 5: float32 [8192, 4096], P(('layer', 'row'), 'col'), parts along dimension 0
There are 2 independent parts. The reference program is written for one: setup_inputs(seed, part) draws one part's arguments, and reference() takes and returns one part's arrays. A program takes and returns all parts, laid end to end along the dimension named above; each array names one.
All inputs are finite; a program needn't handle non-finite values.
Results may differ from the reference program's by a relative error of at most 0.001.
Values are sent between devices in bfloat16 or wider.
A program may use at most 1 GiB of HBM per device.

```python
import jax
import jax.numpy as jnp
from jax import lax

D = 1024
FF = 4096
STEP = 10
RANK = 16
FACTOR_SIDE = 16

BETA1 = 0.9
BETA2 = 0.9
EPS = 1e-8
LR = 0.1
BIAS_ONE = 1.0 - BETA1 ** STEP
BIAS_TWO = 1.0 - BETA2 ** STEP


def random_basis(base_key, matrix_order):
    sub_keys = jax.random.split(base_key, 5)
    side_b = matrix_order // FACTOR_SIDE
    outer_a = jnp.linalg.qr(jax.random.normal(sub_keys[0], (FACTOR_SIDE, FACTOR_SIDE), jnp.float32))[0]
    outer_b = jnp.linalg.qr(jax.random.normal(sub_keys[1], (side_b, side_b), jnp.float32))[0]
    inner_a = jnp.linalg.qr(jax.random.normal(sub_keys[2], (FACTOR_SIDE, FACTOR_SIDE), jnp.float32))[0]
    inner_b = jnp.linalg.qr(jax.random.normal(sub_keys[3], (side_b, side_b), jnp.float32))[0]
    col_order = jax.random.permutation(sub_keys[4], matrix_order)
    first_kron = jnp.kron(outer_a, outer_b)[:, col_order]
    blocks = first_kron.reshape(matrix_order, FACTOR_SIDE, side_b)
    mixed_basis = jnp.einsum("rst,sp,tq->rpq", blocks, inner_a, inner_b)
    return mixed_basis.reshape(matrix_order, matrix_order)


def setup_inputs(seed: int = 0, part: int = 0) -> dict:
    base_key = jax.random.fold_in(jax.random.key(seed), part)
    sub_keys = jax.random.split(base_key, 12)
    grad_scale = (10.0 / FF) ** 0.5
    noise_part = jax.random.normal(sub_keys[0], (D, FF), jnp.float32)
    left_fac = jax.random.normal(sub_keys[1], (D, RANK), jnp.float32)
    right_fac = jax.random.normal(sub_keys[2], (RANK, FF), jnp.float32)
    low_rank = jnp.dot(left_fac, right_fac) * (3.0 / RANK ** 0.5)
    grad_in = (noise_part + low_rank) * FF ** -0.5
    weight = 0.5 * jax.random.normal(sub_keys[3], (D, FF), jnp.float32)
    mom_first = 0.1 * grad_scale * jax.random.normal(sub_keys[4], (D, FF), jnp.float32)
    mom_second = 0.1 * grad_scale ** 2 * (0.25 + jax.random.normal(sub_keys[5], (D, FF), jnp.float32) ** 2)
    stat_fac_left = jax.random.normal(sub_keys[6], (D, RANK), jnp.float32)
    stat_left = 0.5 * ((9.0 / RANK) * jnp.dot(stat_fac_left, stat_fac_left.T) + jnp.eye(D, dtype=jnp.float32))
    stat_fac_right = jax.random.normal(sub_keys[7], (RANK, FF), jnp.float32)
    stat_right = 0.5 * (D / FF) * ((9.0 / RANK) * jnp.dot(stat_fac_right.T, stat_fac_right) + jnp.eye(FF, dtype=jnp.float32))
    basis_left = random_basis(sub_keys[8], D)
    basis_right = random_basis(sub_keys[9], FF)
    return {"weight": weight, "grad_in": grad_in, "mom_first": mom_first, "mom_second": mom_second, "stat_left": stat_left, "stat_right": stat_right, "basis_left": basis_left, "basis_right": basis_right}


def reference(weight, grad_in, mom_first, mom_second, stat_left, stat_right, basis_left, basis_right):
    highest = lax.Precision.HIGHEST
    new_left = BETA2 * stat_left + (1.0 - BETA2) * jnp.dot(grad_in, grad_in.T, precision=highest, preferred_element_type=jnp.float32)
    new_right = BETA2 * stat_right + (1.0 - BETA2) * jnp.dot(grad_in.T, grad_in, precision=highest, preferred_element_type=jnp.float32)
    left_bf = basis_left.astype(jnp.bfloat16)
    right_bf = basis_right.astype(jnp.bfloat16)
    inner_rot = jnp.dot(grad_in.astype(jnp.bfloat16), right_bf, preferred_element_type=jnp.float32).astype(jnp.bfloat16)
    rotated = jnp.dot(left_bf.T, inner_rot, preferred_element_type=jnp.float32)
    new_first = BETA1 * mom_first + (1.0 - BETA1) * rotated
    new_second = BETA2 * mom_second + (1.0 - BETA2) * rotated * rotated
    direction = (new_first / BIAS_ONE) / (jnp.sqrt(new_second / BIAS_TWO) + EPS)
    back_inner = jnp.dot(left_bf, direction.astype(jnp.bfloat16), preferred_element_type=jnp.float32).astype(jnp.bfloat16)
    step_update = jnp.dot(back_inner, right_bf.T, preferred_element_type=jnp.float32)
    new_weight = weight - LR * step_update
    return (new_weight, new_first, new_second, new_left, new_right)
```

```python
import jax
import jax.numpy as jnp
from jax import lax
from jax.experimental import pallas as pl
from jax.experimental.pallas import tpu as pltpu
from jax.sharding import PartitionSpec as P

BETA1 = 0.9
BETA2 = 0.9
EPS = 1e-8
LR = 0.1
STEP = 10
BIAS_ONE = 1.0 - BETA1 ** STEP
BIAS_TWO = 1.0 - BETA2 ** STEP

MESH = pl.DeviceIdType.MESH
F32 = jnp.float32
BF16 = jnp.bfloat16
NQ = 4
NH = 2
NU = 2
NDEV = 4
NSEND = 160

ROWS_T = (((0,), (0,)), ((), ()))
COLS_T = (((1,), (1,)), ((), ()))


def split3(x):
    a0 = x.astype(BF16)
    r = x - a0.astype(F32)
    a1 = r.astype(BF16)
    a2 = (r - a1.astype(F32)).astype(BF16)
    return a0, a1, a2


def kernel(
    w_hbm, g_hbm, m_hbm, v_hbm, l_hbm, r_hbm, ql_hbm, qr_hbm,
    w_out, m_out, v_out, l_out, r_out,
    grow, gbf, gi, gj, qrc, hcol, ncol, gis, gicat, gjcat, racc, ubuf, urecv,
    wbuf, mbuf, vbuf, qlr, qlc, hacc, kb, qlf, lbuf, lx, lrecv,
    ssem, lsem, r_gbf, r_qlr, r_g32, r_qr, r_qlc, r_h, r_n, r_gj, r_gi, r_u, r_l,
):
    lay = lax.axis_index("layer")
    z = lax.axis_index("col")
    i = lax.axis_index("row")
    y, c = i // 2, i % 2
    sib = 2 * y + (1 - c)
    opp = 2 * (1 - y) + c
    dia = 2 * (1 - y) + (1 - c)
    tr, tc = grow.shape[1], grow.shape[2]
    qrows = tc // NQ
    hcols = tc // NH
    urows = tr // NU

    waits = []
    count = [0]

    def dev(row, col):
        return (lay, col, row)

    def send(src, dst, rsem, row, col, cond=None):
        n = count[0]
        count[0] += 1

        def make():
            return pltpu.make_async_remote_copy(
                src_ref=src(), dst_ref=dst(), send_sem=ssem.at[n], recv_sem=rsem(),
                device_id=dev(row, col), device_id_type=MESH,
            )

        def go():
            make().start()

        def done():
            make().wait_send()

        if cond is None:
            go()
        else:
            pl.when(cond)(go)
        waits.append((cond, done))

    def arrived(dst, rsem, row, col):
        pltpu.make_async_remote_copy(
            src_ref=dst, dst_ref=dst, send_sem=ssem.at[0], recv_sem=rsem,
            device_id=dev(row, col), device_id_type=MESH,
        ).wait_recv()

    loads = {}

    def load(name, n, src, dst):
        cp = pltpu.make_async_copy(src, dst, lsem.at[n])
        cp.start()
        loads[name] = cp

    load("g", 0, g_hbm, grow.at[z])
    for q in range(NQ):
        rows = pl.ds(q * qrows, qrows)
        load(("qr", q), 1 + q, qr_hbm.at[rows], racc.at[rows])
    load("ql", 5, ql_hbm, qlf)
    load("m", 6, m_hbm, mbuf)
    load("v", 7, v_hbm, vbuf)
    load("w", 8, w_hbm, wbuf)
    load("l", 9, l_hbm, lbuf)

    barrier = pltpu.get_barrier_semaphore()
    for row in (sib, opp, dia):
        pl.semaphore_signal(barrier, inc=1, device_id=dev(row, z), device_id_type=MESH)

    @pl.when(z > 0)
    def _():
        pl.semaphore_signal(barrier, inc=1, device_id=dev(i, z - 1), device_id_type=MESH)

    @pl.when(z < NDEV - 1)
    def _():
        pl.semaphore_signal(barrier, inc=1, device_id=dev(i, z + 1), device_id_type=MESH)

    inner = jnp.logical_and(z > 0, z < NDEV - 1)

    @pl.when(inner)
    def _():
        pl.semaphore_wait(barrier, 5)

    @pl.when(jnp.logical_not(inner))
    def _():
        pl.semaphore_wait(barrier, 4)

    def line_own(buf, rs):
        send(lambda: buf.at[z], lambda: buf.at[z], lambda: rs.at[z], i, z + 1, z < NDEV - 1)
        send(lambda: buf.at[z], lambda: buf.at[z], lambda: rs.at[z], i, z - 1, z > 0)

    def line_forward(buf, rs, s):
        right = jnp.logical_and(z >= s, z < NDEV - 1)
        left = jnp.logical_and(z + s < NDEV, z > 0)

        @pl.when(right)
        def _():
            arrived(buf.at[z - s], rs.at[z - s], i, z - 1)

        send(lambda: buf.at[z - s], lambda: buf.at[z - s], lambda: rs.at[z - s], i, z + 1, right)

        @pl.when(left)
        def _():
            arrived(buf.at[z + s], rs.at[z + s], i, z + 1)

        send(lambda: buf.at[z + s], lambda: buf.at[z + s], lambda: rs.at[z + s], i, z - 1, left)

    def line_last(buf, rs, s):
        @pl.when(jnp.logical_and(z >= s, z == NDEV - 1))
        def _():
            arrived(buf.at[z - s], rs.at[z - s], i, z - 1)

        @pl.when(jnp.logical_and(z + s < NDEV, z == 0))
        def _():
            arrived(buf.at[z + s], rs.at[z + s], i, z + 1)

    loads["g"].wait()
    gbf[z] = grow[z].astype(BF16)
    loads["ql"].wait()
    qlr[z] = qlf[...].astype(BF16)

    def qr_own(q):
        rows = pl.ds(q * qrows, qrows)
        for row in (opp, sib):
            send(lambda: qrc.at[i, rows], lambda: qrc.at[i, rows], lambda: r_qr.at[i, q], row, z)

    line_own(gbf, r_gbf)
    for q in range(NQ):
        rows = pl.ds(q * qrows, qrows)
        loads[("qr", q)].wait()
        qrc[i, rows] = racc[rows].astype(BF16)
        if q == 1:
            line_own(qlr, r_qlr)
        if q >= 1:
            qr_own(q - 1)
    load("r", 10, r_hbm, racc)

    def qr_forward(q):
        rows = pl.ds(q * qrows, qrows)
        arrived(qrc.at[opp, rows], r_qr.at[opp, q], opp, z)
        send(lambda: qrc.at[opp, rows], lambda: qrc.at[opp, rows], lambda: r_qr.at[opp, q], sib, z)

    def h_add(k, q, first=False):
        rows = pl.ds(q * qrows, qrows)
        part = jnp.dot(gbf[k, :, rows], qrc[k, rows], preferred_element_type=F32)
        if first:
            hacc[...] = part
        else:
            hacc[...] += part

    qr_own(NQ - 1)

    line_forward(gbf, r_gbf, 1)
    line_forward(qlr, r_qlr, 1)
    qr_forward(0)
    line_forward(gbf, r_gbf, 2)
    line_forward(qlr, r_qlr, 2)
    line_own(grow, r_g32)
    qr_forward(1)
    for s in range(1, NDEV):
        line_last(gbf, r_gbf, s)
        line_last(qlr, r_qlr, s)

    for row in (opp, dia, sib):
        send(lambda row=row: qlr.at[row], lambda: qlc.at[i], lambda: r_qlc.at[i], row, z)
    qlc[i] = qlr[i]

    for q in range(NQ):
        h_add(i, q, first=q == 0)
    for q in range(NQ):
        rows = pl.ds(q * qrows, qrows)
        arrived(qrc.at[sib, rows], r_qr.at[sib, q], sib, z)
        h_add(sib, q)
    qr_forward(2)
    for q in range(2):
        h_add(opp, q)
    for q in range(2):
        rows = pl.ds(q * qrows, qrows)
        arrived(qrc.at[dia, rows], r_qr.at[dia, q], sib, z)
        h_add(dia, q)
    h_add(opp, 2)
    qr_forward(3)
    h_add(opp, 3)
    for q in range(2, NQ):
        rows = pl.ds(q * qrows, qrows)
        arrived(qrc.at[dia, rows], r_qr.at[dia, q], sib, z)
        h_add(dia, q)

    def own_part(buf, rs, n):
        cols = pl.ds(n * hcols, hcols)
        for row in (opp, sib):
            send(lambda: buf.at[i, :, cols], lambda: buf.at[i, :, cols], lambda: rs.at[i, n], row, z)

    def forward_part(buf, rs, n):
        cols = pl.ds(n * hcols, hcols)
        arrived(buf.at[opp, :, cols], rs.at[opp, n], opp, z)
        send(lambda: buf.at[opp, :, cols], lambda: buf.at[opp, :, cols], lambda: rs.at[opp, n], sib, z)

    def rest_part(buf, rs, n):
        cols = pl.ds(n * hcols, hcols)
        arrived(buf.at[sib, :, cols], rs.at[sib, n], sib, z)
        arrived(buf.at[dia, :, cols], rs.at[dia, n], sib, z)

    hcol[i] = hacc[...].astype(BF16)
    for n in range(NH):
        own_part(hcol, r_h, n)

    line_forward(grow, r_g32, 1)
    for row in (opp, dia, sib):
        arrived(qlc.at[row], r_qlc.at[row], row, z)
    loads["m"].wait()
    loads["v"].wait()

    for n in range(NH):
        cols = pl.ds(n * hcols, hcols)
        forward_part(hcol, r_h, n)
        rest_part(hcol, r_h, n)
        rotated = sum(
            lax.dot_general(qlc[k], hcol[k, :, cols], ROWS_T, preferred_element_type=F32) for k in range(NDEV)
        )
        hacc[:, cols] = rotated
        rotated = hacc[:, cols]
        new_first = BETA1 * mbuf[:, cols] + (1.0 - BETA1) * rotated
        new_second = BETA2 * vbuf[:, cols] + (1.0 - BETA2) * rotated * rotated
        mbuf[:, cols] = new_first
        vbuf[:, cols] = new_second
        direction = (new_first / BIAS_ONE) / (jnp.sqrt(new_second / BIAS_TWO) + EPS)
        ncol[i, :, cols] = direction.astype(BF16)
        own_part(ncol, r_n, n)
    stores = []

    def store(n, src, dst):
        cp = pltpu.make_async_copy(src, dst, lsem.at[n])
        cp.start()
        stores.append(cp)

    store(11, mbuf, m_out)
    store(12, vbuf, v_out)

    line_forward(grow, r_g32, 2)
    for row, slot in ((opp, 1), (sib, 0)):
        send(lambda: grow.at[z], lambda slot=slot: gj.at[slot], lambda slot=slot: r_gj.at[slot], row, z)

    def gi_send(b, valid):
        send(lambda: grow.at[b], lambda: gi.at[i], lambda: r_gi.at[i], b, z, jnp.logical_and(valid, b != i))

    gi_send(z, z >= 0)
    line_last(grow, r_g32, 1)
    gi_send(z - 1, z >= 1)
    gi_send(z + 1, z + 1 < NDEV)

    for n in range(NH):
        forward_part(ncol, r_n, n)
        rest_part(ncol, r_n, n)
        cols = pl.ds(n * hcols, hcols)
        kb[:, cols] = sum(
            jnp.dot(qlr[k], ncol[k, :, cols], preferred_element_type=F32) for k in range(NDEV)
        ).astype(BF16)

    def u_send(a, h, slot, col, cond):
        rows = pl.ds(h * urows, urows)
        send(lambda: ubuf.at[a, rows], lambda: urecv.at[slot, rows], lambda: r_u.at[slot, h], i, col, cond)

    for piece in (3, 0, 2, 1):
        ubuf[piece] = lax.dot_general(kb[...], qrc[piece], COLS_T, preferred_element_type=F32)
        for h in range(NU):
            if piece > 0:
                u_send(piece, h, piece, z + 1, z == 0)
            if piece < NDEV - 1:
                u_send(piece, h, NDEV if piece == NDEV - 2 else piece, z - 1, z == NDEV - 1)

    def u_at(a, h, station, to_right):
        rows = pl.ds(h * urows, urows)
        slot = NDEV if (not to_right and station == a) else a

        @pl.when(z == station)
        def _():
            arrived(urecv.at[slot, rows], r_u.at[slot, h], i, station - 1 if to_right else station + 1)
            ubuf[a, rows] += urecv[slot, rows]

        if station != a:
            nxt = station + 1 if to_right else station - 1
            nslot = NDEV if (not to_right and nxt == a) else a
            u_send(a, h, nslot, nxt, z == station)

    line_last(grow, r_g32, 2)
    gi_send(z - 2, z >= 2)
    gi_send(z + 2, z + 2 < NDEV)

    def u_round(t):
        for h in range(NU):
            for a in (3, 2, 1):
                st = t - (3 - a)
                if 1 <= st <= a:
                    u_at(a, h, st, True)
                    u_at(NDEV - 1 - a, h, NDEV - 1 - st, False)

    def to_row():
        gi[i] = grow[i]

    def gj_forward():
        arrived(gj.at[1], r_gj.at[1], opp, z)
        send(lambda: gj.at[1], lambda: gj.at[2], lambda: r_gj.at[2], sib, z)

    def split_gi(k):
        a0, a1, a2 = split3(gi[k])
        gis[k, 0] = a0
        gis[k, 1] = a1
        gis[k, 2] = a2

    mrows = tr

    def right_add(k, gj_ref, first=False):
        b0, b1, b2 = split3(gj_ref[...])
        for n, b in enumerate((b0, b1, b2, b0, b1, b0)):
            gjcat[pl.ds(n * tr, tr)] = b
        a = [gis[k, n].T for n in range(3)]
        for n, t in enumerate((0, 0, 0, 1, 1, 2)):
            gicat[:, pl.ds(n * tr, tr)] = a[t]

        def body(m, carry):
            rows = pl.ds(pl.multiple_of(m * mrows, mrows), mrows)
            part = jnp.dot(gicat[rows], gjcat[...], preferred_element_type=F32)
            old = racc[rows]
            racc[rows] = (BETA2 * old if first else old) + (1.0 - BETA2) * part
            return carry

        lax.fori_loop(0, tc // mrows, body, 0)

    u_round(1)
    line_last(grow, r_g32, 3)
    gi_send(z - 3, z >= 3)
    gi_send(z + 3, z + 3 < NDEV)
    to_row()
    gj_forward()
    loads["r"].wait()
    split_gi(i)
    right_add(i, grow.at[z], first=True)

    def gi_wait(row):
        arrived(gi.at[row], r_gi.at[row], row, z)
        split_gi(row)

    gi_wait(sib)
    arrived(gj.at[0], r_gj.at[0], sib, z)
    right_add(sib, gj.at[0])
    u_round(2)
    gi_wait(opp)
    right_add(opp, gj.at[1])
    gi_wait(dia)

    def left_part(k, n):
        pieces = [gis[k, t] for t in range(3)]
        other = [gis[z, t] for t in range(3)]
        total = None
        for t, u in ((0, 0), (0, 1), (1, 0), (1, 1), (0, 2), (2, 0)):
            d = lax.dot_general(pieces[t], other[u], COLS_T, preferred_element_type=F32)
            total = d if total is None else total + d
        lx[n] = total

    left_part(dia, 3)
    left_part(opp, 2)
    send(lambda: lx.at[3], lambda: lrecv.at[2], lambda: r_l.at[2], dia, z)
    send(lambda: lx.at[2], lambda: lrecv.at[1], lambda: r_l.at[1], opp, z)
    left_part(sib, 1)
    left_part(i, 0)
    send(lambda: lx.at[1], lambda: lrecv.at[0], lambda: r_l.at[0], sib, z)

    arrived(gj.at[2], r_gj.at[2], sib, z)
    right_add(dia, gj.at[2])
    store(13, racc, r_out)
    loads["w"].wait()
    u_round(3)
    wbuf[...] = wbuf[...] - LR * ubuf[z]
    store(14, wbuf, w_out)
    loads["l"].wait()
    arrived(lrecv.at[0], r_l.at[0], sib, z)
    arrived(lrecv.at[1], r_l.at[1], opp, z)
    arrived(lrecv.at[2], r_l.at[2], dia, z)
    left_sum = (lx[0] + lrecv[0]) + (lrecv[1] + lrecv[2])
    lbuf[...] = BETA2 * lbuf[...] + (1.0 - BETA2) * left_sum
    store(15, lbuf, l_out)

    for cond, done in waits:
        if cond is None:
            done()
        else:
            pl.when(cond)(done)
    for cp in stores:
        cp.wait()
    assert count[0] <= NSEND, count[0]


def solution(mesh):
    tile_spec = P(("layer", "row"), "col")

    def local_step(weight, grad_in, mom_first, mom_second, stat_left, stat_right, basis_left, basis_right):
        tr, tc = grad_in.shape
        tl = stat_left.shape[0]
        dma = pltpu.SemaphoreType.DMA
        scratch = [
            pltpu.VMEM((4, tr, tc), F32),
            pltpu.VMEM((4, tr, tc), BF16),
            pltpu.VMEM((4, tr, tc), F32),
            pltpu.VMEM((3, tr, tc), F32),
            pltpu.VMEM((4, tc, tc), BF16),
            pltpu.VMEM((4, tr, tc), BF16),
            pltpu.VMEM((4, tr, tc), BF16),
            pltpu.VMEM((4, 3, tr, tc), BF16),
            pltpu.VMEM((tc, 6 * tr), BF16),
            pltpu.VMEM((6 * tr, tc), BF16),
            pltpu.VMEM((tc, tc), F32),
            pltpu.VMEM((4, tr, tc), F32),
            pltpu.VMEM((5, tr, tc), F32),
            pltpu.VMEM((tr, tc), F32),
            pltpu.VMEM((tr, tc), F32),
            pltpu.VMEM((tr, tc), F32),
            pltpu.VMEM((4, tl, tl), BF16),
            pltpu.VMEM((4, tl, tl), BF16),
            pltpu.VMEM((tr, tc), F32),
            pltpu.VMEM((tr, tc), BF16),
            pltpu.VMEM((tl, tl), F32),
            pltpu.VMEM((tl, tl), F32),
            pltpu.VMEM((4, tl, tl), F32),
            pltpu.VMEM((3, tl, tl), F32),
            dma((NSEND,)),
            dma((16,)),
            dma((4,)), dma((4,)), dma((4,)),
            dma((4, NQ)), dma((4,)),
            dma((4, NH)), dma((4, NH)),
            dma((3,)), dma((4,)),
            dma((5, NU)), dma((3,)),
        ]
        any_spec = pl.BlockSpec(memory_space=pl.ANY)
        outs = [weight, mom_first, mom_second, stat_left, stat_right]
        return pl.pallas_call(
            kernel,
            name="soap_step",
            out_shape=[jax.ShapeDtypeStruct(o.shape, o.dtype) for o in outs],
            in_specs=[any_spec] * 8,
            out_specs=[any_spec] * 5,
            scratch_shapes=scratch,
            compiler_params=pltpu.CompilerParams(
                collective_id=0, has_side_effects=True, vmem_limit_bytes=67043328,
            ),
        )(weight, grad_in, mom_first, mom_second, stat_left, stat_right, basis_left, basis_right)

    return jax.shard_map(local_step, mesh=mesh, in_specs=(tile_spec,) * 8, out_specs=(tile_spec,) * 5, check_vma=False)
```

```python
import jax
import jax.numpy as jnp
from jax import lax
from jax.experimental import pallas as pl
from jax.experimental.pallas import tpu as pltpu
from jax.sharding import PartitionSpec as P

BETA1 = 0.9
BETA2 = 0.9
EPS = 1e-8
LR = 0.1
STEP = 10
BIAS_ONE = 1.0 - BETA1 ** STEP
BIAS_TWO = 1.0 - BETA2 ** STEP

MESH = pl.DeviceIdType.MESH
F32 = jnp.float32
BF16 = jnp.bfloat16
NQ = 4
NH = 2
NU = 2
NG = 2
NDEV = 4
NSEND = 160
VMEM_BYTES = 54 * 2**20

ROWS_T = (((0,), (0,)), ((), ()))
COLS_T = (((1,), (1,)), ((), ()))


def split3(x):
    a0 = x.astype(BF16)
    r = x - a0.astype(F32)
    a1 = r.astype(BF16)
    a2 = (r - a1.astype(F32)).astype(BF16)
    return a0, a1, a2


def kernel(
    w_hbm, g_hbm, m_hbm, v_hbm, l_hbm, r_hbm, ql_hbm, qr_hbm,
    wbuf, mbuf, vbuf, lbuf, racc,
    grow, gbf, gi, gj, qrc, hcol, ncol, gis, ubuf, urecv,
    qlr, qlc, hacc, kb, qlf, lx, lrecv,
    ssem, lsem, r_gbf, r_qlr, r_g32, r_qr, r_qlc, r_h, r_n, r_gj, r_gi, r_u, r_l,
):
    lay = lax.axis_index("layer")
    z = lax.axis_index("col")
    i = lax.axis_index("row")
    y, c = i // 2, i % 2
    sib = 2 * y + (1 - c)
    opp = 2 * (1 - y) + c
    dia = 2 * (1 - y) + (1 - c)
    tr, tc = grow.shape[1], grow.shape[2]
    qrows = tc // NQ
    hcols = tc // NH
    urows = tr // NU
    grows = tr // NG

    waits, qr_waits = [], []
    count = [0]

    def dev(row, col):
        return (lay, col, row)

    def send(src, dst, rsem, row, col, cond=None, held=None):
        n = count[0]
        count[0] += 1

        def make():
            return pltpu.make_async_remote_copy(
                src_ref=src(), dst_ref=dst(), send_sem=ssem.at[n], recv_sem=rsem(),
                device_id=dev(row, col), device_id_type=MESH,
            )

        def go():
            make().start()

        def done():
            make().wait_send()

        if cond is None:
            go()
        else:
            pl.when(cond)(go)
        if held is None:
            waits.append((cond, done))
        else:
            held.append(done)

    def settle():
        for cond, done in waits:
            if cond is None:
                done()
            else:
                pl.when(cond)(done)
        waits.clear()

    def arrived(dst, rsem, row, col):
        pltpu.make_async_remote_copy(
            src_ref=dst, dst_ref=dst, send_sem=ssem.at[0], recv_sem=rsem,
            device_id=dev(row, col), device_id_type=MESH,
        ).wait_recv()

    loads = {}

    def load(name, n, src, dst):
        cp = pltpu.make_async_copy(src, dst, lsem.at[n])
        cp.start()
        loads[name] = cp

    load("g", 0, g_hbm, grow.at[z])
    for q in range(NQ):
        rows = pl.ds(q * qrows, qrows)
        load(("qr", q), 1 + q, qr_hbm.at[rows], racc.at[rows])
    load("ql", 5, ql_hbm, qlf)
    load("m", 6, m_hbm, mbuf)
    load("v", 7, v_hbm, vbuf)
    load("w", 8, w_hbm, wbuf)
    load("l", 9, l_hbm, lbuf)

    barrier = pltpu.get_barrier_semaphore()
    for row in (sib, opp, dia):
        pl.semaphore_signal(barrier, inc=1, device_id=dev(row, z), device_id_type=MESH)

    @pl.when(z > 0)
    def _():
        pl.semaphore_signal(barrier, inc=1, device_id=dev(i, z - 1), device_id_type=MESH)

    @pl.when(z < NDEV - 1)
    def _():
        pl.semaphore_signal(barrier, inc=1, device_id=dev(i, z + 1), device_id_type=MESH)

    inner = jnp.logical_and(z > 0, z < NDEV - 1)

    @pl.when(inner)
    def _():
        pl.semaphore_wait(barrier, 5)

    @pl.when(jnp.logical_not(inner))
    def _():
        pl.semaphore_wait(barrier, 4)

    def line_own(buf, rs):
        send(lambda: buf.at[z], lambda: buf.at[z], lambda: rs.at[z], i, z + 1, z < NDEV - 1)
        send(lambda: buf.at[z], lambda: buf.at[z], lambda: rs.at[z], i, z - 1, z > 0)

    def line_forward(buf, rs, s):
        right = jnp.logical_and(z >= s, z < NDEV - 1)
        left = jnp.logical_and(z + s < NDEV, z > 0)

        @pl.when(right)
        def _():
            arrived(buf.at[z - s], rs.at[z - s], i, z - 1)

        send(lambda: buf.at[z - s], lambda: buf.at[z - s], lambda: rs.at[z - s], i, z + 1, right)

        @pl.when(left)
        def _():
            arrived(buf.at[z + s], rs.at[z + s], i, z + 1)

        send(lambda: buf.at[z + s], lambda: buf.at[z + s], lambda: rs.at[z + s], i, z - 1, left)

    def line_last(buf, rs, s):
        @pl.when(jnp.logical_and(z >= s, z == NDEV - 1))
        def _():
            arrived(buf.at[z - s], rs.at[z - s], i, z - 1)

        @pl.when(jnp.logical_and(z + s < NDEV, z == 0))
        def _():
            arrived(buf.at[z + s], rs.at[z + s], i, z + 1)

    loads["g"].wait()
    gbf[z] = grow[z].astype(BF16)
    loads["ql"].wait()
    qlr[z] = qlf[...].astype(BF16)

    def qr_own(q):
        rows = pl.ds(q * qrows, qrows)
        for row in (opp, sib):
            send(lambda: qrc.at[i, rows], lambda: qrc.at[i, rows], lambda: r_qr.at[i, q], row, z, held=qr_waits)

    line_own(gbf, r_gbf)
    for q in range(NQ):
        rows = pl.ds(q * qrows, qrows)
        loads[("qr", q)].wait()
        qrc[i, rows] = racc[rows].astype(BF16)
        if q == 1:
            line_own(qlr, r_qlr)
        if q >= 1:
            qr_own(q - 1)
    load("r", 10, r_hbm, racc)

    def qr_forward(q):
        rows = pl.ds(q * qrows, qrows)
        arrived(qrc.at[opp, rows], r_qr.at[opp, q], opp, z)
        send(lambda: qrc.at[opp, rows], lambda: qrc.at[opp, rows], lambda: r_qr.at[opp, q], sib, z, held=qr_waits)

    def h_add(k, q, first=False):
        rows = pl.ds(q * qrows, qrows)
        part = jnp.dot(gbf[k, :, rows], qrc[k, rows], preferred_element_type=F32)
        if first:
            hacc[...] = part
        else:
            hacc[...] += part

    qr_own(NQ - 1)

    line_forward(gbf, r_gbf, 1)
    line_forward(qlr, r_qlr, 1)
    qr_forward(0)
    line_forward(gbf, r_gbf, 2)
    line_forward(qlr, r_qlr, 2)
    line_own(grow, r_g32)
    qr_forward(1)
    for s in range(1, NDEV):
        line_last(gbf, r_gbf, s)
        line_last(qlr, r_qlr, s)

    for row in (opp, dia, sib):
        send(lambda row=row: qlr.at[row], lambda: qlc.at[i], lambda: r_qlc.at[i], row, z)
    qlc[i] = qlr[i]

    for q in range(NQ):
        h_add(i, q, first=q == 0)
    for q in range(NQ):
        rows = pl.ds(q * qrows, qrows)
        arrived(qrc.at[sib, rows], r_qr.at[sib, q], sib, z)
        h_add(sib, q)
    qr_forward(2)
    for q in range(2):
        h_add(opp, q)
    for q in range(2):
        rows = pl.ds(q * qrows, qrows)
        arrived(qrc.at[dia, rows], r_qr.at[dia, q], sib, z)
        h_add(dia, q)
    h_add(opp, 2)
    qr_forward(3)
    h_add(opp, 3)
    for q in range(2, NQ):
        rows = pl.ds(q * qrows, qrows)
        arrived(qrc.at[dia, rows], r_qr.at[dia, q], sib, z)
        h_add(dia, q)

    def own_part(buf, rs, n):
        cols = pl.ds(n * hcols, hcols)
        for row in (opp, sib):
            send(lambda: buf.at[i, :, cols], lambda: buf.at[i, :, cols], lambda: rs.at[i, n], row, z)

    def forward_part(buf, rs, n):
        cols = pl.ds(n * hcols, hcols)
        arrived(buf.at[opp, :, cols], rs.at[opp, n], opp, z)
        send(lambda: buf.at[opp, :, cols], lambda: buf.at[opp, :, cols], lambda: rs.at[opp, n], sib, z)

    def rest_part(buf, rs, n):
        cols = pl.ds(n * hcols, hcols)
        arrived(buf.at[sib, :, cols], rs.at[sib, n], sib, z)
        arrived(buf.at[dia, :, cols], rs.at[dia, n], sib, z)

    hcol[i] = hacc[...].astype(BF16)
    for n in range(NH):
        own_part(hcol, r_h, n)

    line_forward(grow, r_g32, 1)
    for row in (opp, dia, sib):
        arrived(qlc.at[row], r_qlc.at[row], row, z)
    loads["m"].wait()
    loads["v"].wait()

    for n in range(NH):
        cols = pl.ds(n * hcols, hcols)
        forward_part(hcol, r_h, n)
        rest_part(hcol, r_h, n)
        rotated = sum(
            lax.dot_general(qlc[k], hcol[k, :, cols], ROWS_T, preferred_element_type=F32) for k in range(NDEV)
        )
        hacc[:, cols] = rotated
        rotated = hacc[:, cols]
        new_first = BETA1 * mbuf[:, cols] + (1.0 - BETA1) * rotated
        new_second = BETA2 * vbuf[:, cols] + (1.0 - BETA2) * rotated * rotated
        mbuf[:, cols] = new_first
        vbuf[:, cols] = new_second
        direction = (new_first / BIAS_ONE) / (jnp.sqrt(new_second / BIAS_TWO) + EPS)
        ncol[i, :, cols] = direction.astype(BF16)
        own_part(ncol, r_n, n)
    for row, slot in ((opp, 1), (sib, 0)):
        send(lambda: grow.at[z], lambda slot=slot: gj.at[slot], lambda slot=slot: r_gj.at[slot], row, z)

    def gi_send(b, valid):
        for n in range(NG):
            rows = pl.ds(n * grows, grows)
            send(lambda: grow.at[b, rows], lambda: gi.at[i, rows], lambda: r_gi.at[i, n], b, z, jnp.logical_and(valid, b != i))

    gi_send(z, z >= 0)
    line_last(grow, r_g32, 1)
    gi_send(z - 1, z >= 1)
    gi_send(z + 1, z + 1 < NDEV)

    for n in range(NH):
        forward_part(ncol, r_n, n)
        rest_part(ncol, r_n, n)
        cols = pl.ds(n * hcols, hcols)
        kb[:, cols] = sum(
            jnp.dot(qlr[k], ncol[k, :, cols], preferred_element_type=F32) for k in range(NDEV)
        ).astype(BF16)

    def u_send(a, h, slot, col, cond):
        rows = pl.ds(h * urows, urows)
        send(lambda: ubuf.at[a, rows], lambda: urecv.at[slot, rows], lambda: r_u.at[slot, h], i, col, cond)

    def u_first(a, to_right):
        for h in range(NU):
            if to_right:
                u_send(a, h, a, z + 1, z == 0)
            else:
                u_send(a, h, NDEV if a == NDEV - 2 else a, z - 1, z == NDEV - 1)

    for piece, starts in ((3, ((3, True),)), (0, ((0, False),)), (2, ((2, True),)), (1, ((1, False), (1, True), (2, False)))):
        ubuf[piece] = lax.dot_general(kb[...], qrc[piece], COLS_T, preferred_element_type=F32)
        for a, to_right in starts:
            u_first(a, to_right)
    line_forward(grow, r_g32, 2)

    def u_at(a, h, station, to_right):
        rows = pl.ds(h * urows, urows)
        slot = NDEV if (not to_right and station == a) else a

        @pl.when(z == station)
        def _():
            arrived(urecv.at[slot, rows], r_u.at[slot, h], i, station - 1 if to_right else station + 1)
            ubuf[a, rows] += urecv[slot, rows]

        if station != a:
            nxt = station + 1 if to_right else station - 1
            nslot = NDEV if (not to_right and nxt == a) else a
            u_send(a, h, nslot, nxt, z == station)

    line_last(grow, r_g32, 2)
    gi_send(z - 2, z >= 2)
    gi_send(z + 2, z + 2 < NDEV)

    def u_round(t):
        for h in range(NU):
            for a in (3, 2, 1):
                st = t - (3 - a)
                if 1 <= st <= a:
                    u_at(a, h, st, True)
                    u_at(NDEV - 1 - a, h, NDEV - 1 - st, False)

    def gj_split(slot, ref):
        for t, term in enumerate(split3(ref[...])):
            qrc[slot, pl.ds(t * tr, tr)] = term

    def gi_split(k, ref, n):
        rows = pl.ds(n * grows, grows)
        for t, term in enumerate(split3(ref[rows])):
            gis[k, t, rows] = term

    def right_add(k, slot, n, first=False):
        def body(m, carry):
            rows = pl.ds(pl.multiple_of(m * tr, tr), tr)
            part = pl.ds(n * grows, grows)
            a0, a1, a2 = [gis[k, t, part, rows].T for t in range(3)]
            b0, b1, b2 = [qrc[slot, pl.ds(t * tr + n * grows, grows)] for t in range(3)]
            left = jnp.concatenate([a0, a0, a0, a1, a1, a2], axis=1)
            right = jnp.concatenate([b0, b1, b2, b0, b1, b0], axis=0)
            share = (1.0 - BETA2) * jnp.dot(left, right, preferred_element_type=F32)
            old = racc[rows]
            racc[rows] = (BETA2 * old if first else old) + share
            return carry

        lax.fori_loop(0, tc // tr, body, 0)

    def gi_arrived(row, n):
        rows = pl.ds(n * grows, grows)
        arrived(gi.at[row, rows], r_gi.at[row, n], row, z)
        gi_split(row, gi.at[row], n)

    def left_part(k, slot):
        pieces = [gis[k, t] for t in range(3)]
        other = [gis[z, t] for t in range(3)]
        total = None
        for t, u in ((0, 0), (0, 1), (1, 0), (1, 1), (0, 2), (2, 0)):
            d = lax.dot_general(pieces[t], other[u], COLS_T, preferred_element_type=F32)
            total = d if total is None else total + d
        lx[slot] = total

    for done in qr_waits:
        done()
    gj_split(0, grow.at[z])
    arrived(gj.at[0], r_gj.at[0], sib, z)
    gj_split(1, gj.at[0])
    arrived(gj.at[1], r_gj.at[1], opp, z)
    send(lambda: gj.at[1], lambda: gj.at[2], lambda: r_gj.at[2], sib, z)
    gj_split(2, gj.at[1])
    u_round(1)
    line_last(grow, r_g32, 3)
    gi_send(z - 3, z >= 3)
    gi_send(z + 3, z + 3 < NDEV)
    arrived(gj.at[2], r_gj.at[2], sib, z)
    gj_split(3, gj.at[2])
    loads["r"].wait()
    for n in range(NG):
        gi_split(i, grow.at[i], n)
        right_add(i, 0, n, first=n == 0)
    u_round(2)
    for n in range(NG):
        gi_arrived(sib, n)
        right_add(sib, 1, n)
    for n in range(NG - 1):
        gi_arrived(opp, n)
        right_add(opp, 2, n)
        gi_arrived(dia, n)
        right_add(dia, 3, n)
    loads["w"].wait()
    loads["l"].wait()
    gi_arrived(dia, NG - 1)
    gi_arrived(opp, NG - 1)

    left_part(dia, 3)
    send(lambda: lx.at[3], lambda: lrecv.at[2], lambda: r_l.at[2], sib, z)
    left_part(opp, 2)
    left_part(sib, 1)
    send(lambda: lx.at[1], lambda: lrecv.at[0], lambda: r_l.at[0], sib, z)
    arrived(lrecv.at[2], r_l.at[2], sib, z)
    lx[2] += lrecv[2]
    left_part(i, 0)
    send(lambda: lx.at[2], lambda: lrecv.at[1], lambda: r_l.at[1], opp, z)
    right_add(opp, 2, NG - 1)
    right_add(dia, 3, NG - 1)

    u_round(3)
    wbuf[...] = wbuf[...] - LR * ubuf[z]
    arrived(lrecv.at[0], r_l.at[0], sib, z)
    left_sum = lx[0] + lrecv[0]
    arrived(lrecv.at[1], r_l.at[1], opp, z)
    left_sum += lrecv[1]
    lbuf[...] = BETA2 * lbuf[...] + (1.0 - BETA2) * left_sum

    settle()
    assert count[0] <= NSEND, count[0]


def write_out(*refs):
    ins, outs, sem = refs[:5], refs[5:10], refs[10]
    copies = [pltpu.make_async_copy(a, b, sem.at[n]) for n, (a, b) in enumerate(zip(ins, outs))]
    for cp in copies:
        cp.start()
    for cp in copies:
        cp.wait()


def solution(mesh):
    tile_spec = P(("layer", "row"), "col")

    def local_step(weight, grad_in, mom_first, mom_second, stat_left, stat_right, basis_left, basis_right):
        tr, tc = grad_in.shape
        tl = stat_left.shape[0]
        dma = pltpu.SemaphoreType.DMA
        scratch = [
            pltpu.VMEM((4, tr, tc), F32),
            pltpu.VMEM((4, tr, tc), BF16),
            pltpu.VMEM((4, tr, tc), F32),
            pltpu.VMEM((3, tr, tc), F32),
            pltpu.VMEM((4, tc, tc), BF16),
            pltpu.VMEM((4, tr, tc), BF16),
            pltpu.VMEM((4, tr, tc), BF16),
            pltpu.VMEM((4, 3, tr, tc), BF16),
            pltpu.VMEM((4, tr, tc), F32),
            pltpu.VMEM((5, tr, tc), F32),
            pltpu.VMEM((4, tl, tl), BF16),
            pltpu.VMEM((4, tl, tl), BF16),
            pltpu.VMEM((tr, tc), F32),
            pltpu.VMEM((tr, tc), BF16),
            pltpu.VMEM((tl, tl), F32),
            pltpu.VMEM((4, tl, tl), F32),
            pltpu.VMEM((3, tl, tl), F32),
            dma((NSEND,)),
            dma((16,)),
            dma((4,)), dma((4,)), dma((4,)),
            dma((4, NQ)), dma((4,)),
            dma((4, NH)), dma((4, NH)),
            dma((3,)), dma((4, NG)),
            dma((5, NU)), dma((3,)),
        ]
        any_spec = pl.BlockSpec(memory_space=pl.ANY)
        vmem_spec = pl.BlockSpec(memory_space=pltpu.VMEM)
        outs = [weight, mom_first, mom_second, stat_left, stat_right]
        results = pl.pallas_call(
            kernel,
            name="soap_step",
            out_shape=[pltpu.VMEM(o.shape, o.dtype) for o in outs],
            in_specs=[any_spec] * 8,
            out_specs=[vmem_spec] * 5,
            scratch_shapes=scratch,
            compiler_params=pltpu.CompilerParams(
                collective_id=0, has_side_effects=True, vmem_limit_bytes=VMEM_BYTES,
            ),
        )(weight, grad_in, mom_first, mom_second, stat_left, stat_right, basis_left, basis_right)
        results = [pltpu.with_memory_space_constraint(r, pltpu.VMEM) for r in results]
        return pl.pallas_call(
            write_out,
            name="write_out",
            out_shape=[jax.ShapeDtypeStruct(o.shape, o.dtype) for o in outs],
            in_specs=[vmem_spec] * 5,
            out_specs=[any_spec] * 5,
            scratch_shapes=[dma((5,))],
            compiler_params=pltpu.CompilerParams(vmem_limit_bytes=2**20),
        )(*results)

    return jax.shard_map(local_step, mesh=mesh, in_specs=(tile_spec,) * 8, out_specs=(tile_spec,) * 5, check_vma=False)
```

```python
import jax
import jax.numpy as jnp
from jax import lax
from jax.experimental import pallas as pl
from jax.experimental.pallas import tpu as pltpu
from jax.sharding import PartitionSpec as P

BETA1 = 0.9
BETA2 = 0.9
EPS = 1e-8
LR = 0.1
STEP = 10
BIAS_ONE = 1.0 - BETA1 ** STEP
BIAS_TWO = 1.0 - BETA2 ** STEP

MESH = pl.DeviceIdType.MESH
F32 = jnp.float32
BF16 = jnp.bfloat16
NQ = 4
NH = 2
NU = 2
NG = 2
NDEV = 4
NSEND = 160
VMEM_BYTES = 54 * 2**20

ROWS_T = (((0,), (0,)), ((), ()))
COLS_T = (((1,), (1,)), ((), ()))


def split3(x):
    a0 = x.astype(BF16)
    r = x - a0.astype(F32)
    a1 = r.astype(BF16)
    a2 = (r - a1.astype(F32)).astype(BF16)
    return a0, a1, a2


def kernel(
    w_hbm, g_hbm, m_hbm, v_hbm, l_hbm, r_hbm, ql_hbm, qr_hbm,
    wbuf, mbuf, vbuf, lbuf, racc,
    grow, gbf, gi, gj, qrc, hcol, ncol, gis, ubuf, urecv,
    qlr, qlc, hacc, kb, qrx, kx, qlf, lx, lrecv,
    ssem, lsem, r_gbf, r_qlr, r_g32, r_qr, r_qlc, r_h, r_n, r_gj, r_gi, r_u, r_qx, r_l,
):
    lay = lax.axis_index("layer")
    z = lax.axis_index("col")
    i = lax.axis_index("row")
    y, c = i // 2, i % 2
    sib = 2 * y + (1 - c)
    opp = 2 * (1 - y) + c
    dia = 2 * (1 - y) + (1 - c)
    tr, tc = grow.shape[1], grow.shape[2]
    qrows = tc // NQ
    hcols = tc // NH
    urows = tr // NU
    grows = tr // NG
    early = tc - tc // 4

    waits, qr_waits, late_waits = [], [], []
    count = [0]

    def dev(row, col):
        return (lay, col, row)

    def send(src, dst, rsem, row, col, cond=None, held=None):
        n = count[0]
        count[0] += 1

        def make():
            return pltpu.make_async_remote_copy(
                src_ref=src(), dst_ref=dst(), send_sem=ssem.at[n], recv_sem=rsem(),
                device_id=dev(row, col), device_id_type=MESH,
            )

        def go():
            make().start()

        def done():
            make().wait_send()

        if cond is None:
            go()
        else:
            pl.when(cond)(go)
        if held is None:
            waits.append((cond, done))
        else:
            held.append((cond, done))

    def settle(sent):
        for cond, done in sent:
            if cond is None:
                done()
            else:
                pl.when(cond)(done)
        sent.clear()

    def arrived(dst, rsem, row, col):
        pltpu.make_async_remote_copy(
            src_ref=dst, dst_ref=dst, send_sem=ssem.at[0], recv_sem=rsem,
            device_id=dev(row, col), device_id_type=MESH,
        ).wait_recv()

    loads = {}

    def load(name, n, src, dst):
        cp = pltpu.make_async_copy(src, dst, lsem.at[n])
        cp.start()
        loads[name] = cp

    for q in range(NQ):
        rows = pl.ds(q * qrows, qrows)
        load(("qr", q), 1 + q, qr_hbm.at[rows], racc.at[rows])
        if q == 0:
            load("g", 0, g_hbm, grow.at[z])
            load("ql", 5, ql_hbm, qlf)
    load("m", 6, m_hbm, mbuf)
    load("v", 7, v_hbm, vbuf)
    load("w", 8, w_hbm, wbuf)
    load("l", 9, l_hbm, lbuf)

    barrier = pltpu.get_barrier_semaphore()
    for row in (sib, opp, dia):
        pl.semaphore_signal(barrier, inc=1, device_id=dev(row, z), device_id_type=MESH)

    @pl.when(z > 0)
    def _():
        pl.semaphore_signal(barrier, inc=1, device_id=dev(i, z - 1), device_id_type=MESH)

    @pl.when(z < NDEV - 1)
    def _():
        pl.semaphore_signal(barrier, inc=1, device_id=dev(i, z + 1), device_id_type=MESH)

    def qr_cast(q):
        rows = pl.ds(q * qrows, qrows)
        loads[("qr", q)].wait()
        qrc[i, rows] = racc[rows].astype(BF16)

    qr_cast(0)
    loads["g"].wait()
    gbf[z] = grow[z].astype(BF16)

    inner = jnp.logical_and(z > 0, z < NDEV - 1)

    @pl.when(inner)
    def _():
        pl.semaphore_wait(barrier, 5)

    @pl.when(jnp.logical_not(inner))
    def _():
        pl.semaphore_wait(barrier, 4)

    def line_own(buf, rs):
        send(lambda: buf.at[z], lambda: buf.at[z], lambda: rs.at[z], i, z + 1, z < NDEV - 1)
        send(lambda: buf.at[z], lambda: buf.at[z], lambda: rs.at[z], i, z - 1, z > 0)

    def line_forward(buf, rs, s):
        right = jnp.logical_and(z >= s, z < NDEV - 1)
        left = jnp.logical_and(z + s < NDEV, z > 0)

        @pl.when(right)
        def _():
            arrived(buf.at[z - s], rs.at[z - s], i, z - 1)

        send(lambda: buf.at[z - s], lambda: buf.at[z - s], lambda: rs.at[z - s], i, z + 1, right)

        @pl.when(left)
        def _():
            arrived(buf.at[z + s], rs.at[z + s], i, z + 1)

        send(lambda: buf.at[z + s], lambda: buf.at[z + s], lambda: rs.at[z + s], i, z - 1, left)

    def line_last(buf, rs, s):
        @pl.when(jnp.logical_and(z >= s, z == NDEV - 1))
        def _():
            arrived(buf.at[z - s], rs.at[z - s], i, z - 1)

        @pl.when(jnp.logical_and(z + s < NDEV, z == 0))
        def _():
            arrived(buf.at[z + s], rs.at[z + s], i, z + 1)

    def qr_own(q):
        rows = pl.ds(q * qrows, qrows)
        for row in (opp, sib):
            send(lambda: qrc.at[i, rows], lambda: qrc.at[i, rows], lambda: r_qr.at[i, q], row, z, held=qr_waits)

    qr_own(0)
    line_own(gbf, r_gbf)
    loads["ql"].wait()
    qlr[z] = qlf[...].astype(BF16)
    qr_cast(1)
    line_own(qlr, r_qlr)
    for q in range(2, NQ):
        qr_cast(q)
        qr_own(q - 1)
    load("r", 10, r_hbm, racc)

    def qr_forward(q):
        rows = pl.ds(q * qrows, qrows)
        arrived(qrc.at[opp, rows], r_qr.at[opp, q], opp, z)
        send(lambda: qrc.at[opp, rows], lambda: qrc.at[opp, rows], lambda: r_qr.at[opp, q], sib, z, held=qr_waits)

    def h_add(k, q, first=False):
        rows = pl.ds(q * qrows, qrows)
        part = jnp.dot(gbf[k, :, rows], qrc[k, rows], preferred_element_type=F32)
        if first:
            hacc[...] = part
        else:
            hacc[...] += part

    qr_own(NQ - 1)

    line_forward(gbf, r_gbf, 1)
    line_forward(qlr, r_qlr, 1)
    qr_forward(0)
    line_forward(gbf, r_gbf, 2)
    line_forward(qlr, r_qlr, 2)
    line_own(grow, r_g32)
    qr_forward(1)
    for s in range(1, NDEV):
        line_last(gbf, r_gbf, s)
        line_last(qlr, r_qlr, s)

    for row in (opp, dia, sib):
        send(lambda row=row: qlr.at[row], lambda: qlc.at[i], lambda: r_qlc.at[i], row, z)
    qlc[i] = qlr[i]

    for q in range(NQ):
        h_add(i, q, first=q == 0)
    for q in range(NQ):
        rows = pl.ds(q * qrows, qrows)
        arrived(qrc.at[sib, rows], r_qr.at[sib, q], sib, z)
        h_add(sib, q)
    qr_forward(2)
    for q in range(2):
        h_add(opp, q)
    for q in range(2):
        rows = pl.ds(q * qrows, qrows)
        arrived(qrc.at[dia, rows], r_qr.at[dia, q], sib, z)
        h_add(dia, q)
    h_add(opp, 2)
    qr_forward(3)
    h_add(opp, 3)
    for q in range(2, NQ):
        rows = pl.ds(q * qrows, qrows)
        arrived(qrc.at[dia, rows], r_qr.at[dia, q], sib, z)
        h_add(dia, q)

    def own_part(buf, rs, n):
        cols = pl.ds(n * hcols, hcols)
        for row in (opp, sib):
            send(lambda: buf.at[i, :, cols], lambda: buf.at[i, :, cols], lambda: rs.at[i, n], row, z)

    def forward_part(buf, rs, n):
        cols = pl.ds(n * hcols, hcols)
        arrived(buf.at[opp, :, cols], rs.at[opp, n], opp, z)
        send(lambda: buf.at[opp, :, cols], lambda: buf.at[opp, :, cols], lambda: rs.at[opp, n], sib, z)

    def rest_part(buf, rs, n):
        cols = pl.ds(n * hcols, hcols)
        arrived(buf.at[sib, :, cols], rs.at[sib, n], sib, z)
        arrived(buf.at[dia, :, cols], rs.at[dia, n], sib, z)

    hcol[i] = hacc[...].astype(BF16)
    for n in range(NH):
        own_part(hcol, r_h, n)

    half = pl.ds(pl.multiple_of(c * (tc // 2), tc // 2), tc // 2)
    other_half = pl.ds(pl.multiple_of((1 - c) * (tc // 2), tc // 2), tc // 2)
    send(lambda: qrc.at[1, half], lambda: qrx.at[half], lambda: r_qx.at[0], i, 1, z == 0, held=qr_waits)
    send(lambda: qrc.at[2, half], lambda: qrx.at[half], lambda: r_qx.at[0], i, 2, z == 3, held=qr_waits)

    line_forward(grow, r_g32, 1)
    for row in (opp, dia, sib):
        arrived(qlc.at[row], r_qlc.at[row], row, z)
    loads["m"].wait()
    loads["v"].wait()

    for n in range(NH):
        cols = pl.ds(n * hcols, hcols)
        forward_part(hcol, r_h, n)
        rest_part(hcol, r_h, n)
        rotated = sum(
            lax.dot_general(qlc[k], hcol[k, :, cols], ROWS_T, preferred_element_type=F32) for k in range(NDEV)
        )
        hacc[:, cols] = rotated
        rotated = hacc[:, cols]
        new_first = BETA1 * mbuf[:, cols] + (1.0 - BETA1) * rotated
        new_second = BETA2 * vbuf[:, cols] + (1.0 - BETA2) * rotated * rotated
        mbuf[:, cols] = new_first
        vbuf[:, cols] = new_second
        direction = (new_first / BIAS_ONE) / (jnp.sqrt(new_second / BIAS_TWO) + EPS)
        ncol[i, :, cols] = direction.astype(BF16)
        own_part(ncol, r_n, n)
    def gj_part(src, slot, late):
        cols = pl.ds(early, tc - early) if late else pl.ds(0, early)
        n = slot + 2 * late
        return (lambda: src.at[:, cols]), (lambda: gj.at[slot, :, cols]), (lambda: r_gj.at[n])

    send(*gj_part(grow.at[z], 1, False), opp, z)
    send(lambda: grow.at[z], lambda: gj.at[0], lambda: r_gj.at[0], sib, z)

    def gi_send(b, valid):
        for n in range(NG):
            rows = pl.ds(n * grows, grows)
            send(lambda: grow.at[b, rows], lambda: gi.at[i, rows], lambda: r_gi.at[i, n], b, z, jnp.logical_and(valid, b != i))

    gi_send(z, z >= 0)
    line_last(grow, r_g32, 1)
    gi_send(z - 1, z >= 1)
    gi_send(z + 1, z + 1 < NDEV)

    for n in range(NH):
        forward_part(ncol, r_n, n)
        rest_part(ncol, r_n, n)
        cols = pl.ds(n * hcols, hcols)
        kb[:, cols] = sum(
            jnp.dot(qlr[k], ncol[k, :, cols], preferred_element_type=F32) for k in range(NDEV)
        ).astype(BF16)

    def u_send(a, h, slot, col, cond):
        rows = pl.ds(h * urows, urows)
        send(lambda: ubuf.at[a, rows], lambda: urecv.at[slot, rows], lambda: r_u.at[slot, h], i, col, cond)

    def u_first(a, to_right):
        for h in range(NU):
            if to_right:
                u_send(a, h, a, z + 1, z == 0)
            else:
                u_send(a, h, NDEV if a == NDEV - 2 else a, z - 1, z == NDEV - 1)

    for piece, starts in ((3, ((3, True),)), (0, ((0, False),)), (2, ((2, True),)), (1, ((1, False),))):
        ubuf[piece] = lax.dot_general(kb[...], qrc[piece], COLS_T, preferred_element_type=F32)
        for a, to_right in starts:
            u_first(a, to_right)
    send(lambda: kb, lambda: kx, lambda: r_qx.at[2], i, 1, z == 0)
    send(lambda: kb, lambda: kx, lambda: r_qx.at[2], i, 2, z == 3)
    line_forward(grow, r_g32, 2)

    @pl.when(inner)
    def _():
        arrived(qrx.at[half], r_qx.at[0], i, 3 * (z // 2))

    send(lambda: qrx.at[half], lambda: qrx.at[half], lambda: r_qx.at[1], sib, z, inner)

    def u_at(a, h, station, to_right):
        rows = pl.ds(h * urows, urows)
        slot = NDEV if (not to_right and station == a) else a

        @pl.when(z == station)
        def _():
            arrived(urecv.at[slot, rows], r_u.at[slot, h], i, station - 1 if to_right else station + 1)
            ubuf[a, rows] += urecv[slot, rows]

        if station != a:
            nxt = station + 1 if to_right else station - 1
            nslot = NDEV if (not to_right and nxt == a) else a
            u_send(a, h, nslot, nxt, z == station)

    line_last(grow, r_g32, 2)
    gi_send(z - 2, z >= 2)
    gi_send(z + 2, z + 2 < NDEV)

    def u_round(t):
        for h in range(NU):
            for a in (3, 2, 1):
                st = t - (3 - a)
                if 1 <= st <= a and a > 1:
                    u_at(a, h, st, True)
                    u_at(NDEV - 1 - a, h, NDEV - 1 - st, False)

    def gj_split(slot, ref, start=0, size=None):
        cols = pl.ds(start, size or tc)
        for t, term in enumerate(split3(ref[:, cols])):
            qrc[slot, pl.ds(t * tr, tr), cols] = term

    def gi_split(k, ref, n):
        rows = pl.ds(n * grows, grows)
        for t, term in enumerate(split3(ref[rows])):
            gis[k, t, rows] = term

    def right_add(k, slot, n=None, start=0, size=None, first=False):
        begin, depth = (0, tr) if n is None else (n * grows, grows)
        cols = pl.ds(start, size or tc)

        def body(m, carry):
            rows = pl.ds(pl.multiple_of(m * tr, tr), tr)
            a0, a1, a2 = [gis[k, t, pl.ds(begin, depth), rows].T for t in range(3)]
            b0, b1, b2 = [qrc[slot, pl.ds(t * tr + begin, depth), cols] for t in range(3)]
            left = jnp.concatenate([a0, a0, a0, a1, a1, a2], axis=1)
            right = jnp.concatenate([b0, b1, b2, b0, b1, b0], axis=0)
            share = (1.0 - BETA2) * jnp.dot(left, right, preferred_element_type=F32)
            old = racc[rows, cols]
            racc[rows, cols] = (BETA2 * old if first else old) + share
            return carry

        lax.fori_loop(0, tc // tr, body, 0)

    def gi_arrived(row, n):
        rows = pl.ds(n * grows, grows)
        arrived(gi.at[row, rows], r_gi.at[row, n], row, z)
        gi_split(row, gi.at[row], n)

    def left_part(k, slot):
        pieces = [gis[k, t] for t in range(3)]
        other = [gis[z, t] for t in range(3)]
        total = None
        for t, u in ((0, 0), (0, 1), (1, 0), (1, 1), (0, 2), (2, 0)):
            d = lax.dot_general(pieces[t], other[u], COLS_T, preferred_element_type=F32)
            total = d if total is None else total + d
        lx[slot] = total

    settle(qr_waits)
    gj_split(0, grow.at[z])
    arrived(gj.at[0], r_gj.at[0], sib, z)
    gj_split(1, gj.at[0])
    arrived(gj.at[1, :, pl.ds(0, early)], r_gj.at[1], opp, z)
    send(*gj_part(gj.at[1], 2, False), sib, z)
    gj_split(2, gj.at[1], 0, early)
    u_round(1)
    line_last(grow, r_g32, 3)
    gi_send(z - 3, z >= 3)
    gi_send(z + 3, z + 3 < NDEV)
    send(*gj_part(grow.at[z], 1, True), opp, z, held=late_waits)
    arrived(gj.at[2, :, pl.ds(0, early)], r_gj.at[2], sib, z)
    gj_split(3, gj.at[2], 0, early)
    loads["r"].wait()
    for n in range(NG):
        gi_split(i, grow.at[i], n)
    right_add(i, 0, first=True)
    u_round(2)
    for n in range(NG):
        gi_arrived(sib, n)
    right_add(sib, 1)
    for n in range(NG - 1):
        gi_arrived(opp, n)
        right_add(opp, 2, n, 0, early)
        gi_arrived(dia, n)
        right_add(dia, 3, n, 0, early)

    @pl.when(inner)
    def _():
        arrived(qrx.at[other_half], r_qx.at[1], sib, z)
        arrived(kx, r_qx.at[2], i, 3 * (z // 2))
        ubuf[z] += lax.dot_general(kx[...], qrx[...], COLS_T, preferred_element_type=F32)

    loads["w"].wait()
    loads["l"].wait()
    gi_arrived(dia, NG - 1)
    gi_arrived(opp, NG - 1)

    left_part(dia, 3)
    send(lambda: lx.at[3], lambda: lrecv.at[2], lambda: r_l.at[2], sib, z)
    left_part(opp, 2)
    left_part(sib, 1)
    send(lambda: lx.at[1], lambda: lrecv.at[0], lambda: r_l.at[0], sib, z)
    arrived(lrecv.at[2], r_l.at[2], sib, z)
    lx[2] += lrecv[2]
    left_part(i, 0)
    send(lambda: lx.at[2], lambda: lrecv.at[1], lambda: r_l.at[1], opp, z, held=late_waits)
    right_add(opp, 2, NG - 1, 0, early)
    arrived(gj.at[1, :, pl.ds(early, tc - early)], r_gj.at[3], opp, z)
    send(*gj_part(gj.at[1], 2, True), sib, z, held=late_waits)
    right_add(dia, 3, NG - 1, 0, early)
    gj_split(2, gj.at[1], early, tc - early)
    right_add(opp, 2, None, early, tc - early)

    u_round(3)
    wbuf[...] = wbuf[...] - LR * ubuf[z]
    settle(waits)
    arrived(gj.at[2, :, pl.ds(early, tc - early)], r_gj.at[4], sib, z)
    gj_split(3, gj.at[2], early, tc - early)
    right_add(dia, 3, None, early, tc - early)
    arrived(lrecv.at[0], r_l.at[0], sib, z)
    left_sum = lx[0] + lrecv[0]
    arrived(lrecv.at[1], r_l.at[1], opp, z)
    left_sum += lrecv[1]
    lbuf[...] = BETA2 * lbuf[...] + (1.0 - BETA2) * left_sum

    settle(waits)
    settle(late_waits)
    assert count[0] <= NSEND, count[0]


def write_out(*refs):
    ins, outs, sem = refs[:5], refs[5:10], refs[10]
    copies = [pltpu.make_async_copy(a, b, sem.at[n]) for n, (a, b) in enumerate(zip(ins, outs))]
    for cp in copies:
        cp.start()
    for cp in copies:
        cp.wait()


def solution(mesh):
    tile_spec = P(("layer", "row"), "col")

    def local_step(weight, grad_in, mom_first, mom_second, stat_left, stat_right, basis_left, basis_right):
        tr, tc = grad_in.shape
        tl = stat_left.shape[0]
        dma = pltpu.SemaphoreType.DMA
        scratch = [
            pltpu.VMEM((4, tr, tc), F32),
            pltpu.VMEM((4, tr, tc), BF16),
            pltpu.VMEM((4, tr, tc), F32),
            pltpu.VMEM((3, tr, tc), F32),
            pltpu.VMEM((4, tc, tc), BF16),
            pltpu.VMEM((4, tr, tc), BF16),
            pltpu.VMEM((4, tr, tc), BF16),
            pltpu.VMEM((4, 3, tr, tc), BF16),
            pltpu.VMEM((4, tr, tc), F32),
            pltpu.VMEM((5, tr, tc), F32),
            pltpu.VMEM((4, tl, tl), BF16),
            pltpu.VMEM((4, tl, tl), BF16),
            pltpu.VMEM((tr, tc), F32),
            pltpu.VMEM((tr, tc), BF16),
            pltpu.VMEM((tc, tc), BF16),
            pltpu.VMEM((tr, tc), BF16),
            pltpu.VMEM((tl, tl), F32),
            pltpu.VMEM((4, tl, tl), F32),
            pltpu.VMEM((3, tl, tl), F32),
            dma((NSEND,)),
            dma((16,)),
            dma((4,)), dma((4,)), dma((4,)),
            dma((4, NQ)), dma((4,)),
            dma((4, NH)), dma((4, NH)),
            dma((5,)), dma((4, NG)),
            dma((5, NU)), dma((3,)), dma((3,)),
        ]
        any_spec = pl.BlockSpec(memory_space=pl.ANY)
        vmem_spec = pl.BlockSpec(memory_space=pltpu.VMEM)
        outs = [weight, mom_first, mom_second, stat_left, stat_right]
        results = pl.pallas_call(
            kernel,
            name="soap_step",
            out_shape=[pltpu.VMEM(o.shape, o.dtype) for o in outs],
            in_specs=[any_spec] * 8,
            out_specs=[vmem_spec] * 5,
            scratch_shapes=scratch,
            compiler_params=pltpu.CompilerParams(
                collective_id=0, has_side_effects=True, vmem_limit_bytes=VMEM_BYTES,
            ),
        )(weight, grad_in, mom_first, mom_second, stat_left, stat_right, basis_left, basis_right)
        results = [pltpu.with_memory_space_constraint(r, pltpu.VMEM) for r in results]
        return pl.pallas_call(
            write_out,
            name="write_out",
            out_shape=[jax.ShapeDtypeStruct(o.shape, o.dtype) for o in outs],
            in_specs=[vmem_spec] * 5,
            out_specs=[any_spec] * 5,
            scratch_shapes=[dma((5,))],
            compiler_params=pltpu.CompilerParams(vmem_limit_bytes=2**20),
        )(*results)

    return jax.shard_map(local_step, mesh=mesh, in_specs=(tile_spec,) * 8, out_specs=(tile_spec,) * 5, check_vma=False)
```

```python
import jax
import jax.numpy as jnp
from jax import lax
from jax.experimental import pallas as pl
from jax.experimental.pallas import tpu as pltpu
from jax.sharding import PartitionSpec as P

BETA1 = 0.9
BETA2 = 0.9
EPS = 1e-8
LR = 0.1
STEP = 10
BIAS_ONE = 1.0 - BETA1 ** STEP
BIAS_TWO = 1.0 - BETA2 ** STEP

MESH = pl.DeviceIdType.MESH
F32 = jnp.float32
BF16 = jnp.bfloat16
NQ = 4
NH = 2
NU = 2
NG = 2
NDEV = 4
NSEND = 69
VMEM_BYTES = 54 * 2**20

ROWS_T = (((0,), (0,)), ((), ()))
COLS_T = (((1,), (1,)), ((), ()))


def split3(x):
    a0 = x.astype(BF16)
    r = x - a0.astype(F32)
    a1 = r.astype(BF16)
    a2 = (r - a1.astype(F32)).astype(BF16)
    return a0, a1, a2


def kernel(
    w_hbm, g_hbm, m_hbm, v_hbm, l_hbm, r_hbm, ql_hbm, qr_hbm,
    wbuf, mbuf, vbuf, lbuf, racc,
    grow, gbf, gi, gj, qrc, hcol, ncol, gis, ubuf, urecv,
    qlr, qlc, hacc, kb, qrx, kx, qlf, lx, lrecv, git,
    ssem, lsem, r_gbf, r_qlr, r_g32, r_qr, r_qlc, r_h, r_n, r_gj, r_gi, r_u, r_qx, r_l,
):
    lay = lax.axis_index("layer")
    z = lax.axis_index("col")
    i = lax.axis_index("row")
    y, c = i // 2, i % 2
    sib = 2 * y + (1 - c)
    opp = 2 * (1 - y) + c
    dia = 2 * (1 - y) + (1 - c)
    tr, tc = grow.shape[1], grow.shape[2]
    qrows = tc // NQ
    hcols = tc // NH
    urows = tr // NU
    grows = tr // NG
    gparts = (pl.ds(0, grows // 2), pl.ds(grows // 2, grows // 2), pl.ds(grows, grows))
    early = tc - tc // 4

    waits, qr_waits, late_waits, line_waits = [], [], [], []
    unused, most = list(range(NSEND)), [0]

    def dev(row, col):
        return (lay, col, row)

    def send(src, dst, rsem, row, col, cond=None, held=None):
        src, dst, rsem = src(), dst(), rsem()
        n = unused.pop(0)
        most[0] = max(most[0], n + 1)

        def make():
            return pltpu.make_async_remote_copy(
                src_ref=src, dst_ref=dst, send_sem=ssem.at[n], recv_sem=rsem,
                device_id=dev(row, col), device_id_type=MESH,
            )

        def go():
            make().start()

        def done():
            make().wait_send()

        if cond is None:
            go()
        else:
            pl.when(cond)(go)
        if held is None:
            waits.append((cond, done, n))
        else:
            held.append((cond, done, n))

    def settle(sent):
        for cond, done, n in sent:
            if cond is None:
                done()
            else:
                pl.when(cond)(done)
            unused.append(n)
        unused.sort()
        sent.clear()

    def arrived(dst, rsem, row, col):
        pltpu.make_async_remote_copy(
            src_ref=dst, dst_ref=dst, send_sem=ssem.at[0], recv_sem=rsem,
            device_id=dev(row, col), device_id_type=MESH,
        ).wait_recv()

    loads = {}

    def load(name, n, src, dst):
        cp = pltpu.make_async_copy(src, dst, lsem.at[n])
        cp.start()
        loads[name] = cp

    for q in range(NQ):
        rows = pl.ds(q * qrows, qrows)
        load(("qr", q), 1 + q, qr_hbm.at[rows], racc.at[rows])
        if q == 0:
            load("g", 0, g_hbm, grow.at[z])
            load("ql", 5, ql_hbm, qlf)
    load("m", 6, m_hbm, mbuf)
    load("v", 7, v_hbm, vbuf)
    load("w", 8, w_hbm, wbuf)
    load("l", 9, l_hbm, lbuf)

    barrier = pltpu.get_barrier_semaphore()
    for row in (sib, opp, dia):
        pl.semaphore_signal(barrier, inc=1, device_id=dev(row, z), device_id_type=MESH)

    @pl.when(z > 0)
    def _():
        pl.semaphore_signal(barrier, inc=1, device_id=dev(i, z - 1), device_id_type=MESH)

    @pl.when(z < NDEV - 1)
    def _():
        pl.semaphore_signal(barrier, inc=1, device_id=dev(i, z + 1), device_id_type=MESH)

    def qr_cast(q):
        rows = pl.ds(q * qrows, qrows)
        loads[("qr", q)].wait()
        qrc[i, rows] = racc[rows].astype(BF16)

    qr_cast(0)
    inner = jnp.logical_and(z > 0, z < NDEV - 1)

    @pl.when(inner)
    def _():
        pl.semaphore_wait(barrier, 5)

    @pl.when(jnp.logical_not(inner))
    def _():
        pl.semaphore_wait(barrier, 4)

    def line_own(buf, rs, held=None):
        send(lambda: buf.at[z], lambda: buf.at[z], lambda: rs.at[z], i, z + 1, z < NDEV - 1, held)
        send(lambda: buf.at[z], lambda: buf.at[z], lambda: rs.at[z], i, z - 1, z > 0, held)

    def line_forward(buf, rs, s, held=None):
        right = jnp.logical_and(z >= s, z < NDEV - 1)
        left = jnp.logical_and(z + s < NDEV, z > 0)

        @pl.when(right)
        def _():
            arrived(buf.at[z - s], rs.at[z - s], i, z - 1)

        send(lambda: buf.at[z - s], lambda: buf.at[z - s], lambda: rs.at[z - s], i, z + 1, right, held)

        @pl.when(left)
        def _():
            arrived(buf.at[z + s], rs.at[z + s], i, z + 1)

        send(lambda: buf.at[z + s], lambda: buf.at[z + s], lambda: rs.at[z + s], i, z - 1, left, held)

    def line_last(buf, rs, s):
        @pl.when(jnp.logical_and(z >= s, z == NDEV - 1))
        def _():
            arrived(buf.at[z - s], rs.at[z - s], i, z - 1)

        @pl.when(jnp.logical_and(z + s < NDEV, z == 0))
        def _():
            arrived(buf.at[z + s], rs.at[z + s], i, z + 1)

    def qr_own(q):
        rows = pl.ds(q * qrows, qrows)
        for row in (opp, sib):
            send(lambda: qrc.at[i, rows], lambda: qrc.at[i, rows], lambda: r_qr.at[i, q], row, z, held=qr_waits)

    qr_own(0)
    loads["g"].wait()
    gbf[z] = grow[z].astype(BF16)
    line_own(gbf, r_gbf)
    loads["ql"].wait()
    qlr[z] = qlf[...].astype(BF16)
    qr_cast(1)
    line_own(qlr, r_qlr)
    for q in range(2, NQ):
        qr_cast(q)
        qr_own(q - 1)
    load("r", 10, r_hbm, racc)

    def qr_forward(q):
        rows = pl.ds(q * qrows, qrows)
        arrived(qrc.at[opp, rows], r_qr.at[opp, q], opp, z)
        send(lambda: qrc.at[opp, rows], lambda: qrc.at[opp, rows], lambda: r_qr.at[opp, q], sib, z, held=qr_waits)

    def h_add(k, q, first=False):
        rows = pl.ds(q * qrows, qrows)
        part = jnp.dot(gbf[k, :, rows], qrc[k, rows], preferred_element_type=F32)
        if first:
            hacc[...] = part
        else:
            hacc[...] += part

    qr_own(NQ - 1)

    line_forward(gbf, r_gbf, 1)
    line_forward(qlr, r_qlr, 1)
    qr_forward(0)
    line_forward(gbf, r_gbf, 2)
    line_forward(qlr, r_qlr, 2)
    line_own(grow, r_g32, line_waits)
    qr_forward(1)
    for s in range(1, NDEV):
        line_last(gbf, r_gbf, s)
        line_last(qlr, r_qlr, s)

    for row in (opp, dia, sib):
        send(lambda row=row: qlr.at[row], lambda: qlc.at[i], lambda: r_qlc.at[i], row, z)
    qlc[i] = qlr[i]

    for q in range(NQ):
        h_add(i, q, first=q == 0)
    for q in range(NQ):
        rows = pl.ds(q * qrows, qrows)
        arrived(qrc.at[sib, rows], r_qr.at[sib, q], sib, z)
        h_add(sib, q)
    qr_forward(2)
    for q in range(2):
        h_add(opp, q)
    for q in range(2):
        rows = pl.ds(q * qrows, qrows)
        arrived(qrc.at[dia, rows], r_qr.at[dia, q], sib, z)
        h_add(dia, q)
    h_add(opp, 2)
    qr_forward(3)
    h_add(opp, 3)
    for q in range(2, NQ):
        rows = pl.ds(q * qrows, qrows)
        arrived(qrc.at[dia, rows], r_qr.at[dia, q], sib, z)
        h_add(dia, q)

    def own_part(buf, rs, n):
        cols = pl.ds(n * hcols, hcols)
        for row in (opp, sib):
            send(lambda: buf.at[i, :, cols], lambda: buf.at[i, :, cols], lambda: rs.at[i, n], row, z)

    def forward_part(buf, rs, n):
        cols = pl.ds(n * hcols, hcols)
        arrived(buf.at[opp, :, cols], rs.at[opp, n], opp, z)
        send(lambda: buf.at[opp, :, cols], lambda: buf.at[opp, :, cols], lambda: rs.at[opp, n], sib, z)

    def rest_part(buf, rs, n):
        cols = pl.ds(n * hcols, hcols)
        arrived(buf.at[sib, :, cols], rs.at[sib, n], sib, z)
        arrived(buf.at[dia, :, cols], rs.at[dia, n], sib, z)

    hcol[i] = hacc[...].astype(BF16)
    for n in range(NH):
        own_part(hcol, r_h, n)

    half = pl.ds(pl.multiple_of(c * (tc // 2), tc // 2), tc // 2)
    other_half = pl.ds(pl.multiple_of((1 - c) * (tc // 2), tc // 2), tc // 2)
    send(lambda: qrc.at[1, half], lambda: qrx.at[half], lambda: r_qx.at[0], i, 1, z == 0, held=qr_waits)
    send(lambda: qrc.at[2, half], lambda: qrx.at[half], lambda: r_qx.at[0], i, 2, z == 3, held=qr_waits)

    early_waits = waits[:]
    waits.clear()

    line_forward(grow, r_g32, 1, line_waits)
    for row in (opp, dia, sib):
        arrived(qlc.at[row], r_qlc.at[row], row, z)
    loads["m"].wait()
    loads["v"].wait()

    for n in range(NH):
        cols = pl.ds(n * hcols, hcols)
        forward_part(hcol, r_h, n)
        rest_part(hcol, r_h, n)
        rotated = sum(
            lax.dot_general(qlc[k], hcol[k, :, cols], ROWS_T, preferred_element_type=F32) for k in range(NDEV)
        )
        hacc[:, cols] = rotated
        rotated = hacc[:, cols]
        new_first = BETA1 * mbuf[:, cols] + (1.0 - BETA1) * rotated
        new_second = BETA2 * vbuf[:, cols] + (1.0 - BETA2) * rotated * rotated
        mbuf[:, cols] = new_first
        vbuf[:, cols] = new_second
        direction = (new_first / BIAS_ONE) / (jnp.sqrt(new_second / BIAS_TWO) + EPS)
        ncol[i, :, cols] = direction.astype(BF16)
        own_part(ncol, r_n, n)
    def gj_part(src, slot, late):
        cols = pl.ds(early, tc - early) if late else pl.ds(0, early)
        n = slot + 2 * late
        return (lambda: src.at[:, cols]), (lambda: gj.at[slot, :, cols]), (lambda: r_gj.at[n])

    head = gparts[0]
    ahead = 1 - 2 * y

    def relay(station, came_row, came_col):
        @pl.when(z == station)
        def _():
            arrived(gi.at[opp, head], r_gi.at[opp, 0], came_row, came_col)

        send(lambda: gi.at[opp, head], lambda: gi.at[opp, head], lambda: r_gi.at[opp, 0], i, z + ahead, z == station)

    send(lambda: grow.at[opp, head], lambda: gi.at[i, head], lambda: r_gi.at[i, 0], opp, z, z == 2 - y)

    send(*gj_part(grow.at[z], 1, False), opp, z)
    send(lambda: grow.at[z], lambda: gj.at[0], lambda: r_gj.at[0], sib, z)

    def gi_send(b, valid):
        there = jnp.logical_and(valid, b != i)
        for n, rows in enumerate(gparts):
            cond = jnp.logical_and(there, jnp.logical_or(b != opp, z == 3 - 3 * y)) if n == 0 else there
            send(lambda: grow.at[b, rows], lambda: gi.at[i, rows], lambda: r_gi.at[i, n], b, z, cond)

    gi_send(z, z >= 0)
    line_last(grow, r_g32, 1)
    gi_send(z - 1, z >= 1)
    gi_send(z + 1, z + 1 < NDEV)

    for n in range(NH):
        forward_part(ncol, r_n, n)
        rest_part(ncol, r_n, n)
        cols = pl.ds(n * hcols, hcols)
        kb[:, cols] = sum(
            jnp.dot(qlr[k], ncol[k, :, cols], preferred_element_type=F32) for k in range(NDEV)
        ).astype(BF16)

    settle(early_waits)

    def u_send(a, h, slot, col, cond):
        rows = pl.ds(h * urows, urows)
        send(lambda: ubuf.at[a, rows], lambda: urecv.at[slot, rows], lambda: r_u.at[slot, h], i, col, cond)

    def u_first(a, to_right):
        for h in range(NU):
            if to_right:
                u_send(a, h, a, z + 1, z == 0)
            else:
                u_send(a, h, NDEV if a == NDEV - 2 else a, z - 1, z == NDEV - 1)

    for piece, starts in ((3, ((3, True),)), (0, ((0, False),)), (2, ((2, True),)), (1, ((1, False),))):
        ubuf[piece] = lax.dot_general(kb[...], qrc[piece], COLS_T, preferred_element_type=F32)
        for a, to_right in starts:
            u_first(a, to_right)
    send(lambda: kb, lambda: kx, lambda: r_qx.at[2], i, 1, z == 0)
    send(lambda: kb, lambda: kx, lambda: r_qx.at[2], i, 2, z == 3)
    line_forward(grow, r_g32, 2, line_waits)

    relay(1 + y, opp, z)

    @pl.when(inner)
    def _():
        arrived(qrx.at[half], r_qx.at[0], i, 3 * (z // 2))

    send(lambda: qrx.at[half], lambda: qrx.at[half], lambda: r_qx.at[1], sib, z, inner)

    def u_at(a, h, station, to_right):
        rows = pl.ds(h * urows, urows)
        slot = NDEV if (not to_right and station == a) else a

        @pl.when(z == station)
        def _():
            arrived(urecv.at[slot, rows], r_u.at[slot, h], i, station - 1 if to_right else station + 1)
            ubuf[a, rows] += urecv[slot, rows]

        if station != a:
            nxt = station + 1 if to_right else station - 1
            nslot = NDEV if (not to_right and nxt == a) else a
            u_send(a, h, nslot, nxt, z == station)

    line_last(grow, r_g32, 2)
    gi_send(z - 2, z >= 2)
    gi_send(z + 2, z + 2 < NDEV)

    def u_round(t):
        for h in range(NU):
            for a in (3, 2, 1):
                st = t - (3 - a)
                if 1 <= st <= a and a > 1:
                    u_at(a, h, st, True)
                    u_at(NDEV - 1 - a, h, NDEV - 1 - st, False)

    def gj_split(slot, ref, start=0, size=None):
        cols = pl.ds(start, size or tc)
        for t, term in enumerate(split3(ref[:, cols])):
            qrc[slot, pl.ds(t * tr, tr), cols] = term

    def gi_split(k, ref, n):
        rows = pl.ds(n * grows, grows)
        for t, term in enumerate(split3(ref[rows])):
            gis[k, t, rows] = term

    def right_add(k, slot, n=None, start=0, size=None, first=False, turned=None):
        begin, depth = (0, tr) if n is None else (n * grows, grows)
        cols = pl.ds(start, size or tc)

        def body(m, carry):
            rows = pl.ds(pl.multiple_of(m * tr, tr), tr)
            if turned is None:
                a0, a1, a2 = [gis[k, t, pl.ds(begin, depth), rows].T for t in range(3)]
            else:
                a0, a1, a2 = [git[turned, rows, pl.ds(t * tr + begin, depth)] for t in range(3)]
            b0, b1, b2 = [qrc[slot, pl.ds(t * tr + begin, depth), cols] for t in range(3)]
            left = jnp.concatenate([a0, a0, a0, a1, a1, a2], axis=1)
            right = jnp.concatenate([b0, b1, b2, b0, b1, b0], axis=0)
            share = (1.0 - BETA2) * jnp.dot(left, right, preferred_element_type=F32)
            old = racc[rows, cols]
            racc[rows, cols] = (BETA2 * old if first else old) + share
            return carry

        lax.fori_loop(0, tc // tr, body, 0)

    def gi_arrived(row, n, turned=None):
        if n == 1:
            arrived(gi.at[row, gparts[2]], r_gi.at[row, 2], row, z)
        else:
            arrived(gi.at[row, gparts[1]], r_gi.at[row, 1], row, z)
            if row is opp:
                @pl.when(z == 3 * y)
                def _():
                    arrived(gi.at[row, head], r_gi.at[row, 0], row, z)

                @pl.when(z == 3 - 3 * y)
                def _():
                    arrived(gi.at[row, head], r_gi.at[row, 0], i, z - ahead)
            else:
                arrived(gi.at[row, head], r_gi.at[row, 0], row, z)
        gi_split(row, gi.at[row], n)
        if turned is not None:
            for t in range(3):
                git[turned, :, pl.ds(t * tr + n * grows, grows)] = gis[row, t, pl.ds(n * grows, grows)].T

    def left_part(k, slot):
        pieces = [gis[k, t] for t in range(3)]
        other = [gis[z, t] for t in range(3)]
        total = None
        for t, u in ((0, 0), (0, 1), (1, 0), (1, 1), (0, 2), (2, 0)):
            d = lax.dot_general(pieces[t], other[u], COLS_T, preferred_element_type=F32)
            total = d if total is None else total + d
        lx[slot] = total

    settle(qr_waits)
    gj_split(0, grow.at[z])
    arrived(gj.at[0], r_gj.at[0], sib, z)
    gj_split(1, gj.at[0])
    arrived(gj.at[1, :, pl.ds(0, early)], r_gj.at[1], opp, z)
    send(*gj_part(gj.at[1], 2, False), sib, z)
    relay(2 - y, i, z - ahead)
    gj_split(2, gj.at[1], 0, early)
    u_round(1)
    line_last(grow, r_g32, 3)
    gi_send(z - 3, z >= 3)
    gi_send(z + 3, z + 3 < NDEV)
    send(*gj_part(grow.at[z], 1, True), opp, z, held=late_waits)
    arrived(gj.at[2, :, pl.ds(0, early)], r_gj.at[2], sib, z)
    gj_split(3, gj.at[2], 0, early)
    loads["r"].wait()
    for n in range(NG):
        gi_split(i, grow.at[i], n)
    right_add(i, 0, first=True)
    u_round(2)
    for n in range(NG):
        gi_arrived(sib, n)
    right_add(sib, 1)
    for n in range(NG - 1):
        gi_arrived(opp, n, 0)
        right_add(opp, 2, n, 0, early, turned=0)
        gi_arrived(dia, n, 1)
        right_add(dia, 3, n, 0, early, turned=1)

    @pl.when(inner)
    def _():
        arrived(qrx.at[other_half], r_qx.at[1], sib, z)
        arrived(kx, r_qx.at[2], i, 3 * (z // 2))
        ubuf[z] += lax.dot_general(kx[...], qrx[...], COLS_T, preferred_element_type=F32)

    loads["w"].wait()
    loads["l"].wait()
    gi_arrived(dia, NG - 1, 1)
    gi_arrived(opp, NG - 1, 0)

    left_part(dia, 3)
    send(lambda: lx.at[3], lambda: lrecv.at[2], lambda: r_l.at[2], sib, z)
    left_part(opp, 2)
    left_part(sib, 1)
    send(lambda: lx.at[1], lambda: lrecv.at[0], lambda: r_l.at[0], sib, z)
    arrived(lrecv.at[2], r_l.at[2], sib, z)
    lx[2] += lrecv[2]
    send(lambda: lx.at[2], lambda: lrecv.at[1], lambda: r_l.at[1], opp, z, held=late_waits)
    left_part(i, 0)
    right_add(opp, 2, NG - 1, 0, early, turned=0)
    arrived(gj.at[1, :, pl.ds(early, tc - early)], r_gj.at[3], opp, z)
    send(*gj_part(gj.at[1], 2, True), sib, z, held=late_waits)
    right_add(dia, 3, NG - 1, 0, early, turned=1)
    gj_split(2, gj.at[1], early, tc - early)
    right_add(opp, 2, None, early, tc - early, turned=0)

    u_round(3)
    wbuf[...] = wbuf[...] - LR * ubuf[z]
    settle(waits)
    settle(line_waits)
    arrived(gj.at[2, :, pl.ds(early, tc - early)], r_gj.at[4], sib, z)
    gj_split(3, gj.at[2], early, tc - early)
    right_add(dia, 3, None, early, tc - early, turned=1)
    arrived(lrecv.at[0], r_l.at[0], sib, z)
    left_sum = lx[0] + lrecv[0]
    arrived(lrecv.at[1], r_l.at[1], opp, z)
    left_sum += lrecv[1]
    lbuf[...] = BETA2 * lbuf[...] + (1.0 - BETA2) * left_sum

    settle(waits)
    settle(late_waits)
    assert most[0] == NSEND, most[0]


def write_out(*refs):
    ins, outs, sem = refs[:5], refs[5:10], refs[10]
    copies = []
    for a, b in zip(ins, outs):
        step = a.shape[0] // 4
        for n in range(4):
            rows = pl.ds(n * step, step)
            copies.append(pltpu.make_async_copy(a.at[rows], b.at[rows], sem.at[len(copies)]))
    for cp in copies:
        cp.start()
    for cp in copies:
        cp.wait()


def solution(mesh):
    tile_spec = P(("layer", "row"), "col")

    def local_step(weight, grad_in, mom_first, mom_second, stat_left, stat_right, basis_left, basis_right):
        tr, tc = grad_in.shape
        tl = stat_left.shape[0]
        dma = pltpu.SemaphoreType.DMA
        scratch = [
            pltpu.VMEM((4, tr, tc), F32),
            pltpu.VMEM((4, tr, tc), BF16),
            pltpu.VMEM((4, tr, tc), F32),
            pltpu.VMEM((3, tr, tc), F32),
            pltpu.VMEM((4, tc, tc), BF16),
            pltpu.VMEM((4, tr, tc), BF16),
            pltpu.VMEM((4, tr, tc), BF16),
            pltpu.VMEM((4, 3, tr, tc), BF16),
            pltpu.VMEM((4, tr, tc), F32),
            pltpu.VMEM((5, tr, tc), F32),
            pltpu.VMEM((4, tl, tl), BF16),
            pltpu.VMEM((4, tl, tl), BF16),
            pltpu.VMEM((tr, tc), F32),
            pltpu.VMEM((tr, tc), BF16),
            pltpu.VMEM((tc, tc), BF16),
            pltpu.VMEM((tr, tc), BF16),
            pltpu.VMEM((tl, tl), F32),
            pltpu.VMEM((4, tl, tl), F32),
            pltpu.VMEM((3, tl, tl), F32),
            pltpu.VMEM((2, tc, 3 * tr), BF16),
            dma((NSEND,)),
            dma((11,)),
            dma((4,)), dma((4,)), dma((4,)),
            dma((4, NQ)), dma((4,)),
            dma((4, NH)), dma((4, NH)),
            dma((5,)), dma((4, 3)),
            dma((5, NU)), dma((3,)), dma((3,)),
        ]
        any_spec = pl.BlockSpec(memory_space=pl.ANY)
        vmem_spec = pl.BlockSpec(memory_space=pltpu.VMEM)
        outs = [weight, mom_first, mom_second, stat_left, stat_right]
        results = pl.pallas_call(
            kernel,
            name="soap_step",
            out_shape=[pltpu.VMEM(o.shape, o.dtype) for o in outs],
            in_specs=[any_spec] * 8,
            out_specs=[vmem_spec] * 5,
            scratch_shapes=scratch,
            compiler_params=pltpu.CompilerParams(
                collective_id=0, has_side_effects=True, vmem_limit_bytes=VMEM_BYTES,
            ),
        )(weight, grad_in, mom_first, mom_second, stat_left, stat_right, basis_left, basis_right)
        results = [pltpu.with_memory_space_constraint(r, pltpu.VMEM) for r in results]
        return pl.pallas_call(
            write_out,
            name="write_out",
            out_shape=[jax.ShapeDtypeStruct(o.shape, o.dtype) for o in outs],
            in_specs=[vmem_spec] * 5,
            out_specs=[any_spec] * 5,
            scratch_shapes=[dma((20,))],
            compiler_params=pltpu.CompilerParams(vmem_limit_bytes=2**20),
        )(*results)

    return jax.shard_map(local_step, mesh=mesh, in_specs=(tile_spec,) * 8, out_specs=(tile_spec,) * 5, check_vma=False)
```

```python
import jax
import jax.numpy as jnp
from jax import lax
from jax.experimental import pallas as pl
from jax.experimental.pallas import tpu as pltpu
from jax.sharding import PartitionSpec as P

BETA1 = 0.9
BETA2 = 0.9
EPS = 1e-8
LR = 0.1
STEP = 10
BIAS_ONE = 1.0 - BETA1 ** STEP
BIAS_TWO = 1.0 - BETA2 ** STEP

MESH = pl.DeviceIdType.MESH
F32 = jnp.float32
BF16 = jnp.bfloat16
NQ = 4
NH = 2
NU = 2
NG = 2
NDEV = 4
NSEND = 69
VMEM_BYTES = 56 * 2**20

ROWS_T = (((0,), (0,)), ((), ()))
COLS_T = (((1,), (1,)), ((), ()))


def split3(x):
    a0 = x.astype(BF16)
    r = x - a0.astype(F32)
    a1 = r.astype(BF16)
    a2 = (r - a1.astype(F32)).astype(BF16)
    return a0, a1, a2


def kernel(
    w_hbm, g_hbm, m_hbm, v_hbm, l_hbm, r_hbm, ql_hbm, qr_hbm,
    wbuf, mbuf, vbuf, lbuf, racc,
    grow, gbf, gi, gj, qrc, hcol, ncol, gis, ubuf, urecv,
    qlr, qlc, hacc, kb, qrx, kx, qlf, lx, lrecv, git,
    ssem, lsem, r_gbf, r_qlr, r_g32, r_qr, r_qlc, r_h, r_n, r_gj, r_gi, r_u, r_qx, r_l,
):
    lay = lax.axis_index("layer")
    z = lax.axis_index("col")
    i = lax.axis_index("row")
    y, c = i // 2, i % 2
    sib = 2 * y + (1 - c)
    opp = 2 * (1 - y) + c
    dia = 2 * (1 - y) + (1 - c)
    tr, tc = grow.shape[1], grow.shape[2]
    qrows = tc // NQ
    hcols = tc // NH
    urows = tr // NU
    grows = tr // NG
    head_rows = 3 * grows // 4
    gparts = (pl.ds(0, head_rows), pl.ds(head_rows, grows - head_rows), pl.ds(grows, grows))
    early = tc - tc // 4

    waits, qr_waits, late_waits, line_waits = [], [], [], []
    unused, most = list(range(NSEND)), [0]

    def dev(row, col):
        return (lay, col, row)

    def send(src, dst, rsem, row, col, cond=None, held=None):
        src, dst, rsem = src(), dst(), rsem()
        n = unused.pop(0)
        most[0] = max(most[0], n + 1)

        def make():
            return pltpu.make_async_remote_copy(
                src_ref=src, dst_ref=dst, send_sem=ssem.at[n], recv_sem=rsem,
                device_id=dev(row, col), device_id_type=MESH,
            )

        def go():
            make().start()

        def done():
            make().wait_send()

        if cond is None:
            go()
        else:
            pl.when(cond)(go)
        if held is None:
            waits.append((cond, done, n))
        else:
            held.append((cond, done, n))

    def settle(sent):
        for cond, done, n in sent:
            if cond is None:
                done()
            else:
                pl.when(cond)(done)
            unused.append(n)
        unused.sort()
        sent.clear()

    def arrived(dst, rsem, row, col):
        pltpu.make_async_remote_copy(
            src_ref=dst, dst_ref=dst, send_sem=ssem.at[0], recv_sem=rsem,
            device_id=dev(row, col), device_id_type=MESH,
        ).wait_recv()

    loads = {}

    def load(name, n, src, dst):
        cp = pltpu.make_async_copy(src, dst, lsem.at[n])
        cp.start()
        loads[name] = cp

    for q in range(NQ):
        rows = pl.ds(q * qrows, qrows)
        load(("qr", q), 1 + q, qr_hbm.at[rows], racc.at[rows])
        if q == 0:
            load("g", 0, g_hbm, grow.at[z])
            load("ql", 5, ql_hbm, qlf)
    load("m", 6, m_hbm, mbuf)
    load("v", 7, v_hbm, vbuf)
    load("w", 8, w_hbm, wbuf)
    load("l", 9, l_hbm, lbuf)

    barrier = pltpu.get_barrier_semaphore()
    for row in (sib, opp, dia):
        pl.semaphore_signal(barrier, inc=1, device_id=dev(row, z), device_id_type=MESH)

    @pl.when(z > 0)
    def _():
        pl.semaphore_signal(barrier, inc=1, device_id=dev(i, z - 1), device_id_type=MESH)

    @pl.when(z < NDEV - 1)
    def _():
        pl.semaphore_signal(barrier, inc=1, device_id=dev(i, z + 1), device_id_type=MESH)

    def qr_cast(q):
        rows = pl.ds(q * qrows, qrows)
        loads[("qr", q)].wait()
        qrc[i, rows] = racc[rows].astype(BF16)

    qr_cast(0)
    inner = jnp.logical_and(z > 0, z < NDEV - 1)

    @pl.when(inner)
    def _():
        pl.semaphore_wait(barrier, 5)

    @pl.when(jnp.logical_not(inner))
    def _():
        pl.semaphore_wait(barrier, 4)

    def line_own(buf, rs, held=None):
        send(lambda: buf.at[z], lambda: buf.at[z], lambda: rs.at[z], i, z + 1, z < NDEV - 1, held)
        send(lambda: buf.at[z], lambda: buf.at[z], lambda: rs.at[z], i, z - 1, z > 0, held)

    def line_forward(buf, rs, s, held=None):
        right = jnp.logical_and(z >= s, z < NDEV - 1)
        left = jnp.logical_and(z + s < NDEV, z > 0)

        @pl.when(right)
        def _():
            arrived(buf.at[z - s], rs.at[z - s], i, z - 1)

        send(lambda: buf.at[z - s], lambda: buf.at[z - s], lambda: rs.at[z - s], i, z + 1, right, held)

        @pl.when(left)
        def _():
            arrived(buf.at[z + s], rs.at[z + s], i, z + 1)

        send(lambda: buf.at[z + s], lambda: buf.at[z + s], lambda: rs.at[z + s], i, z - 1, left, held)

    def line_last(buf, rs, s):
        @pl.when(jnp.logical_and(z >= s, z == NDEV - 1))
        def _():
            arrived(buf.at[z - s], rs.at[z - s], i, z - 1)

        @pl.when(jnp.logical_and(z + s < NDEV, z == 0))
        def _():
            arrived(buf.at[z + s], rs.at[z + s], i, z + 1)

    def qr_own(q):
        rows = pl.ds(q * qrows, qrows)
        for row in (opp, sib):
            send(lambda: qrc.at[i, rows], lambda: qrc.at[i, rows], lambda: r_qr.at[i, q], row, z, held=qr_waits)

    qr_own(0)
    loads["g"].wait()
    gbf[z] = grow[z].astype(BF16)
    line_own(gbf, r_gbf)
    loads["ql"].wait()
    qlr[z] = qlf[...].astype(BF16)
    qr_cast(1)
    line_own(qlr, r_qlr)
    for q in range(2, NQ):
        qr_cast(q)
        qr_own(q - 1)
    load("r", 10, r_hbm, racc)

    def qr_forward(q):
        rows = pl.ds(q * qrows, qrows)
        arrived(qrc.at[opp, rows], r_qr.at[opp, q], opp, z)
        send(lambda: qrc.at[opp, rows], lambda: qrc.at[opp, rows], lambda: r_qr.at[opp, q], sib, z, held=qr_waits)

    def h_add(k, q, first=False):
        rows = pl.ds(q * qrows, qrows)
        part = jnp.dot(gbf[k, :, rows], qrc[k, rows], preferred_element_type=F32)
        if first:
            hacc[...] = part
        else:
            hacc[...] += part

    qr_own(NQ - 1)

    line_forward(gbf, r_gbf, 1)
    line_forward(qlr, r_qlr, 1)
    qr_forward(0)
    line_forward(gbf, r_gbf, 2)
    line_forward(qlr, r_qlr, 2)
    line_own(grow, r_g32, line_waits)
    qr_forward(1)
    for s in range(1, NDEV):
        line_last(gbf, r_gbf, s)
        line_last(qlr, r_qlr, s)

    for row in (opp, dia, sib):
        send(lambda row=row: qlr.at[row], lambda: qlc.at[i], lambda: r_qlc.at[i], row, z)
    qlc[i] = qlr[i]

    for q in range(NQ):
        h_add(i, q, first=q == 0)
    for q in range(NQ):
        rows = pl.ds(q * qrows, qrows)
        arrived(qrc.at[sib, rows], r_qr.at[sib, q], sib, z)
        h_add(sib, q)
    qr_forward(2)
    for q in range(2):
        h_add(opp, q)
    for q in range(2):
        rows = pl.ds(q * qrows, qrows)
        arrived(qrc.at[dia, rows], r_qr.at[dia, q], sib, z)
        h_add(dia, q)
    h_add(opp, 2)
    qr_forward(3)
    h_add(opp, 3)
    for q in range(2, NQ):
        rows = pl.ds(q * qrows, qrows)
        arrived(qrc.at[dia, rows], r_qr.at[dia, q], sib, z)
        h_add(dia, q)

    def own_part(buf, rs, n):
        cols = pl.ds(n * hcols, hcols)
        for row in (opp, sib):
            send(lambda: buf.at[i, :, cols], lambda: buf.at[i, :, cols], lambda: rs.at[i, n], row, z)

    def forward_part(buf, rs, n):
        cols = pl.ds(n * hcols, hcols)
        arrived(buf.at[opp, :, cols], rs.at[opp, n], opp, z)
        send(lambda: buf.at[opp, :, cols], lambda: buf.at[opp, :, cols], lambda: rs.at[opp, n], sib, z)

    def rest_part(buf, rs, n):
        cols = pl.ds(n * hcols, hcols)
        arrived(buf.at[sib, :, cols], rs.at[sib, n], sib, z)
        arrived(buf.at[dia, :, cols], rs.at[dia, n], sib, z)

    hcol[i] = hacc[...].astype(BF16)
    for n in range(NH):
        own_part(hcol, r_h, n)

    half = pl.ds(pl.multiple_of(c * (tc // 2), tc // 2), tc // 2)
    other_half = pl.ds(pl.multiple_of((1 - c) * (tc // 2), tc // 2), tc // 2)
    send(lambda: qrc.at[1, half], lambda: qrx.at[half], lambda: r_qx.at[0], i, 1, z == 0, held=qr_waits)
    send(lambda: qrc.at[2, half], lambda: qrx.at[half], lambda: r_qx.at[0], i, 2, z == 3, held=qr_waits)

    early_waits = waits[:]
    waits.clear()

    line_forward(grow, r_g32, 1, line_waits)
    for row in (opp, dia, sib):
        arrived(qlc.at[row], r_qlc.at[row], row, z)
    loads["m"].wait()
    loads["v"].wait()

    for n in range(NH):
        cols = pl.ds(n * hcols, hcols)
        forward_part(hcol, r_h, n)
        rest_part(hcol, r_h, n)
        rotated = sum(
            lax.dot_general(qlc[k], hcol[k, :, cols], ROWS_T, preferred_element_type=F32) for k in range(NDEV)
        )
        hacc[:, cols] = rotated
        rotated = hacc[:, cols]
        new_first = BETA1 * mbuf[:, cols] + (1.0 - BETA1) * rotated
        new_second = BETA2 * vbuf[:, cols] + (1.0 - BETA2) * rotated * rotated
        mbuf[:, cols] = new_first
        vbuf[:, cols] = new_second
        direction = (new_first / BIAS_ONE) / (jnp.sqrt(new_second / BIAS_TWO) + EPS)
        ncol[i, :, cols] = direction.astype(BF16)
        own_part(ncol, r_n, n)
    def gj_part(src, slot, late):
        cols = pl.ds(early, tc - early) if late else pl.ds(0, early)
        n = slot + 2 * late
        return (lambda: src.at[:, cols]), (lambda: gj.at[slot, :, cols]), (lambda: r_gj.at[n])

    head = gparts[0]
    ahead = 1 - 2 * y

    def relay(station, came_row, came_col):
        @pl.when(z == station)
        def _():
            arrived(gi.at[opp, head], r_gi.at[opp, 0], came_row, came_col)

        send(lambda: gi.at[opp, head], lambda: gi.at[opp, head], lambda: r_gi.at[opp, 0], i, z + ahead, z == station)

    send(lambda: grow.at[opp, head], lambda: gi.at[i, head], lambda: r_gi.at[i, 0], opp, z, z == 2 - y)

    send(*gj_part(grow.at[z], 1, False), opp, z)
    send(lambda: grow.at[z], lambda: gj.at[0], lambda: r_gj.at[0], sib, z)

    def gi_send(b, valid):
        there = jnp.logical_and(valid, b != i)
        for n, rows in enumerate(gparts):
            cond = jnp.logical_and(there, jnp.logical_or(b != opp, z == 3 - 3 * y)) if n == 0 else there
            send(lambda: grow.at[b, rows], lambda: gi.at[i, rows], lambda: r_gi.at[i, n], b, z, cond)

    gi_send(z, z >= 0)
    line_last(grow, r_g32, 1)
    gi_send(z - 1, z >= 1)
    gi_send(z + 1, z + 1 < NDEV)

    for n in range(NH):
        forward_part(ncol, r_n, n)
        rest_part(ncol, r_n, n)
        cols = pl.ds(n * hcols, hcols)
        kb[:, cols] = sum(
            jnp.dot(qlr[k], ncol[k, :, cols], preferred_element_type=F32) for k in range(NDEV)
        ).astype(BF16)

    settle(early_waits)

    def u_send(a, h, slot, col, cond):
        rows = pl.ds(h * urows, urows)
        send(lambda: ubuf.at[a, rows], lambda: urecv.at[slot, rows], lambda: r_u.at[slot, h], i, col, cond)

    def u_first(a, to_right):
        for h in range(NU):
            if to_right:
                u_send(a, h, a, z + 1, z == 0)
            else:
                u_send(a, h, NDEV if a == NDEV - 2 else a, z - 1, z == NDEV - 1)

    for piece, starts in ((3, ((3, True),)), (0, ((0, False),)), (2, ((2, True),)), (1, ((1, False),))):
        ubuf[piece] = lax.dot_general(kb[...], qrc[piece], COLS_T, preferred_element_type=F32)
        for a, to_right in starts:
            u_first(a, to_right)
    send(lambda: kb, lambda: kx, lambda: r_qx.at[2], i, 1, z == 0)
    send(lambda: kb, lambda: kx, lambda: r_qx.at[2], i, 2, z == 3)
    line_forward(grow, r_g32, 2, line_waits)

    relay(1 + y, opp, z)

    @pl.when(inner)
    def _():
        arrived(qrx.at[half], r_qx.at[0], i, 3 * (z // 2))

    send(lambda: qrx.at[half], lambda: qrx.at[half], lambda: r_qx.at[1], sib, z, inner)

    def u_at(a, h, station, to_right):
        rows = pl.ds(h * urows, urows)
        slot = NDEV if (not to_right and station == a) else a

        @pl.when(z == station)
        def _():
            arrived(urecv.at[slot, rows], r_u.at[slot, h], i, station - 1 if to_right else station + 1)
            ubuf[a, rows] += urecv[slot, rows]

        if station != a:
            nxt = station + 1 if to_right else station - 1
            nslot = NDEV if (not to_right and nxt == a) else a
            u_send(a, h, nslot, nxt, z == station)

    line_last(grow, r_g32, 2)
    gi_send(z - 2, z >= 2)
    gi_send(z + 2, z + 2 < NDEV)
    far = jnp.logical_or(jnp.logical_and(z == 0, i == 3), jnp.logical_and(z == 3, i == 0))

    def u_round(t):
        for h in range(NU):
            for a in (3, 2, 1):
                st = t - (3 - a)
                if 1 <= st <= a and a > 1:
                    u_at(a, h, st, True)
                    u_at(NDEV - 1 - a, h, NDEV - 1 - st, False)

    def gj_split(slot, ref, start=0, size=None):
        cols = pl.ds(start, size or tc)
        for t, term in enumerate(split3(ref[:, cols])):
            qrc[slot, pl.ds(t * tr, tr), cols] = term

    def gi_split(k, ref, n):
        rows = pl.ds(n * grows, grows)
        for t, term in enumerate(split3(ref[rows])):
            gis[k, t, rows] = term

    def right_add(k, slot, n=None, start=0, size=None, first=False, turned=None):
        begin, depth = (0, tr) if n is None else (n * grows, grows)
        cols = pl.ds(start, size or tc)

        def body(m, carry):
            rows = pl.ds(pl.multiple_of(m * tr, tr), tr)
            if turned is None:
                a0, a1, a2 = [gis[k, t, pl.ds(begin, depth), rows].T for t in range(3)]
            else:
                a0, a1, a2 = [git[turned, rows, pl.ds(t * tr + begin, depth)] for t in range(3)]
            b0, b1, b2 = [qrc[slot, pl.ds(t * tr + begin, depth), cols] for t in range(3)]
            left = jnp.concatenate([a0, a0, a0, a1, a1, a2], axis=1)
            right = jnp.concatenate([b0, b1, b2, b0, b1, b0], axis=0)
            share = (1.0 - BETA2) * jnp.dot(left, right, preferred_element_type=F32)
            old = racc[rows, cols]
            racc[rows, cols] = (BETA2 * old if first else old) + share
            return carry

        lax.fori_loop(0, tc // tr, body, 0)

    def gi_arrived(row, n, turned=None):
        if n == 1:
            arrived(gi.at[row, gparts[2]], r_gi.at[row, 2], row, z)
        else:
            arrived(gi.at[row, gparts[1]], r_gi.at[row, 1], row, z)
            if row is opp:
                @pl.when(z == 3 * y)
                def _():
                    arrived(gi.at[row, head], r_gi.at[row, 0], row, z)

                @pl.when(z == 3 - 3 * y)
                def _():
                    arrived(gi.at[row, head], r_gi.at[row, 0], i, z - ahead)
            else:
                arrived(gi.at[row, head], r_gi.at[row, 0], row, z)
        gi_split(row, gi.at[row], n)
        if turned is not None:
            for t in range(3):
                git[turned, :, pl.ds(t * tr + n * grows, grows)] = gis[row, t, pl.ds(n * grows, grows)].T

    def left_part(k, slot):
        pieces = [gis[k, t] for t in range(3)]
        other = [gis[z, t] for t in range(3)]
        total = None
        for t, u in ((0, 0), (0, 1), (1, 0), (1, 1), (0, 2), (2, 0)):
            d = lax.dot_general(pieces[t], other[u], COLS_T, preferred_element_type=F32)
            total = d if total is None else total + d
        lx[slot] = total

    settle(qr_waits)
    gj_split(0, grow.at[z])
    arrived(gj.at[0], r_gj.at[0], sib, z)
    gj_split(1, gj.at[0])
    loads["r"].wait()

    def chip_rows():
        for n in range(NG):
            gi_split(i, grow.at[i], n)
        right_add(i, 0, first=True)
        for n in range(NG):
            gi_arrived(sib, n)
        right_add(sib, 1)

    pl.when(jnp.logical_not(far))(chip_rows)
    arrived(gj.at[1, :, pl.ds(0, early)], r_gj.at[1], opp, z)
    send(*gj_part(gj.at[1], 2, False), sib, z)
    relay(2 - y, i, z - ahead)
    gj_split(2, gj.at[1], 0, early)
    u_round(1)
    line_last(grow, r_g32, 3)
    gi_send(z - 3, z >= 3)
    gi_send(z + 3, z + 3 < NDEV)
    send(*gj_part(grow.at[z], 1, True), opp, z, held=late_waits)
    arrived(gj.at[2, :, pl.ds(0, early)], r_gj.at[2], sib, z)
    gj_split(3, gj.at[2], 0, early)
    pl.when(far)(chip_rows)
    u_round(2)
    for n in range(NG - 1):
        gi_arrived(opp, n, 0)
        right_add(opp, 2, n, 0, early, turned=0)
        gi_arrived(dia, n, 1)
        right_add(dia, 3, n, 0, early, turned=1)

    @pl.when(inner)
    def _():
        arrived(qrx.at[other_half], r_qx.at[1], sib, z)
        arrived(kx, r_qx.at[2], i, 3 * (z // 2))
        ubuf[z] += lax.dot_general(kx[...], qrx[...], COLS_T, preferred_element_type=F32)

    loads["w"].wait()
    loads["l"].wait()
    gi_arrived(dia, NG - 1, 1)
    gi_arrived(opp, NG - 1, 0)

    left_part(dia, 3)
    send(lambda: lx.at[3], lambda: lrecv.at[2], lambda: r_l.at[2], sib, z)
    left_part(opp, 2)
    left_part(sib, 1)
    send(lambda: lx.at[1], lambda: lrecv.at[0], lambda: r_l.at[0], sib, z)
    arrived(lrecv.at[2], r_l.at[2], sib, z)
    lx[2] += lrecv[2]
    send(lambda: lx.at[2], lambda: lrecv.at[1], lambda: r_l.at[1], opp, z, held=late_waits)
    left_part(i, 0)
    right_add(opp, 2, NG - 1, 0, early, turned=0)
    arrived(gj.at[1, :, pl.ds(early, tc - early)], r_gj.at[3], opp, z)
    send(*gj_part(gj.at[1], 2, True), sib, z, held=late_waits)
    right_add(dia, 3, NG - 1, 0, early, turned=1)
    gj_split(2, gj.at[1], early, tc - early)
    right_add(opp, 2, None, early, tc - early, turned=0)

    u_round(3)
    wbuf[...] = wbuf[...] - LR * ubuf[z]
    settle(waits)
    settle(line_waits)
    arrived(gj.at[2, :, pl.ds(early, tc - early)], r_gj.at[4], sib, z)
    gj_split(3, gj.at[2], early, tc - early)
    right_add(dia, 3, None, early, tc - early, turned=1)
    arrived(lrecv.at[0], r_l.at[0], sib, z)
    left_sum = lx[0] + lrecv[0]
    arrived(lrecv.at[1], r_l.at[1], opp, z)
    left_sum += lrecv[1]
    lbuf[...] = BETA2 * lbuf[...] + (1.0 - BETA2) * left_sum

    settle(waits)
    settle(late_waits)
    assert most[0] == NSEND, most[0]


def write_out(*refs):
    ins, outs, sem = refs[:5], refs[5:10], refs[10]
    copies = []
    for a, b in zip(ins, outs):
        step = a.shape[0] // 4
        for n in range(4):
            rows = pl.ds(n * step, step)
            copies.append(pltpu.make_async_copy(a.at[rows], b.at[rows], sem.at[len(copies)]))
    for cp in copies:
        cp.start()
    for cp in copies:
        cp.wait()


def solution(mesh):
    tile_spec = P(("layer", "row"), "col")

    def local_step(weight, grad_in, mom_first, mom_second, stat_left, stat_right, basis_left, basis_right):
        tr, tc = grad_in.shape
        tl = stat_left.shape[0]
        dma = pltpu.SemaphoreType.DMA
        scratch = [
            pltpu.VMEM((4, tr, tc), F32),
            pltpu.VMEM((4, tr, tc), BF16),
            pltpu.VMEM((4, tr, tc), F32),
            pltpu.VMEM((3, tr, tc), F32),
            pltpu.VMEM((4, tc, tc), BF16),
            pltpu.VMEM((4, tr, tc), BF16),
            pltpu.VMEM((4, tr, tc), BF16),
            pltpu.VMEM((4, 3, tr, tc), BF16),
            pltpu.VMEM((4, tr, tc), F32),
            pltpu.VMEM((5, tr, tc), F32),
            pltpu.VMEM((4, tl, tl), BF16),
            pltpu.VMEM((4, tl, tl), BF16),
            pltpu.VMEM((tr, tc), F32),
            pltpu.VMEM((tr, tc), BF16),
            pltpu.VMEM((tc, tc), BF16),
            pltpu.VMEM((tr, tc), BF16),
            pltpu.VMEM((tl, tl), F32),
            pltpu.VMEM((4, tl, tl), F32),
            pltpu.VMEM((3, tl, tl), F32),
            pltpu.VMEM((2, tc, 3 * tr), BF16),
            dma((NSEND,)),
            dma((11,)),
            dma((4,)), dma((4,)), dma((4,)),
            dma((4, NQ)), dma((4,)),
            dma((4, NH)), dma((4, NH)),
            dma((5,)), dma((4, 3)),
            dma((5, NU)), dma((3,)), dma((3,)),
        ]
        any_spec = pl.BlockSpec(memory_space=pl.ANY)
        vmem_spec = pl.BlockSpec(memory_space=pltpu.VMEM)
        outs = [weight, mom_first, mom_second, stat_left, stat_right]
        results = pl.pallas_call(
            kernel,
            name="soap_step",
            out_shape=[pltpu.VMEM(o.shape, o.dtype) for o in outs],
            in_specs=[any_spec] * 8,
            out_specs=[vmem_spec] * 5,
            scratch_shapes=scratch,
            compiler_params=pltpu.CompilerParams(
                collective_id=0, has_side_effects=True, vmem_limit_bytes=VMEM_BYTES,
            ),
        )(weight, grad_in, mom_first, mom_second, stat_left, stat_right, basis_left, basis_right)
        results = [pltpu.with_memory_space_constraint(r, pltpu.VMEM) for r in results]
        return pl.pallas_call(
            write_out,
            name="write_out",
            out_shape=[jax.ShapeDtypeStruct(o.shape, o.dtype) for o in outs],
            in_specs=[vmem_spec] * 5,
            out_specs=[any_spec] * 5,
            scratch_shapes=[dma((20,))],
            compiler_params=pltpu.CompilerParams(vmem_limit_bytes=2**20),
        )(*results)

    return jax.shard_map(local_step, mesh=mesh, in_specs=(tile_spec,) * 8, out_specs=(tile_spec,) * 5, check_vma=False)
```

```python
import jax
import jax.numpy as jnp
from jax import lax
from jax.experimental import pallas as pl
from jax.experimental.pallas import tpu as pltpu
from jax.sharding import PartitionSpec as P

BETA1 = 0.9
BETA2 = 0.9
EPS = 1e-8
LR = 0.1
STEP = 10
BIAS_ONE = 1.0 - BETA1 ** STEP
BIAS_TWO = 1.0 - BETA2 ** STEP

MESH = pl.DeviceIdType.MESH
F32 = jnp.float32
BF16 = jnp.bfloat16
NQ = 4
NH = 2
NU = 2
NG = 2
NDEV = 4
NSEND = 68
VMEM_BYTES = 56 * 2**20

ROWS_T = (((0,), (0,)), ((), ()))
COLS_T = (((1,), (1,)), ((), ()))


def split3(x):
    a0 = x.astype(BF16)
    r = x - a0.astype(F32)
    a1 = r.astype(BF16)
    a2 = (r - a1.astype(F32)).astype(BF16)
    return a0, a1, a2


def kernel(
    w_hbm, g_hbm, m_hbm, v_hbm, l_hbm, r_hbm, ql_hbm, qr_hbm,
    wbuf, mbuf, vbuf, lbuf, racc,
    grow, gbf, gi, gj, qrc, hcol, ncol, gis, ubuf, urecv,
    qlr, qlc, hacc, kb, qrx, kx, qlf, lx, lrecv, git,
    ssem, lsem, r_gbf, r_qlr, r_g32, r_qr, r_qlc, r_h, r_n, r_gj, r_gi, r_u, r_qx, r_l,
):
    lay = lax.axis_index("layer")
    z = lax.axis_index("col")
    i = lax.axis_index("row")
    y, c = i // 2, i % 2
    sib = 2 * y + (1 - c)
    opp = 2 * (1 - y) + c
    dia = 2 * (1 - y) + (1 - c)
    tr, tc = grow.shape[1], grow.shape[2]
    qrows = tc // NQ
    hcols = tc // NH
    urows = tr // NU
    grows = tr // NG
    head_rows = 3 * grows // 4
    gparts = (pl.ds(0, head_rows), pl.ds(head_rows, grows - head_rows), pl.ds(grows, grows))
    early = tc - tc // 4

    waits, qr_waits, late_waits, line_waits = [], [], [], []
    unused, most = list(range(NSEND)), [0]

    def dev(row, col):
        return (lay, col, row)

    def send(src, dst, rsem, row, col, cond=None, held=None):
        src, dst, rsem = src(), dst(), rsem()
        n = unused.pop(0)
        most[0] = max(most[0], n + 1)

        def make():
            return pltpu.make_async_remote_copy(
                src_ref=src, dst_ref=dst, send_sem=ssem.at[n], recv_sem=rsem,
                device_id=dev(row, col), device_id_type=MESH,
            )

        def go():
            make().start()

        def done():
            make().wait_send()

        if cond is None:
            go()
        else:
            pl.when(cond)(go)
        if held is None:
            waits.append((cond, done, n))
        else:
            held.append((cond, done, n))

    def settle(sent):
        for cond, done, n in sent:
            if cond is None:
                done()
            else:
                pl.when(cond)(done)
            unused.append(n)
        unused.sort()
        sent.clear()

    def arrived(dst, rsem, row, col):
        pltpu.make_async_remote_copy(
            src_ref=dst, dst_ref=dst, send_sem=ssem.at[0], recv_sem=rsem,
            device_id=dev(row, col), device_id_type=MESH,
        ).wait_recv()

    loads = {}

    def load(name, n, src, dst):
        cp = pltpu.make_async_copy(src, dst, lsem.at[n])
        cp.start()
        loads[name] = cp

    for q in range(NQ):
        rows = pl.ds(q * qrows, qrows)
        load(("qr", q), 1 + q, qr_hbm.at[rows], racc.at[rows])
        if q == 0:
            load("g", 0, g_hbm, grow.at[z])
            load("ql", 5, ql_hbm, qlf)
    load("m", 6, m_hbm, mbuf)
    load("v", 7, v_hbm, vbuf)
    load("w", 8, w_hbm, wbuf)
    load("l", 9, l_hbm, lbuf)

    barrier = pltpu.get_barrier_semaphore()
    for row in (sib, opp, dia):
        pl.semaphore_signal(barrier, inc=1, device_id=dev(row, z), device_id_type=MESH)

    @pl.when(z > 0)
    def _():
        pl.semaphore_signal(barrier, inc=1, device_id=dev(i, z - 1), device_id_type=MESH)

    @pl.when(z < NDEV - 1)
    def _():
        pl.semaphore_signal(barrier, inc=1, device_id=dev(i, z + 1), device_id_type=MESH)

    def qr_cast(q):
        rows = pl.ds(q * qrows, qrows)
        loads[("qr", q)].wait()
        qrc[i, rows] = racc[rows].astype(BF16)

    qr_cast(0)
    inner = jnp.logical_and(z > 0, z < NDEV - 1)

    @pl.when(inner)
    def _():
        pl.semaphore_wait(barrier, 5)

    @pl.when(jnp.logical_not(inner))
    def _():
        pl.semaphore_wait(barrier, 4)

    def line_own(buf, rs, held=None):
        send(lambda: buf.at[z], lambda: buf.at[z], lambda: rs.at[z], i, z + 1, z < NDEV - 1, held)
        send(lambda: buf.at[z], lambda: buf.at[z], lambda: rs.at[z], i, z - 1, z > 0, held)

    def line_forward(buf, rs, s, held=None):
        right = jnp.logical_and(z >= s, z < NDEV - 1)
        left = jnp.logical_and(z + s < NDEV, z > 0)

        @pl.when(right)
        def _():
            arrived(buf.at[z - s], rs.at[z - s], i, z - 1)

        send(lambda: buf.at[z - s], lambda: buf.at[z - s], lambda: rs.at[z - s], i, z + 1, right, held)

        @pl.when(left)
        def _():
            arrived(buf.at[z + s], rs.at[z + s], i, z + 1)

        send(lambda: buf.at[z + s], lambda: buf.at[z + s], lambda: rs.at[z + s], i, z - 1, left, held)

    def line_last(buf, rs, s):
        @pl.when(jnp.logical_and(z >= s, z == NDEV - 1))
        def _():
            arrived(buf.at[z - s], rs.at[z - s], i, z - 1)

        @pl.when(jnp.logical_and(z + s < NDEV, z == 0))
        def _():
            arrived(buf.at[z + s], rs.at[z + s], i, z + 1)

    def qr_own(q):
        rows = pl.ds(q * qrows, qrows)
        for row in (opp, sib):
            send(lambda: qrc.at[i, rows], lambda: qrc.at[i, rows], lambda: r_qr.at[i, q], row, z, held=qr_waits)

    qr_own(0)
    loads["g"].wait()
    gbf[z] = grow[z].astype(BF16)
    line_own(gbf, r_gbf)
    loads["ql"].wait()
    qlr[z] = qlf[...].astype(BF16)
    qr_cast(1)
    line_own(qlr, r_qlr)
    for q in range(2, NQ):
        qr_cast(q)
        qr_own(q - 1)
    load("r", 10, r_hbm, racc)

    def qr_forward(q):
        rows = pl.ds(q * qrows, qrows)
        arrived(qrc.at[opp, rows], r_qr.at[opp, q], opp, z)
        send(lambda: qrc.at[opp, rows], lambda: qrc.at[opp, rows], lambda: r_qr.at[opp, q], sib, z, held=qr_waits)

    def h_add(k, q, first=False):
        rows = pl.ds(q * qrows, qrows)
        part = jnp.dot(gbf[k, :, rows], qrc[k, rows], preferred_element_type=F32)
        if first:
            hacc[...] = part
        else:
            hacc[...] += part

    qr_own(NQ - 1)

    line_forward(gbf, r_gbf, 1)
    line_forward(qlr, r_qlr, 1)
    qr_forward(0)
    line_forward(gbf, r_gbf, 2)
    line_forward(qlr, r_qlr, 2)
    line_own(grow, r_g32, line_waits)
    qr_forward(1)
    for s in range(1, NDEV):
        line_last(gbf, r_gbf, s)
        line_last(qlr, r_qlr, s)

    for row in (opp, dia, sib):
        send(lambda row=row: qlr.at[row], lambda: qlc.at[i], lambda: r_qlc.at[i], row, z)
    qlc[i] = qlr[i]

    for q in range(NQ):
        h_add(i, q, first=q == 0)
    for q in range(NQ):
        rows = pl.ds(q * qrows, qrows)
        arrived(qrc.at[sib, rows], r_qr.at[sib, q], sib, z)
        h_add(sib, q)
    qr_forward(2)
    for q in range(2):
        h_add(opp, q)
    for q in range(2):
        rows = pl.ds(q * qrows, qrows)
        arrived(qrc.at[dia, rows], r_qr.at[dia, q], sib, z)
        h_add(dia, q)
    h_add(opp, 2)
    qr_forward(3)
    h_add(opp, 3)
    for q in range(2, NQ):
        rows = pl.ds(q * qrows, qrows)
        arrived(qrc.at[dia, rows], r_qr.at[dia, q], sib, z)
        h_add(dia, q)

    def own_part(buf, rs, n):
        cols = pl.ds(n * hcols, hcols)
        for row in (opp, sib):
            send(lambda: buf.at[i, :, cols], lambda: buf.at[i, :, cols], lambda: rs.at[i, n], row, z)

    def forward_part(buf, rs, n):
        cols = pl.ds(n * hcols, hcols)
        arrived(buf.at[opp, :, cols], rs.at[opp, n], opp, z)
        send(lambda: buf.at[opp, :, cols], lambda: buf.at[opp, :, cols], lambda: rs.at[opp, n], sib, z)

    def rest_part(buf, rs, n):
        cols = pl.ds(n * hcols, hcols)
        arrived(buf.at[sib, :, cols], rs.at[sib, n], sib, z)
        arrived(buf.at[dia, :, cols], rs.at[dia, n], sib, z)

    hcol[i] = hacc[...].astype(BF16)
    for n in range(NH):
        own_part(hcol, r_h, n)

    half = pl.ds(pl.multiple_of(c * (tc // 2), tc // 2), tc // 2)
    other_half = pl.ds(pl.multiple_of((1 - c) * (tc // 2), tc // 2), tc // 2)
    send(lambda: qrc.at[1, half], lambda: qrx.at[half], lambda: r_qx.at[0], i, 1, z == 0, held=qr_waits)
    send(lambda: qrc.at[2, half], lambda: qrx.at[half], lambda: r_qx.at[0], i, 2, z == 3, held=qr_waits)

    early_waits = waits[:]
    waits.clear()

    line_forward(grow, r_g32, 1, line_waits)
    for row in (opp, dia, sib):
        arrived(qlc.at[row], r_qlc.at[row], row, z)
    loads["m"].wait()
    loads["v"].wait()

    for n in range(NH):
        cols = pl.ds(n * hcols, hcols)
        forward_part(hcol, r_h, n)
        rest_part(hcol, r_h, n)
        rotated = sum(
            lax.dot_general(qlc[k], hcol[k, :, cols], ROWS_T, preferred_element_type=F32) for k in range(NDEV)
        )
        hacc[:, cols] = rotated
        rotated = hacc[:, cols]
        new_first = BETA1 * mbuf[:, cols] + (1.0 - BETA1) * rotated
        new_second = BETA2 * vbuf[:, cols] + (1.0 - BETA2) * rotated * rotated
        mbuf[:, cols] = new_first
        vbuf[:, cols] = new_second
        direction = (new_first / BIAS_ONE) / (jnp.sqrt(new_second / BIAS_TWO) + EPS)
        ncol[i, :, cols] = direction.astype(BF16)
        own_part(ncol, r_n, n)
    def gj_part(src, slot, late):
        cols = pl.ds(early, tc - early) if late else pl.ds(0, early)
        n = slot + 2 * late
        return (lambda: src.at[:, cols]), (lambda: gj.at[slot, :, cols]), (lambda: r_gj.at[n])

    head = gparts[0]
    ahead = 1 - 2 * y

    def relay(station, came_row, came_col):
        @pl.when(z == station)
        def _():
            arrived(gi.at[opp, head], r_gi.at[opp, 0], came_row, came_col)

        send(lambda: gi.at[opp, head], lambda: gi.at[opp, head], lambda: r_gi.at[opp, 0], i, z + ahead, z == station)

    send(lambda: grow.at[opp, head], lambda: gi.at[i, head], lambda: r_gi.at[i, 0], opp, z, z == 2 - y)

    calm = y == z // 2
    dup = i == z
    send(*gj_part(grow.at[z], 1, False), opp, z)
    send(*gj_part(grow.at[z], 1, True), opp, z, jnp.logical_not(calm))
    send(lambda: grow.at[z], lambda: gj.at[0], lambda: r_gj.at[0], sib, z)

    def gi_send(b, valid):
        there = jnp.logical_and(valid, b != i)
        for n, rows in enumerate(gparts):
            cond = jnp.logical_and(there, jnp.logical_or(b != opp, z == 3 - 3 * y)) if n == 0 else there
            send(lambda: grow.at[b, rows], lambda: gi.at[i, rows], lambda: r_gi.at[i, n], b, z, cond)

    line_last(grow, r_g32, 1)
    gi_send(z - 1, z >= 1)
    gi_send(z + 1, z + 1 < NDEV)

    for n in range(NH):
        forward_part(ncol, r_n, n)
        rest_part(ncol, r_n, n)
        cols = pl.ds(n * hcols, hcols)
        kb[:, cols] = sum(
            jnp.dot(qlr[k], ncol[k, :, cols], preferred_element_type=F32) for k in range(NDEV)
        ).astype(BF16)

    settle(early_waits)

    def u_send(a, h, slot, col, cond):
        rows = pl.ds(h * urows, urows)
        send(lambda: ubuf.at[a, rows], lambda: urecv.at[slot, rows], lambda: r_u.at[slot, h], i, col, cond)

    def u_first(a, to_right):
        for h in range(NU):
            if to_right:
                u_send(a, h, a, z + 1, z == 0)
            else:
                u_send(a, h, NDEV if a == NDEV - 2 else a, z - 1, z == NDEV - 1)

    for piece, starts in ((3, ((3, True),)), (0, ((0, False),)), (2, ((2, True),)), (1, ((1, False),))):
        ubuf[piece] = lax.dot_general(kb[...], qrc[piece], COLS_T, preferred_element_type=F32)
        for a, to_right in starts:
            u_first(a, to_right)
    send(lambda: kb, lambda: kx, lambda: r_qx.at[2], i, 1, z == 0)
    send(lambda: kb, lambda: kx, lambda: r_qx.at[2], i, 2, z == 3)
    line_forward(grow, r_g32, 2, line_waits)

    relay(1 + y, opp, z)

    @pl.when(inner)
    def _():
        arrived(qrx.at[half], r_qx.at[0], i, 3 * (z // 2))

    send(lambda: qrx.at[half], lambda: qrx.at[half], lambda: r_qx.at[1], sib, z, inner)

    def u_at(a, h, station, to_right):
        rows = pl.ds(h * urows, urows)
        slot = NDEV if (not to_right and station == a) else a

        @pl.when(z == station)
        def _():
            arrived(urecv.at[slot, rows], r_u.at[slot, h], i, station - 1 if to_right else station + 1)
            ubuf[a, rows] += urecv[slot, rows]

        if station != a:
            nxt = station + 1 if to_right else station - 1
            nslot = NDEV if (not to_right and nxt == a) else a
            u_send(a, h, nslot, nxt, z == station)

    line_last(grow, r_g32, 2)
    gi_send(z - 2, z >= 2)
    gi_send(z + 2, z + 2 < NDEV)
    far = jnp.logical_or(jnp.logical_and(z == 0, i == 3), jnp.logical_and(z == 3, i == 0))

    def u_round(t):
        for h in range(NU):
            for a in (3, 2, 1):
                st = t - (3 - a)
                if 1 <= st <= a and a > 1:
                    u_at(a, h, st, True)
                    u_at(NDEV - 1 - a, h, NDEV - 1 - st, False)

    def gj_split(slot, ref, start=0, size=None):
        cols = pl.ds(start, size or tc)
        for t, term in enumerate(split3(ref[:, cols])):
            qrc[slot, pl.ds(t * tr, tr), cols] = term

    def gi_split(k, ref, n):
        rows = pl.ds(n * grows, grows)
        for t, term in enumerate(split3(ref[rows])):
            gis[k, t, rows] = term

    def right_add(k, slot, n=None, start=0, size=None, first=False, turned=None):
        begin, depth = (0, tr) if n is None else (n * grows, grows)
        cols = pl.ds(start, size or tc)

        def body(m, carry):
            rows = pl.ds(pl.multiple_of(m * tr, tr), tr)
            if turned is None:
                a0, a1, a2 = [gis[k, t, pl.ds(begin, depth), rows].T for t in range(3)]
            else:
                a0, a1, a2 = [git[turned, rows, pl.ds(t * tr + begin, depth)] for t in range(3)]
            b0, b1, b2 = [qrc[slot, pl.ds(t * tr + begin, depth), cols] for t in range(3)]
            left = jnp.concatenate([a0, a0, a0, a1, a1, a2], axis=1)
            right = jnp.concatenate([b0, b1, b2, b0, b1, b0], axis=0)
            share = (1.0 - BETA2) * jnp.dot(left, right, preferred_element_type=F32)
            old = racc[rows, cols]
            racc[rows, cols] = (BETA2 * old if first else old) + share
            return carry

        lax.fori_loop(0, tc // tr, body, 0)

    def gi_arrived(row, n, slot, turned=None):
        @pl.when(jnp.logical_not(dup))
        def _():
            if n == 1:
                arrived(gi.at[row, gparts[2]], r_gi.at[row, 2], row, z)
            else:
                arrived(gi.at[row, gparts[1]], r_gi.at[row, 1], row, z)
                if row is opp:
                    @pl.when(z == 3 * y)
                    def _():
                        arrived(gi.at[row, head], r_gi.at[row, 0], row, z)

                    @pl.when(z == 3 - 3 * y)
                    def _():
                        arrived(gi.at[row, head], r_gi.at[row, 0], i, z - ahead)
                else:
                    arrived(gi.at[row, head], r_gi.at[row, 0], row, z)
            gi_split(row, gi.at[row], n)

        @pl.when(dup)
        def _():
            gi_split(row, gj.at[slot], n)

        if turned is not None:
            for t in range(3):
                git[turned, :, pl.ds(t * tr + n * grows, grows)] = gis[row, t, pl.ds(n * grows, grows)].T

    def left_part(k, slot):
        pieces = [gis[k, t] for t in range(3)]
        other = [gis[z, t] for t in range(3)]
        total = None
        for t, u in ((0, 0), (0, 1), (1, 0), (1, 1), (0, 2), (2, 0)):
            d = lax.dot_general(pieces[t], other[u], COLS_T, preferred_element_type=F32)
            total = d if total is None else total + d
        lx[slot] = total

    settle(qr_waits)
    gj_split(0, grow.at[z])
    arrived(gj.at[0], r_gj.at[0], sib, z)
    gj_split(1, gj.at[0])
    loads["r"].wait()

    def chip_rows():
        for n in range(NG):
            gi_split(i, grow.at[i], n)
        right_add(i, 0, first=True)
        for n in range(NG):
            gi_arrived(sib, n, 0)
        right_add(sib, 1)

    pl.when(jnp.logical_not(far))(chip_rows)
    arrived(gj.at[1, :, pl.ds(0, early)], r_gj.at[1], opp, z)
    send(*gj_part(gj.at[1], 2, False), sib, z)
    relay(2 - y, i, z - ahead)
    gj_split(2, gj.at[1], 0, early)

    def gj_late_arrived():
        arrived(gj.at[1, :, pl.ds(early, tc - early)], r_gj.at[3], opp, z)

    pl.when(calm)(gj_late_arrived)
    send(*gj_part(gj.at[1], 2, True), sib, z, calm)

    @pl.when(calm)
    def _():
        gj_split(2, gj.at[1], early, tc - early)
    u_round(1)
    line_last(grow, r_g32, 3)
    gi_send(z - 3, z >= 3)
    gi_send(z + 3, z + 3 < NDEV)
    send(*gj_part(grow.at[z], 1, True), opp, z, calm, held=late_waits)
    arrived(gj.at[2, :, pl.ds(0, early)], r_gj.at[2], sib, z)
    gj_split(3, gj.at[2], 0, early)

    def gj_last_arrived():
        arrived(gj.at[2, :, pl.ds(early, tc - early)], r_gj.at[4], sib, z)
        gj_split(3, gj.at[2], early, tc - early)

    pl.when(calm)(gj_last_arrived)
    pl.when(far)(chip_rows)
    u_round(2)
    for n in range(NG - 1):
        gi_arrived(opp, n, 1, 0)
        right_add(opp, 2, n, 0, early, turned=0)
        gi_arrived(dia, n, 2, 1)
        right_add(dia, 3, n, 0, early, turned=1)

    loads["w"].wait()
    loads["l"].wait()
    gi_arrived(dia, NG - 1, 2, 1)
    gi_arrived(opp, NG - 1, 1, 0)

    left_part(dia, 3)
    send(lambda: lx.at[3], lambda: lrecv.at[2], lambda: r_l.at[2], sib, z)
    left_part(opp, 2)
    left_part(sib, 1)
    send(lambda: lx.at[1], lambda: lrecv.at[0], lambda: r_l.at[0], sib, z)
    arrived(lrecv.at[2], r_l.at[2], sib, z)
    lx[2] += lrecv[2]
    send(lambda: lx.at[2], lambda: lrecv.at[1], lambda: r_l.at[1], opp, z, held=late_waits)
    left_part(i, 0)
    right_add(opp, 2, NG - 1, 0, early, turned=0)
    pl.when(jnp.logical_not(calm))(gj_late_arrived)
    send(*gj_part(gj.at[1], 2, True), sib, z, jnp.logical_not(calm), held=late_waits)
    right_add(dia, 3, NG - 1, 0, early, turned=1)

    @pl.when(jnp.logical_not(calm))
    def _():
        gj_split(2, gj.at[1], early, tc - early)

    right_add(opp, 2, None, early, tc - early, turned=0)

    @pl.when(inner)
    def _():
        arrived(qrx.at[other_half], r_qx.at[1], sib, z)
        arrived(kx, r_qx.at[2], i, 3 * (z // 2))
        ubuf[z] += lax.dot_general(kx[...], qrx[...], COLS_T, preferred_element_type=F32)

    u_round(3)
    wbuf[...] = wbuf[...] - LR * ubuf[z]
    settle(waits)
    settle(line_waits)
    pl.when(jnp.logical_not(calm))(gj_last_arrived)
    right_add(dia, 3, None, early, tc - early, turned=1)
    arrived(lrecv.at[0], r_l.at[0], sib, z)
    left_sum = lx[0] + lrecv[0]
    arrived(lrecv.at[1], r_l.at[1], opp, z)
    left_sum += lrecv[1]
    lbuf[...] = BETA2 * lbuf[...] + (1.0 - BETA2) * left_sum

    settle(waits)
    settle(late_waits)
    assert most[0] == NSEND, most[0]


def write_out(*refs):
    ins, outs, sem = refs[:5], refs[5:10], refs[10]
    copies = []
    for a, b in zip(ins, outs):
        step = a.shape[0] // 4
        for n in range(4):
            rows = pl.ds(n * step, step)
            copies.append(pltpu.make_async_copy(a.at[rows], b.at[rows], sem.at[len(copies)]))
    for cp in copies:
        cp.start()
    for cp in copies:
        cp.wait()


def solution(mesh):
    tile_spec = P(("layer", "row"), "col")

    def local_step(weight, grad_in, mom_first, mom_second, stat_left, stat_right, basis_left, basis_right):
        tr, tc = grad_in.shape
        tl = stat_left.shape[0]
        dma = pltpu.SemaphoreType.DMA
        scratch = [
            pltpu.VMEM((4, tr, tc), F32),
            pltpu.VMEM((4, tr, tc), BF16),
            pltpu.VMEM((4, tr, tc), F32),
            pltpu.VMEM((3, tr, tc), F32),
            pltpu.VMEM((4, tc, tc), BF16),
            pltpu.VMEM((4, tr, tc), BF16),
            pltpu.VMEM((4, tr, tc), BF16),
            pltpu.VMEM((4, 3, tr, tc), BF16),
            pltpu.VMEM((4, tr, tc), F32),
            pltpu.VMEM((5, tr, tc), F32),
            pltpu.VMEM((4, tl, tl), BF16),
            pltpu.VMEM((4, tl, tl), BF16),
            pltpu.VMEM((tr, tc), F32),
            pltpu.VMEM((tr, tc), BF16),
            pltpu.VMEM((tc, tc), BF16),
            pltpu.VMEM((tr, tc), BF16),
            pltpu.VMEM((tl, tl), F32),
            pltpu.VMEM((4, tl, tl), F32),
            pltpu.VMEM((3, tl, tl), F32),
            pltpu.VMEM((2, tc, 3 * tr), BF16),
            dma((NSEND,)),
            dma((11,)),
            dma((4,)), dma((4,)), dma((4,)),
            dma((4, NQ)), dma((4,)),
            dma((4, NH)), dma((4, NH)),
            dma((5,)), dma((4, 3)),
            dma((5, NU)), dma((3,)), dma((3,)),
        ]
        any_spec = pl.BlockSpec(memory_space=pl.ANY)
        vmem_spec = pl.BlockSpec(memory_space=pltpu.VMEM)
        outs = [weight, mom_first, mom_second, stat_left, stat_right]
        results = pl.pallas_call(
            kernel,
            name="soap_step",
            out_shape=[pltpu.VMEM(o.shape, o.dtype) for o in outs],
            in_specs=[any_spec] * 8,
            out_specs=[vmem_spec] * 5,
            scratch_shapes=scratch,
            compiler_params=pltpu.CompilerParams(
                collective_id=0, has_side_effects=True, vmem_limit_bytes=VMEM_BYTES,
            ),
        )(weight, grad_in, mom_first, mom_second, stat_left, stat_right, basis_left, basis_right)
        results = [pltpu.with_memory_space_constraint(r, pltpu.VMEM) for r in results]
        return pl.pallas_call(
            write_out,
            name="write_out",
            out_shape=[jax.ShapeDtypeStruct(o.shape, o.dtype) for o in outs],
            in_specs=[vmem_spec] * 5,
            out_specs=[any_spec] * 5,
            scratch_shapes=[dma((20,))],
            compiler_params=pltpu.CompilerParams(vmem_limit_bytes=2**20),
        )(*results)

    return jax.shard_map(local_step, mesh=mesh, in_specs=(tile_spec,) * 8, out_specs=(tile_spec,) * 5, check_vma=False)
```

```python
import jax
import jax.numpy as jnp
from jax import lax
from jax.experimental import pallas as pl
from jax.experimental.pallas import tpu as pltpu
from jax.sharding import PartitionSpec as P

BETA1 = 0.9
BETA2 = 0.9
EPS = 1e-8
LR = 0.1
STEP = 10
BIAS_ONE = 1.0 - BETA1 ** STEP
BIAS_TWO = 1.0 - BETA2 ** STEP

MESH = pl.DeviceIdType.MESH
F32 = jnp.float32
BF16 = jnp.bfloat16
NQ = 4
NH = 2
NU = 2
NG = 2
NDEV = 4
NSEND = 68
VMEM_BYTES = 56 * 2**20

ROWS_T = (((0,), (0,)), ((), ()))
COLS_T = (((1,), (1,)), ((), ()))


def split3(x):
    a0 = x.astype(BF16)
    r = x - a0.astype(F32)
    a1 = r.astype(BF16)
    a2 = (r - a1.astype(F32)).astype(BF16)
    return a0, a1, a2


def kernel(
    w_hbm, g_hbm, m_hbm, v_hbm, l_hbm, r_hbm, ql_hbm, qr_hbm,
    wbuf, mbuf, vbuf, lbuf, racc,
    grow, gbf, gi, gj, qrc, hcol, ncol, gis, ubuf, urecv,
    qlr, qlc, hacc, kb, qrx, kx, qlf, lx, lrecv, git,
    ssem, lsem, r_gbf, r_qlr, r_g32, r_qr, r_qlc, r_h, r_n, r_gj, r_gi, r_u, r_qx, r_l,
):
    lay = lax.axis_index("layer")
    z = lax.axis_index("col")
    i = lax.axis_index("row")
    y, c = i // 2, i % 2
    sib = 2 * y + (1 - c)
    opp = 2 * (1 - y) + c
    dia = 2 * (1 - y) + (1 - c)
    tr, tc = grow.shape[1], grow.shape[2]
    qrows = tc // NQ
    hcols = tc // NH
    urows = tr // NU
    grows = tr // NG
    head_rows = 3 * grows // 4
    gparts = (pl.ds(0, head_rows), pl.ds(head_rows, grows - head_rows), pl.ds(grows, grows))
    early = tc - tc // 4

    waits, qr_waits, late_waits, line_waits = [], [], [], []
    unused, most = list(range(NSEND)), [0]

    def dev(row, col):
        return (lay, col, row)

    def send(src, dst, rsem, row, col, cond=None, held=None):
        src, dst, rsem = src(), dst(), rsem()
        n = unused.pop(0)
        most[0] = max(most[0], n + 1)

        def make():
            return pltpu.make_async_remote_copy(
                src_ref=src, dst_ref=dst, send_sem=ssem.at[n], recv_sem=rsem,
                device_id=dev(row, col), device_id_type=MESH,
            )

        def go():
            make().start()

        def done():
            make().wait_send()

        if cond is None:
            go()
        else:
            pl.when(cond)(go)
        if held is None:
            waits.append((cond, done, n))
        else:
            held.append((cond, done, n))

    def settle(sent):
        for cond, done, n in sent:
            if cond is None:
                done()
            else:
                pl.when(cond)(done)
            unused.append(n)
        unused.sort()
        sent.clear()

    def arrived(dst, rsem, row, col):
        pltpu.make_async_remote_copy(
            src_ref=dst, dst_ref=dst, send_sem=ssem.at[0], recv_sem=rsem,
            device_id=dev(row, col), device_id_type=MESH,
        ).wait_recv()

    loads = {}

    def load(name, n, src, dst):
        cp = pltpu.make_async_copy(src, dst, lsem.at[n])
        cp.start()
        loads[name] = cp

    for q in range(NQ):
        rows = pl.ds(q * qrows, qrows)
        load(("qr", q), 1 + q, qr_hbm.at[rows], racc.at[rows])
        if q == 0:
            load("g", 0, g_hbm, grow.at[z])
            load("ql", 5, ql_hbm, qlf)
    load("m", 6, m_hbm, mbuf)
    load("v", 7, v_hbm, vbuf)
    load("w", 8, w_hbm, wbuf)
    load("l", 9, l_hbm, lbuf)

    barrier = pltpu.get_barrier_semaphore()
    for row in (sib, opp, dia):
        pl.semaphore_signal(barrier, inc=1, device_id=dev(row, z), device_id_type=MESH)

    @pl.when(z > 0)
    def _():
        pl.semaphore_signal(barrier, inc=1, device_id=dev(i, z - 1), device_id_type=MESH)

    @pl.when(z < NDEV - 1)
    def _():
        pl.semaphore_signal(barrier, inc=1, device_id=dev(i, z + 1), device_id_type=MESH)

    def qr_cast(q):
        rows = pl.ds(q * qrows, qrows)
        loads[("qr", q)].wait()
        qrc[i, rows] = racc[rows].astype(BF16)

    qr_cast(0)
    inner = jnp.logical_and(z > 0, z < NDEV - 1)

    @pl.when(inner)
    def _():
        pl.semaphore_wait(barrier, 5)

    @pl.when(jnp.logical_not(inner))
    def _():
        pl.semaphore_wait(barrier, 4)

    def line_own(buf, rs, held=None):
        send(lambda: buf.at[z], lambda: buf.at[z], lambda: rs.at[z], i, z + 1, z < NDEV - 1, held)
        send(lambda: buf.at[z], lambda: buf.at[z], lambda: rs.at[z], i, z - 1, z > 0, held)

    def line_forward(buf, rs, s, held=None):
        right = jnp.logical_and(z >= s, z < NDEV - 1)
        left = jnp.logical_and(z + s < NDEV, z > 0)

        @pl.when(right)
        def _():
            arrived(buf.at[z - s], rs.at[z - s], i, z - 1)

        send(lambda: buf.at[z - s], lambda: buf.at[z - s], lambda: rs.at[z - s], i, z + 1, right, held)

        @pl.when(left)
        def _():
            arrived(buf.at[z + s], rs.at[z + s], i, z + 1)

        send(lambda: buf.at[z + s], lambda: buf.at[z + s], lambda: rs.at[z + s], i, z - 1, left, held)

    def line_last(buf, rs, s):
        @pl.when(jnp.logical_and(z >= s, z == NDEV - 1))
        def _():
            arrived(buf.at[z - s], rs.at[z - s], i, z - 1)

        @pl.when(jnp.logical_and(z + s < NDEV, z == 0))
        def _():
            arrived(buf.at[z + s], rs.at[z + s], i, z + 1)

    def qr_own(q):
        rows = pl.ds(q * qrows, qrows)
        for row in (opp, sib):
            send(lambda: qrc.at[i, rows], lambda: qrc.at[i, rows], lambda: r_qr.at[i, q], row, z, held=qr_waits)

    qr_own(0)
    loads["g"].wait()
    gbf[z] = grow[z].astype(BF16)
    line_own(gbf, r_gbf)
    loads["ql"].wait()
    qlr[z] = qlf[...].astype(BF16)
    qr_cast(1)
    line_own(qlr, r_qlr)
    for q in range(2, NQ):
        qr_cast(q)
        qr_own(q - 1)
    load("r", 10, r_hbm, racc)

    def qr_forward(q):
        rows = pl.ds(q * qrows, qrows)
        arrived(qrc.at[opp, rows], r_qr.at[opp, q], opp, z)
        send(lambda: qrc.at[opp, rows], lambda: qrc.at[opp, rows], lambda: r_qr.at[opp, q], sib, z, held=qr_waits)

    def h_add(k, q, first=False):
        rows = pl.ds(q * qrows, qrows)
        part = jnp.dot(gbf[k, :, rows], qrc[k, rows], preferred_element_type=F32)
        if first:
            hacc[...] = part
        else:
            hacc[...] += part

    qr_own(NQ - 1)

    line_forward(gbf, r_gbf, 1)
    line_forward(qlr, r_qlr, 1)
    qr_forward(0)
    line_forward(gbf, r_gbf, 2)
    line_forward(qlr, r_qlr, 2)
    line_own(grow, r_g32, line_waits)
    qr_forward(1)
    for s in range(1, NDEV):
        line_last(gbf, r_gbf, s)
        line_last(qlr, r_qlr, s)

    for row in (opp, dia, sib):
        send(lambda row=row: qlr.at[row], lambda: qlc.at[i], lambda: r_qlc.at[i], row, z)
    qlc[i] = qlr[i]

    for q in range(NQ):
        h_add(i, q, first=q == 0)
    for q in range(NQ):
        rows = pl.ds(q * qrows, qrows)
        arrived(qrc.at[sib, rows], r_qr.at[sib, q], sib, z)
        h_add(sib, q)
    qr_forward(2)
    for q in range(2):
        h_add(opp, q)
    for q in range(2):
        rows = pl.ds(q * qrows, qrows)
        arrived(qrc.at[dia, rows], r_qr.at[dia, q], sib, z)
        h_add(dia, q)
    h_add(opp, 2)
    qr_forward(3)
    h_add(opp, 3)
    for q in range(2, NQ):
        rows = pl.ds(q * qrows, qrows)
        arrived(qrc.at[dia, rows], r_qr.at[dia, q], sib, z)
        h_add(dia, q)

    def own_part(buf, rs, n):
        cols = pl.ds(n * hcols, hcols)
        for row in (opp, sib):
            send(lambda: buf.at[i, :, cols], lambda: buf.at[i, :, cols], lambda: rs.at[i, n], row, z)

    def forward_part(buf, rs, n):
        cols = pl.ds(n * hcols, hcols)
        arrived(buf.at[opp, :, cols], rs.at[opp, n], opp, z)
        send(lambda: buf.at[opp, :, cols], lambda: buf.at[opp, :, cols], lambda: rs.at[opp, n], sib, z)

    def rest_part(buf, rs, n):
        cols = pl.ds(n * hcols, hcols)
        arrived(buf.at[sib, :, cols], rs.at[sib, n], sib, z)
        arrived(buf.at[dia, :, cols], rs.at[dia, n], sib, z)

    hcol[i] = hacc[...].astype(BF16)
    for n in range(NH):
        own_part(hcol, r_h, n)

    half = pl.ds(pl.multiple_of(c * (tc // 2), tc // 2), tc // 2)
    other_half = pl.ds(pl.multiple_of((1 - c) * (tc // 2), tc // 2), tc // 2)
    send(lambda: qrc.at[1, half], lambda: qrx.at[half], lambda: r_qx.at[0], i, 1, z == 0, held=qr_waits)
    send(lambda: qrc.at[2, half], lambda: qrx.at[half], lambda: r_qx.at[0], i, 2, z == 3, held=qr_waits)

    early_waits = waits[:]
    waits.clear()

    line_forward(grow, r_g32, 1, line_waits)
    for row in (opp, dia, sib):
        arrived(qlc.at[row], r_qlc.at[row], row, z)
    loads["m"].wait()
    loads["v"].wait()

    for n in range(NH):
        cols = pl.ds(n * hcols, hcols)
        forward_part(hcol, r_h, n)
        rest_part(hcol, r_h, n)
        rotated = sum(
            lax.dot_general(qlc[k], hcol[k, :, cols], ROWS_T, preferred_element_type=F32) for k in range(NDEV)
        )
        hacc[:, cols] = rotated
        rotated = hacc[:, cols]
        new_first = BETA1 * mbuf[:, cols] + (1.0 - BETA1) * rotated
        new_second = BETA2 * vbuf[:, cols] + (1.0 - BETA2) * rotated * rotated
        mbuf[:, cols] = new_first
        vbuf[:, cols] = new_second
        direction = (new_first / BIAS_ONE) / (jnp.sqrt(new_second / BIAS_TWO) + EPS)
        ncol[i, :, cols] = direction.astype(BF16)
        own_part(ncol, r_n, n)
    def gj_part(src, slot, late):
        cols = pl.ds(early, tc - early) if late else pl.ds(0, early)
        n = slot + 2 * late
        return (lambda: src.at[:, cols]), (lambda: gj.at[slot, :, cols]), (lambda: r_gj.at[n])

    head = gparts[0]
    ahead = 1 - 2 * y

    def relay(station, came_row, came_col):
        @pl.when(z == station)
        def _():
            arrived(gi.at[opp, head], r_gi.at[opp, 0], came_row, came_col)

        send(lambda: gi.at[opp, head], lambda: gi.at[opp, head], lambda: r_gi.at[opp, 0], i, z + ahead, z == station)

    send(lambda: grow.at[opp, head], lambda: gi.at[i, head], lambda: r_gi.at[i, 0], opp, z, z == 2 - y)

    calm = y == z // 2
    dup = i == z
    send(*gj_part(grow.at[z], 1, False), opp, z)
    send(*gj_part(grow.at[z], 1, True), opp, z, jnp.logical_not(calm))
    send(lambda: grow.at[z], lambda: gj.at[0], lambda: r_gj.at[0], sib, z)

    def gi_send(b, valid):
        there = jnp.logical_and(valid, b != i)
        for n, rows in enumerate(gparts):
            cond = jnp.logical_and(there, jnp.logical_or(b != opp, z == 3 - 3 * y)) if n == 0 else there
            send(lambda: grow.at[b, rows], lambda: gi.at[i, rows], lambda: r_gi.at[i, n], b, z, cond)

    line_last(grow, r_g32, 1)
    gi_send(z - 1, z >= 1)
    gi_send(z + 1, z + 1 < NDEV)

    for n in range(NH):
        forward_part(ncol, r_n, n)
        rest_part(ncol, r_n, n)
        cols = pl.ds(n * hcols, hcols)
        kb[:, cols] = sum(
            jnp.dot(qlr[k], ncol[k, :, cols], preferred_element_type=F32) for k in range(NDEV)
        ).astype(BF16)

    settle(early_waits)

    def u_send(a, h, slot, col, cond):
        rows = pl.ds(h * urows, urows)
        send(lambda: ubuf.at[a, rows], lambda: urecv.at[slot, rows], lambda: r_u.at[slot, h], i, col, cond)

    def u_first(a, to_right):
        for h in range(NU):
            if to_right:
                u_send(a, h, a, z + 1, z == 0)
            else:
                u_send(a, h, NDEV if a == NDEV - 2 else a, z - 1, z == NDEV - 1)

    for piece, starts in ((3, ((3, True),)), (0, ((0, False),)), (2, ((2, True),)), (1, ((1, False),))):
        ubuf[piece] = lax.dot_general(kb[...], qrc[piece], COLS_T, preferred_element_type=F32)
        for a, to_right in starts:
            u_first(a, to_right)
    send(lambda: kb, lambda: kx, lambda: r_qx.at[2], i, 1, z == 0)
    send(lambda: kb, lambda: kx, lambda: r_qx.at[2], i, 2, z == 3)
    line_forward(grow, r_g32, 2, line_waits)

    relay(1 + y, opp, z)

    @pl.when(inner)
    def _():
        arrived(qrx.at[half], r_qx.at[0], i, 3 * (z // 2))

    send(lambda: qrx.at[half], lambda: qrx.at[half], lambda: r_qx.at[1], sib, z, inner)

    def u_at(a, h, station, to_right):
        rows = pl.ds(h * urows, urows)
        slot = NDEV if (not to_right and station == a) else a

        @pl.when(z == station)
        def _():
            arrived(urecv.at[slot, rows], r_u.at[slot, h], i, station - 1 if to_right else station + 1)
            ubuf[a, rows] += urecv[slot, rows]

        if station != a:
            nxt = station + 1 if to_right else station - 1
            nslot = NDEV if (not to_right and nxt == a) else a
            u_send(a, h, nslot, nxt, z == station)

    line_last(grow, r_g32, 2)
    gi_send(z - 2, z >= 2)
    gi_send(z + 2, z + 2 < NDEV)
    far = jnp.logical_or(jnp.logical_and(z == 0, i == 3), jnp.logical_and(z == 3, i == 0))

    def u_round(t):
        for h in range(NU):
            for a in (3, 2, 1):
                st = t - (3 - a)
                if 1 <= st <= a and a > 1:
                    u_at(a, h, st, True)
                    u_at(NDEV - 1 - a, h, NDEV - 1 - st, False)

    def gj_split(slot, ref, start=0, size=None):
        cols = pl.ds(start, size or tc)
        for t, term in enumerate(split3(ref[:, cols])):
            qrc[slot, pl.ds(t * tr, tr), cols] = term

    def gi_split(k, ref, n):
        rows = pl.ds(n * grows, grows)
        for t, term in enumerate(split3(ref[rows])):
            gis[k, t, rows] = term

    def right_add(k, slot, n=None, start=0, size=None, first=False, turned=None):
        begin, depth = (0, tr) if n is None else (n * grows, grows)
        cols = pl.ds(start, size or tc)

        def body(m, carry):
            rows = pl.ds(pl.multiple_of(m * tr, tr), tr)
            if turned is None:
                a0, a1, a2 = [gis[k, t, pl.ds(begin, depth), rows].T for t in range(3)]
            else:
                a0, a1, a2 = [git[turned, rows, pl.ds(t * tr + begin, depth)] for t in range(3)]
            b0, b1, b2 = [qrc[slot, pl.ds(t * tr + begin, depth), cols] for t in range(3)]
            left = jnp.concatenate([a0, a0, a0, a1, a1, a2], axis=1)
            right = jnp.concatenate([b0, b1, b2, b0, b1, b0], axis=0)
            share = (1.0 - BETA2) * jnp.dot(left, right, preferred_element_type=F32)
            old = racc[rows, cols]
            racc[rows, cols] = (BETA2 * old if first else old) + share
            return carry

        lax.fori_loop(0, tc // tr, body, 0)

    def gi_arrived(row, n, slot, turned=None):
        @pl.when(jnp.logical_not(dup))
        def _():
            if n == 1:
                arrived(gi.at[row, gparts[2]], r_gi.at[row, 2], row, z)
            else:
                arrived(gi.at[row, gparts[1]], r_gi.at[row, 1], row, z)
                if row is opp:
                    @pl.when(z == 3 * y)
                    def _():
                        arrived(gi.at[row, head], r_gi.at[row, 0], row, z)

                    @pl.when(z == 3 - 3 * y)
                    def _():
                        arrived(gi.at[row, head], r_gi.at[row, 0], i, z - ahead)
                else:
                    arrived(gi.at[row, head], r_gi.at[row, 0], row, z)
            gi_split(row, gi.at[row], n)

        @pl.when(dup)
        def _():
            gi_split(row, gj.at[slot], n)

        if turned is not None:
            for t in range(3):
                git[turned, :, pl.ds(t * tr + n * grows, grows)] = gis[row, t, pl.ds(n * grows, grows)].T

    def left_part(k, slot):
        pieces = [gis[k, t] for t in range(3)]
        other = [gis[z, t] for t in range(3)]
        total = None
        for t, u in ((0, 0), (0, 1), (1, 0), (1, 1), (0, 2), (2, 0)):
            d = lax.dot_general(pieces[t], other[u], COLS_T, preferred_element_type=F32)
            total = d if total is None else total + d
        lx[slot] = total

    settle(qr_waits)
    gj_split(0, grow.at[z])
    arrived(gj.at[0], r_gj.at[0], sib, z)
    gj_split(1, gj.at[0])
    loads["r"].wait()

    def chip_rows():
        for n in range(NG):
            gi_split(i, grow.at[i], n)
        right_add(i, 0, first=True)
        for n in range(NG):
            gi_arrived(sib, n, 0)
        right_add(sib, 1)

    pl.when(jnp.logical_not(far))(chip_rows)
    arrived(gj.at[1, :, pl.ds(0, early)], r_gj.at[1], opp, z)
    send(*gj_part(gj.at[1], 2, False), sib, z)
    relay(2 - y, i, z - ahead)
    gj_split(2, gj.at[1], 0, early)

    def gj_late_arrived():
        arrived(gj.at[1, :, pl.ds(early, tc - early)], r_gj.at[3], opp, z)

    u_round(1)
    line_last(grow, r_g32, 3)
    gi_send(z - 3, z >= 3)
    gi_send(z + 3, z + 3 < NDEV)
    send(*gj_part(grow.at[z], 1, True), opp, z, calm, held=late_waits)
    pl.when(calm)(gj_late_arrived)
    send(*gj_part(gj.at[1], 2, True), sib, z, calm)

    @pl.when(calm)
    def _():
        gj_split(2, gj.at[1], early, tc - early)

    arrived(gj.at[2, :, pl.ds(0, early)], r_gj.at[2], sib, z)
    gj_split(3, gj.at[2], 0, early)

    def gj_last_arrived():
        arrived(gj.at[2, :, pl.ds(early, tc - early)], r_gj.at[4], sib, z)
        gj_split(3, gj.at[2], early, tc - early)

    pl.when(calm)(gj_last_arrived)
    pl.when(far)(chip_rows)
    u_round(2)
    for n in range(NG - 1):
        gi_arrived(opp, n, 1, 0)
        right_add(opp, 2, n, 0, early, turned=0)
        gi_arrived(dia, n, 2, 1)
        right_add(dia, 3, n, 0, early, turned=1)

    loads["w"].wait()
    loads["l"].wait()
    gi_arrived(dia, NG - 1, 2, 1)
    gi_arrived(opp, NG - 1, 1, 0)

    left_part(dia, 3)
    send(lambda: lx.at[3], lambda: lrecv.at[2], lambda: r_l.at[2], sib, z)
    left_part(opp, 2)
    left_part(sib, 1)
    send(lambda: lx.at[1], lambda: lrecv.at[0], lambda: r_l.at[0], sib, z)
    arrived(lrecv.at[2], r_l.at[2], sib, z)
    lx[2] += lrecv[2]
    send(lambda: lx.at[2], lambda: lrecv.at[1], lambda: r_l.at[1], opp, z, held=late_waits)
    left_part(i, 0)
    right_add(opp, 2, NG - 1, 0, early, turned=0)
    pl.when(jnp.logical_not(calm))(gj_late_arrived)
    send(*gj_part(gj.at[1], 2, True), sib, z, jnp.logical_not(calm), held=late_waits)
    right_add(dia, 3, NG - 1, 0, early, turned=1)

    @pl.when(jnp.logical_not(calm))
    def _():
        gj_split(2, gj.at[1], early, tc - early)

    right_add(opp, 2, None, early, tc - early, turned=0)

    @pl.when(inner)
    def _():
        arrived(qrx.at[other_half], r_qx.at[1], sib, z)
        arrived(kx, r_qx.at[2], i, 3 * (z // 2))
        ubuf[z] += lax.dot_general(kx[...], qrx[...], COLS_T, preferred_element_type=F32)

    u_round(3)
    wbuf[...] = wbuf[...] - LR * ubuf[z]
    settle(waits)
    settle(line_waits)
    pl.when(jnp.logical_not(calm))(gj_last_arrived)
    right_add(dia, 3, None, early, tc - early, turned=1)
    arrived(lrecv.at[0], r_l.at[0], sib, z)
    left_sum = lx[0] + lrecv[0]
    arrived(lrecv.at[1], r_l.at[1], opp, z)
    left_sum += lrecv[1]
    lbuf[...] = BETA2 * lbuf[...] + (1.0 - BETA2) * left_sum

    settle(waits)
    settle(late_waits)
    assert most[0] == NSEND, most[0]


def write_out(*refs):
    ins, outs, sem = refs[:5], refs[5:10], refs[10]
    copies = []
    for a, b in zip(ins, outs):
        step = a.shape[0] // 4
        for n in range(4):
            rows = pl.ds(n * step, step)
            copies.append(pltpu.make_async_copy(a.at[rows], b.at[rows], sem.at[len(copies)]))
    for cp in copies:
        cp.start()
    for cp in copies:
        cp.wait()


def solution(mesh):
    tile_spec = P(("layer", "row"), "col")

    def local_step(weight, grad_in, mom_first, mom_second, stat_left, stat_right, basis_left, basis_right):
        tr, tc = grad_in.shape
        tl = stat_left.shape[0]
        dma = pltpu.SemaphoreType.DMA
        scratch = [
            pltpu.VMEM((4, tr, tc), F32),
            pltpu.VMEM((4, tr, tc), BF16),
            pltpu.VMEM((4, tr, tc), F32),
            pltpu.VMEM((3, tr, tc), F32),
            pltpu.VMEM((4, tc, tc), BF16),
            pltpu.VMEM((4, tr, tc), BF16),
            pltpu.VMEM((4, tr, tc), BF16),
            pltpu.VMEM((4, 3, tr, tc), BF16),
            pltpu.VMEM((4, tr, tc), F32),
            pltpu.VMEM((5, tr, tc), F32),
            pltpu.VMEM((4, tl, tl), BF16),
            pltpu.VMEM((4, tl, tl), BF16),
            pltpu.VMEM((tr, tc), F32),
            pltpu.VMEM((tr, tc), BF16),
            pltpu.VMEM((tc, tc), BF16),
            pltpu.VMEM((tr, tc), BF16),
            pltpu.VMEM((tl, tl), F32),
            pltpu.VMEM((4, tl, tl), F32),
            pltpu.VMEM((3, tl, tl), F32),
            pltpu.VMEM((2, tc, 3 * tr), BF16),
            dma((NSEND,)),
            dma((11,)),
            dma((4,)), dma((4,)), dma((4,)),
            dma((4, NQ)), dma((4,)),
            dma((4, NH)), dma((4, NH)),
            dma((5,)), dma((4, 3)),
            dma((5, NU)), dma((3,)), dma((3,)),
        ]
        any_spec = pl.BlockSpec(memory_space=pl.ANY)
        vmem_spec = pl.BlockSpec(memory_space=pltpu.VMEM)
        outs = [weight, mom_first, mom_second, stat_left, stat_right]
        results = pl.pallas_call(
            kernel,
            name="soap_step",
            out_shape=[pltpu.VMEM(o.shape, o.dtype) for o in outs],
            in_specs=[any_spec] * 8,
            out_specs=[vmem_spec] * 5,
            scratch_shapes=scratch,
            compiler_params=pltpu.CompilerParams(
                collective_id=0, has_side_effects=True, vmem_limit_bytes=VMEM_BYTES,
            ),
        )(weight, grad_in, mom_first, mom_second, stat_left, stat_right, basis_left, basis_right)
        results = [pltpu.with_memory_space_constraint(r, pltpu.VMEM) for r in results]
        return pl.pallas_call(
            write_out,
            name="write_out",
            out_shape=[jax.ShapeDtypeStruct(o.shape, o.dtype) for o in outs],
            in_specs=[vmem_spec] * 5,
            out_specs=[any_spec] * 5,
            scratch_shapes=[dma((20,))],
            compiler_params=pltpu.CompilerParams(vmem_limit_bytes=2**20),
        )(*results)

    return jax.shard_map(local_step, mesh=mesh, in_specs=(tile_spec,) * 8, out_specs=(tile_spec,) * 5, check_vma=False)
```

```python
import jax
import jax.numpy as jnp
from jax import lax
from jax.experimental import pallas as pl
from jax.experimental.pallas import tpu as pltpu
from jax.sharding import PartitionSpec as P

BETA1 = 0.9
BETA2 = 0.9
EPS = 1e-8
LR = 0.1
STEP = 10
BIAS_ONE = 1.0 - BETA1 ** STEP
BIAS_TWO = 1.0 - BETA2 ** STEP

MESH = pl.DeviceIdType.MESH
F32 = jnp.float32
BF16 = jnp.bfloat16
NQ = 4
NH = 2
NU = 2
NG = 2
NDEV = 4
NSEND = 69
VMEM_BYTES = 56 * 2**20

ROWS_T = (((0,), (0,)), ((), ()))
COLS_T = (((1,), (1,)), ((), ()))


def split3(x):
    a0 = x.astype(BF16)
    r = x - a0.astype(F32)
    a1 = r.astype(BF16)
    a2 = (r - a1.astype(F32)).astype(BF16)
    return a0, a1, a2


def kernel(
    w_hbm, g_hbm, m_hbm, v_hbm, l_hbm, r_hbm, ql_hbm, qr_hbm,
    wbuf, mbuf, vbuf, lbuf, racc,
    grow, gbf, gi, gj, qrc, hcol, ncol, gis, ubuf, urecv,
    qlr, qlc, hacc, kb, qrx, kx, qlf, lx, lrecv, git,
    ssem, lsem, r_gbf, r_qlr, r_g32, r_qr, r_qlc, r_h, r_n, r_gj, r_gi, r_u, r_qx, r_l,
):
    lay = lax.axis_index("layer")
    z = lax.axis_index("col")
    i = lax.axis_index("row")
    y, c = i // 2, i % 2
    sib = 2 * y + (1 - c)
    opp = 2 * (1 - y) + c
    dia = 2 * (1 - y) + (1 - c)
    tr, tc = grow.shape[1], grow.shape[2]
    qrows = tc // NQ
    hcols = tc // NH
    urows = tr // NU
    grows = tr // NG
    head_rows = 3 * grows // 4
    gparts = (pl.ds(0, head_rows), pl.ds(head_rows, grows - head_rows), pl.ds(grows, grows))
    early = tc - tc // 4

    waits, qr_waits, late_waits, line_waits = [], [], [], []
    unused, most = list(range(NSEND)), [0]

    def dev(row, col):
        return (lay, col, row)

    def send(src, dst, rsem, row, col, cond=None, held=None):
        src, dst, rsem = src(), dst(), rsem()
        n = unused.pop(0)
        most[0] = max(most[0], n + 1)

        def make():
            return pltpu.make_async_remote_copy(
                src_ref=src, dst_ref=dst, send_sem=ssem.at[n], recv_sem=rsem,
                device_id=dev(row, col), device_id_type=MESH,
            )

        def go():
            make().start()

        def done():
            make().wait_send()

        if cond is None:
            go()
        else:
            pl.when(cond)(go)
        if held is None:
            waits.append((cond, done, n))
        else:
            held.append((cond, done, n))

    def settle(sent):
        for cond, done, n in sent:
            if cond is None:
                done()
            else:
                pl.when(cond)(done)
            unused.append(n)
        unused.sort()
        sent.clear()

    def arrived(dst, rsem, row, col):
        pltpu.make_async_remote_copy(
            src_ref=dst, dst_ref=dst, send_sem=ssem.at[0], recv_sem=rsem,
            device_id=dev(row, col), device_id_type=MESH,
        ).wait_recv()

    loads = {}

    def load(name, n, src, dst):
        cp = pltpu.make_async_copy(src, dst, lsem.at[n])
        cp.start()
        loads[name] = cp

    for q in range(NQ):
        rows = pl.ds(q * qrows, qrows)
        load(("qr", q), 1 + q, qr_hbm.at[rows], racc.at[rows])
        if q == 0:
            load("g", 0, g_hbm, grow.at[z])
            load("ql", 5, ql_hbm, qlf)
    load("m", 6, m_hbm, mbuf)
    load("v", 7, v_hbm, vbuf)
    load("w", 8, w_hbm, wbuf)
    load("l", 9, l_hbm, lbuf)

    barrier = pltpu.get_barrier_semaphore()
    for row in (sib, opp, dia):
        pl.semaphore_signal(barrier, inc=1, device_id=dev(row, z), device_id_type=MESH)

    @pl.when(z > 0)
    def _():
        pl.semaphore_signal(barrier, inc=1, device_id=dev(i, z - 1), device_id_type=MESH)

    @pl.when(z < NDEV - 1)
    def _():
        pl.semaphore_signal(barrier, inc=1, device_id=dev(i, z + 1), device_id_type=MESH)

    def qr_cast(q):
        rows = pl.ds(q * qrows, qrows)
        loads[("qr", q)].wait()
        qrc[i, rows] = racc[rows].astype(BF16)

    qr_cast(0)
    inner = jnp.logical_and(z > 0, z < NDEV - 1)

    @pl.when(inner)
    def _():
        pl.semaphore_wait(barrier, 5)

    @pl.when(jnp.logical_not(inner))
    def _():
        pl.semaphore_wait(barrier, 4)

    def line_own(buf, rs, held=None):
        send(lambda: buf.at[z], lambda: buf.at[z], lambda: rs.at[z], i, z + 1, z < NDEV - 1, held)
        send(lambda: buf.at[z], lambda: buf.at[z], lambda: rs.at[z], i, z - 1, z > 0, held)

    def line_forward(buf, rs, s, held=None):
        right = jnp.logical_and(z >= s, z < NDEV - 1)
        left = jnp.logical_and(z + s < NDEV, z > 0)

        @pl.when(right)
        def _():
            arrived(buf.at[z - s], rs.at[z - s], i, z - 1)

        send(lambda: buf.at[z - s], lambda: buf.at[z - s], lambda: rs.at[z - s], i, z + 1, right, held)

        @pl.when(left)
        def _():
            arrived(buf.at[z + s], rs.at[z + s], i, z + 1)

        send(lambda: buf.at[z + s], lambda: buf.at[z + s], lambda: rs.at[z + s], i, z - 1, left, held)

    def line_last(buf, rs, s):
        @pl.when(jnp.logical_and(z >= s, z == NDEV - 1))
        def _():
            arrived(buf.at[z - s], rs.at[z - s], i, z - 1)

        @pl.when(jnp.logical_and(z + s < NDEV, z == 0))
        def _():
            arrived(buf.at[z + s], rs.at[z + s], i, z + 1)

    def qr_own(q):
        rows = pl.ds(q * qrows, qrows)
        for row in (opp, sib):
            send(lambda: qrc.at[i, rows], lambda: qrc.at[i, rows], lambda: r_qr.at[i, q], row, z, held=qr_waits)

    qr_own(0)
    loads["g"].wait()
    gbf[z] = grow[z].astype(BF16)
    line_own(gbf, r_gbf)
    loads["ql"].wait()
    qlr[z] = qlf[...].astype(BF16)
    qr_cast(1)
    line_own(qlr, r_qlr)
    for q in range(2, NQ):
        qr_cast(q)
        qr_own(q - 1)
    load("r", 10, r_hbm, racc)

    def qr_forward(q):
        rows = pl.ds(q * qrows, qrows)
        arrived(qrc.at[opp, rows], r_qr.at[opp, q], opp, z)
        send(lambda: qrc.at[opp, rows], lambda: qrc.at[opp, rows], lambda: r_qr.at[opp, q], sib, z, held=qr_waits)

    def h_add(k, q, first=False):
        rows = pl.ds(q * qrows, qrows)
        part = jnp.dot(gbf[k, :, rows], qrc[k, rows], preferred_element_type=F32)
        if first:
            hacc[...] = part
        else:
            hacc[...] += part

    qr_own(NQ - 1)

    line_forward(gbf, r_gbf, 1)
    line_forward(qlr, r_qlr, 1)
    qr_forward(0)
    line_forward(gbf, r_gbf, 2)
    line_forward(qlr, r_qlr, 2)
    line_own(grow, r_g32, line_waits)
    qr_forward(1)
    for s in range(1, NDEV):
        line_last(gbf, r_gbf, s)
        line_last(qlr, r_qlr, s)

    for row in (opp, dia, sib):
        send(lambda row=row: qlr.at[row], lambda: qlc.at[i], lambda: r_qlc.at[i], row, z)
    qlc[i] = qlr[i]

    for q in range(NQ):
        h_add(i, q, first=q == 0)
    for q in range(NQ):
        rows = pl.ds(q * qrows, qrows)
        arrived(qrc.at[sib, rows], r_qr.at[sib, q], sib, z)
        h_add(sib, q)
    qr_forward(2)
    for q in range(2):
        h_add(opp, q)
    for q in range(2):
        rows = pl.ds(q * qrows, qrows)
        arrived(qrc.at[dia, rows], r_qr.at[dia, q], sib, z)
        h_add(dia, q)
    h_add(opp, 2)
    qr_forward(3)
    h_add(opp, 3)
    for q in range(2, NQ):
        rows = pl.ds(q * qrows, qrows)
        arrived(qrc.at[dia, rows], r_qr.at[dia, q], sib, z)
        h_add(dia, q)

    def own_part(buf, rs, n):
        cols = pl.ds(n * hcols, hcols)
        for row in (opp, sib):
            send(lambda: buf.at[i, :, cols], lambda: buf.at[i, :, cols], lambda: rs.at[i, n], row, z)

    def forward_part(buf, rs, n):
        cols = pl.ds(n * hcols, hcols)
        arrived(buf.at[opp, :, cols], rs.at[opp, n], opp, z)
        send(lambda: buf.at[opp, :, cols], lambda: buf.at[opp, :, cols], lambda: rs.at[opp, n], sib, z)

    def rest_part(buf, rs, n):
        cols = pl.ds(n * hcols, hcols)
        arrived(buf.at[sib, :, cols], rs.at[sib, n], sib, z)
        arrived(buf.at[dia, :, cols], rs.at[dia, n], sib, z)

    hcol[i] = hacc[...].astype(BF16)
    for n in range(NH):
        own_part(hcol, r_h, n)

    half = pl.ds(pl.multiple_of(c * (tc // 2), tc // 2), tc // 2)
    other_half = pl.ds(pl.multiple_of((1 - c) * (tc // 2), tc // 2), tc // 2)
    send(lambda: qrc.at[1, half], lambda: qrx.at[half], lambda: r_qx.at[0], i, 1, z == 0, held=qr_waits)
    send(lambda: qrc.at[2, half], lambda: qrx.at[half], lambda: r_qx.at[0], i, 2, z == 3, held=qr_waits)

    early_waits = waits[:]
    waits.clear()

    line_forward(grow, r_g32, 1, line_waits)
    for row in (opp, dia, sib):
        arrived(qlc.at[row], r_qlc.at[row], row, z)
    loads["m"].wait()
    loads["v"].wait()

    for n in range(NH):
        cols = pl.ds(n * hcols, hcols)
        forward_part(hcol, r_h, n)
        rest_part(hcol, r_h, n)
        rotated = sum(
            lax.dot_general(qlc[k], hcol[k, :, cols], ROWS_T, preferred_element_type=F32) for k in range(NDEV)
        )
        hacc[:, cols] = rotated
        rotated = hacc[:, cols]
        new_first = BETA1 * mbuf[:, cols] + (1.0 - BETA1) * rotated
        new_second = BETA2 * vbuf[:, cols] + (1.0 - BETA2) * rotated * rotated
        mbuf[:, cols] = new_first
        vbuf[:, cols] = new_second
        direction = (new_first / BIAS_ONE) / (jnp.sqrt(new_second / BIAS_TWO) + EPS)
        ncol[i, :, cols] = direction.astype(BF16)
        own_part(ncol, r_n, n)
    def gj_part(src, slot, late):
        cols = pl.ds(early, tc - early) if late else pl.ds(0, early)
        n = slot + 2 * late
        return (lambda: src.at[:, cols]), (lambda: gj.at[slot, :, cols]), (lambda: r_gj.at[n])

    head = gparts[0]
    ahead = 1 - 2 * y

    def relay(station, came_row, came_col):
        @pl.when(z == station)
        def _():
            arrived(gi.at[opp, head], r_gi.at[opp, 0], came_row, came_col)

        send(lambda: gi.at[opp, head], lambda: gi.at[opp, head], lambda: r_gi.at[opp, 0], i, z + ahead, z == station)

    send(lambda: grow.at[opp, head], lambda: gi.at[i, head], lambda: r_gi.at[i, 0], opp, z, z == 2 - y)

    calm = y == z // 2
    dup = i == z
    send(*gj_part(grow.at[z], 1, False), opp, z)
    send(*gj_part(grow.at[z], 1, True), opp, z, jnp.logical_not(calm))
    send(lambda: grow.at[z], lambda: gj.at[0], lambda: r_gj.at[0], sib, z)

    def gi_send(b, valid):
        there = jnp.logical_and(valid, b != i)
        for n, rows in enumerate(gparts):
            cond = jnp.logical_and(there, jnp.logical_or(b != opp, z == 3 - 3 * y)) if n == 0 else there
            send(lambda: grow.at[b, rows], lambda: gi.at[i, rows], lambda: r_gi.at[i, n], b, z, cond)

    line_last(grow, r_g32, 1)
    gi_send(z - 1, z >= 1)
    gi_send(z + 1, z + 1 < NDEV)

    for n in range(NH):
        forward_part(ncol, r_n, n)
        rest_part(ncol, r_n, n)
        cols = pl.ds(n * hcols, hcols)
        kb[:, cols] = sum(
            jnp.dot(qlr[k], ncol[k, :, cols], preferred_element_type=F32) for k in range(NDEV)
        ).astype(BF16)

    settle(early_waits)

    def u_send(a, h, slot, col, cond):
        rows = pl.ds(h * urows, urows)
        send(lambda: ubuf.at[a, rows], lambda: urecv.at[slot, rows], lambda: r_u.at[slot, h], i, col, cond)

    def u_first(a, to_right):
        for h in range(NU):
            if to_right:
                u_send(a, h, a, z + 1, z == 0)
            else:
                u_send(a, h, NDEV if a == NDEV - 2 else a, z - 1, z == NDEV - 1)

    for piece, starts in ((3, ((3, True),)), (0, ((0, False),)), (2, ((2, True),)), (1, ((1, False),))):
        ubuf[piece] = lax.dot_general(kb[...], qrc[piece], COLS_T, preferred_element_type=F32)
        for a, to_right in starts:
            u_first(a, to_right)
    send(lambda: kb, lambda: kx, lambda: r_qx.at[2], i, 1, z == 0)
    send(lambda: kb, lambda: kx, lambda: r_qx.at[2], i, 2, z == 3)
    line_forward(grow, r_g32, 2, line_waits)

    relay(1 + y, opp, z)

    @pl.when(inner)
    def _():
        arrived(qrx.at[half], r_qx.at[0], i, 3 * (z // 2))

    send(lambda: qrx.at[half], lambda: qrx.at[half], lambda: r_qx.at[1], sib, z, inner)

    def u_at(a, h, station, to_right):
        rows = pl.ds(h * urows, urows)
        slot = NDEV if (not to_right and station == a) else a

        @pl.when(z == station)
        def _():
            arrived(urecv.at[slot, rows], r_u.at[slot, h], i, station - 1 if to_right else station + 1)
            ubuf[a, rows] += urecv[slot, rows]

        if station != a:
            nxt = station + 1 if to_right else station - 1
            nslot = NDEV if (not to_right and nxt == a) else a
            u_send(a, h, nslot, nxt, z == station)

    line_last(grow, r_g32, 2)
    gi_send(z - 2, z >= 2)
    gi_send(z + 2, z + 2 < NDEV)
    far = jnp.logical_or(jnp.logical_and(z == 0, i == 3), jnp.logical_and(z == 3, i == 0))

    def u_round(t):
        for h in range(NU):
            for a in (3, 2, 1):
                st = t - (3 - a)
                if 1 <= st <= a and a > 1:
                    u_at(a, h, st, True)
                    u_at(NDEV - 1 - a, h, NDEV - 1 - st, False)

    def gj_split(slot, ref, start=0, size=None):
        cols = pl.ds(start, size or tc)
        for t, term in enumerate(split3(ref[:, cols])):
            qrc[slot, pl.ds(t * tr, tr), cols] = term

    def gi_split(k, ref, n):
        rows = pl.ds(n * grows, grows)
        for t, term in enumerate(split3(ref[rows])):
            gis[k, t, rows] = term

    def right_add(blocks, n=None, start=0, size=None, first=False, unroll=1):
        begin, depth = (0, tr) if n is None else (n * grows, grows)
        cols = pl.ds(start, size or tc)

        def body(m, carry):
            rows = pl.ds(pl.multiple_of(m * tr, tr), tr)
            left, right = [], []
            for k, slot, turned in blocks:
                if turned is None:
                    a = [gis[k, t, pl.ds(begin, depth), rows].T for t in range(3)]
                else:
                    a = [git[turned, rows, pl.ds(t * tr + begin, depth)] for t in range(3)]
                b = [qrc[slot, pl.ds(t * tr + begin, depth), cols] for t in range(3)]
                left += [a[0], a[0], a[0], a[1], a[1], a[2]]
                right += [b[0], b[1], b[2], b[0], b[1], b[0]]
            left, right = jnp.concatenate(left, axis=1), jnp.concatenate(right, axis=0)
            share = (1.0 - BETA2) * jnp.dot(left, right, preferred_element_type=F32)
            old = racc[rows, cols]
            racc[rows, cols] = (BETA2 * old if first else old) + share
            return carry

        lax.fori_loop(0, tc // tr, body, 0, unroll=unroll)

    def gi_arrived(row, n, slot, turned=None):
        @pl.when(jnp.logical_not(dup))
        def _():
            if n == 1:
                arrived(gi.at[row, gparts[2]], r_gi.at[row, 2], row, z)
            else:
                arrived(gi.at[row, gparts[1]], r_gi.at[row, 1], row, z)
                if row is opp:
                    @pl.when(z == 3 * y)
                    def _():
                        arrived(gi.at[row, head], r_gi.at[row, 0], row, z)

                    @pl.when(z == 3 - 3 * y)
                    def _():
                        arrived(gi.at[row, head], r_gi.at[row, 0], i, z - ahead)
                else:
                    arrived(gi.at[row, head], r_gi.at[row, 0], row, z)
            gi_split(row, gi.at[row], n)

        @pl.when(dup)
        def _():
            gi_split(row, gj.at[slot], n)

        if turned is not None:
            for t in range(3):
                git[turned, :, pl.ds(t * tr + n * grows, grows)] = gis[row, t, pl.ds(n * grows, grows)].T

    def left_part(k, slot):
        pieces = [gis[k, t] for t in range(3)]
        other = [gis[z, t] for t in range(3)]
        total = None
        for t, u in ((0, 0), (0, 1), (1, 0), (1, 1), (0, 2), (2, 0)):
            d = lax.dot_general(pieces[t], other[u], COLS_T, preferred_element_type=F32)
            total = d if total is None else total + d
        lx[slot] = total

    settle(qr_waits)
    gj_split(0, grow.at[z])
    arrived(gj.at[0], r_gj.at[0], sib, z)
    gj_split(1, gj.at[0])
    loads["r"].wait()

    def chip_rows():
        for n in range(NG):
            gi_split(i, grow.at[i], n)
        right_add([(i, 0, None)], first=True)
        for n in range(NG):
            gi_arrived(sib, n, 0)
        right_add([(sib, 1, None)])

    pl.when(jnp.logical_not(far))(chip_rows)
    arrived(gj.at[1, :, pl.ds(0, early)], r_gj.at[1], opp, z)
    send(*gj_part(gj.at[1], 2, False), sib, z)
    relay(2 - y, i, z - ahead)
    gj_split(2, gj.at[1], 0, early)

    def gj_late_arrived():
        arrived(gj.at[1, :, pl.ds(early, tc - early)], r_gj.at[3], opp, z)

    u_round(1)
    line_last(grow, r_g32, 3)
    gi_send(z - 3, z >= 3)
    gi_send(z + 3, z + 3 < NDEV)
    send(*gj_part(grow.at[z], 1, True), opp, z, jnp.logical_and(calm, inner), held=late_waits)
    pl.when(calm)(gj_late_arrived)
    send(*gj_part(gj.at[1], 2, True), sib, z, calm)

    @pl.when(calm)
    def _():
        gj_split(2, gj.at[1], early, tc - early)

    arrived(gj.at[2, :, pl.ds(0, early)], r_gj.at[2], sib, z)
    gj_split(3, gj.at[2], 0, early)

    def gj_last_arrived():
        arrived(gj.at[2, :, pl.ds(early, tc - early)], r_gj.at[4], sib, z)
        gj_split(3, gj.at[2], early, tc - early)

    pl.when(calm)(gj_last_arrived)
    pl.when(far)(chip_rows)
    u_round(2)
    others = [(opp, 2, 0), (dia, 3, 1)]
    for n in range(NG - 1):
        gi_arrived(opp, n, 1, 0)
        gi_arrived(dia, n, 2, 1)
        right_add(others, n, 0, early)

    send(*gj_part(grow.at[z], 1, True), opp, z, jnp.logical_and(calm, jnp.logical_not(inner)), held=late_waits)

    loads["w"].wait()
    loads["l"].wait()
    gi_arrived(dia, NG - 1, 2, 1)
    gi_arrived(opp, NG - 1, 1, 0)

    left_part(dia, 3)
    send(lambda: lx.at[3], lambda: lrecv.at[2], lambda: r_l.at[2], sib, z)
    left_part(opp, 2)
    arrived(lrecv.at[2], r_l.at[2], sib, z)
    lx[2] += lrecv[2]
    send(lambda: lx.at[2], lambda: lrecv.at[1], lambda: r_l.at[1], opp, z, held=late_waits)
    left_part(sib, 1)
    send(lambda: lx.at[1], lambda: lrecv.at[0], lambda: r_l.at[0], sib, z, held=late_waits)
    left_part(i, 0)
    right_add(others, NG - 1, 0, early, unroll=2)
    pl.when(jnp.logical_not(calm))(gj_late_arrived)
    send(*gj_part(gj.at[1], 2, True), sib, z, jnp.logical_not(calm), held=late_waits)

    @pl.when(jnp.logical_not(calm))
    def _():
        gj_split(2, gj.at[1], early, tc - early)

    @pl.when(inner)
    def _():
        arrived(qrx.at[other_half], r_qx.at[1], sib, z)
        arrived(kx, r_qx.at[2], i, 3 * (z // 2))
        ubuf[z] += lax.dot_general(kx[...], qrx[...], COLS_T, preferred_element_type=F32)

    pl.when(jnp.logical_not(calm))(gj_last_arrived)
    right_add(others, None, early, tc - early, unroll=2)
    u_round(3)
    wbuf[...] = wbuf[...] - LR * ubuf[z]
    settle(waits)
    settle(line_waits)
    arrived(lrecv.at[0], r_l.at[0], sib, z)
    left_sum = lx[0] + lrecv[0]
    arrived(lrecv.at[1], r_l.at[1], opp, z)
    left_sum += lrecv[1]
    lbuf[...] = BETA2 * lbuf[...] + (1.0 - BETA2) * left_sum

    settle(waits)
    settle(late_waits)
    assert most[0] == NSEND, most[0]


def write_out(*refs):
    ins, outs, sem = refs[:5], refs[5:10], refs[10]
    copies = []
    for a, b in zip(ins, outs):
        step = a.shape[0] // 4
        for n in range(4):
            rows = pl.ds(n * step, step)
            copies.append(pltpu.make_async_copy(a.at[rows], b.at[rows], sem.at[len(copies)]))
    for cp in copies:
        cp.start()
    for cp in copies:
        cp.wait()


def solution(mesh):
    tile_spec = P(("layer", "row"), "col")

    def local_step(weight, grad_in, mom_first, mom_second, stat_left, stat_right, basis_left, basis_right):
        tr, tc = grad_in.shape
        tl = stat_left.shape[0]
        dma = pltpu.SemaphoreType.DMA
        scratch = [
            pltpu.VMEM((4, tr, tc), F32),
            pltpu.VMEM((4, tr, tc), BF16),
            pltpu.VMEM((4, tr, tc), F32),
            pltpu.VMEM((3, tr, tc), F32),
            pltpu.VMEM((4, tc, tc), BF16),
            pltpu.VMEM((4, tr, tc), BF16),
            pltpu.VMEM((4, tr, tc), BF16),
            pltpu.VMEM((4, 3, tr, tc), BF16),
            pltpu.VMEM((4, tr, tc), F32),
            pltpu.VMEM((5, tr, tc), F32),
            pltpu.VMEM((4, tl, tl), BF16),
            pltpu.VMEM((4, tl, tl), BF16),
            pltpu.VMEM((tr, tc), F32),
            pltpu.VMEM((tr, tc), BF16),
            pltpu.VMEM((tc, tc), BF16),
            pltpu.VMEM((tr, tc), BF16),
            pltpu.VMEM((tl, tl), F32),
            pltpu.VMEM((4, tl, tl), F32),
            pltpu.VMEM((3, tl, tl), F32),
            pltpu.VMEM((2, tc, 3 * tr), BF16),
            dma((NSEND,)),
            dma((11,)),
            dma((4,)), dma((4,)), dma((4,)),
            dma((4, NQ)), dma((4,)),
            dma((4, NH)), dma((4, NH)),
            dma((5,)), dma((4, 3)),
            dma((5, NU)), dma((3,)), dma((3,)),
        ]
        any_spec = pl.BlockSpec(memory_space=pl.ANY)
        vmem_spec = pl.BlockSpec(memory_space=pltpu.VMEM)
        outs = [weight, mom_first, mom_second, stat_left, stat_right]
        results = pl.pallas_call(
            kernel,
            name="soap_step",
            out_shape=[pltpu.VMEM(o.shape, o.dtype) for o in outs],
            in_specs=[any_spec] * 8,
            out_specs=[vmem_spec] * 5,
            scratch_shapes=scratch,
            compiler_params=pltpu.CompilerParams(
                collective_id=0, has_side_effects=True, vmem_limit_bytes=VMEM_BYTES,
            ),
        )(weight, grad_in, mom_first, mom_second, stat_left, stat_right, basis_left, basis_right)
        results = [pltpu.with_memory_space_constraint(r, pltpu.VMEM) for r in results]
        return pl.pallas_call(
            write_out,
            name="write_out",
            out_shape=[jax.ShapeDtypeStruct(o.shape, o.dtype) for o in outs],
            in_specs=[vmem_spec] * 5,
            out_specs=[any_spec] * 5,
            scratch_shapes=[dma((20,))],
            compiler_params=pltpu.CompilerParams(vmem_limit_bytes=2**20),
        )(*results)

    return jax.shard_map(local_step, mesh=mesh, in_specs=(tile_spec,) * 8, out_specs=(tile_spec,) * 5, check_vma=False)
```

```python
import jax
import jax.numpy as jnp
from jax import lax
from jax.experimental import pallas as pl
from jax.experimental.pallas import tpu as pltpu
from jax.sharding import PartitionSpec as P

BETA1 = 0.9
BETA2 = 0.9
EPS = 1e-8
LR = 0.1
STEP = 10
BIAS_ONE = 1.0 - BETA1 ** STEP
BIAS_TWO = 1.0 - BETA2 ** STEP

MESH = pl.DeviceIdType.MESH
F32 = jnp.float32
BF16 = jnp.bfloat16
NQ = 4
NH = 2
NU = 2
NG = 2
NDEV = 4
NSEND = 64
VMEM_BYTES = 56 * 2**20

ROWS_T = (((0,), (0,)), ((), ()))
COLS_T = (((1,), (1,)), ((), ()))


def split3(x):
    a0 = x.astype(BF16)
    r = x - a0.astype(F32)
    a1 = r.astype(BF16)
    a2 = (r - a1.astype(F32)).astype(BF16)
    return a0, a1, a2


def kernel(
    w_hbm, g_hbm, m_hbm, v_hbm, l_hbm, r_hbm, ql_hbm, qr_hbm,
    wbuf, mbuf, vbuf, lbuf, racc,
    grow, gbf, gi, gj, qrc, hcol, ncol, gis, ubuf, urecv,
    qlr, qlc, hacc, kb, qrx, kx, qlf, lx, lrecv, git,
    ssem, lsem, r_gbf, r_qlr, r_g32, r_qr, r_qlc, r_h, r_n, r_gj, r_gi, r_u, r_qx, r_l,
):
    lay = lax.axis_index("layer")
    z = lax.axis_index("col")
    i = lax.axis_index("row")
    y, c = i // 2, i % 2
    sib = 2 * y + (1 - c)
    opp = 2 * (1 - y) + c
    dia = 2 * (1 - y) + (1 - c)
    tr, tc = grow.shape[1], grow.shape[2]
    qrows = tc // NQ
    hcols = tc // NH
    urows = tr // NU
    grows = tr // NG
    head_rows = 5 * grows // 8
    gparts = (pl.ds(0, head_rows), pl.ds(head_rows, grows - head_rows), pl.ds(grows, grows))
    early = tc - tc // 4

    waits, qr_waits, late_waits, line_waits, far_waits = [], [], [], [], []
    unused, most = list(range(NSEND)), [0]

    def dev(row, col):
        return (lay, col, row)

    def send(src, dst, rsem, row, col, cond=None, held=None):
        src, dst, rsem = src(), dst(), rsem()
        n = unused.pop(0)
        most[0] = max(most[0], n + 1)

        def make():
            return pltpu.make_async_remote_copy(
                src_ref=src, dst_ref=dst, send_sem=ssem.at[n], recv_sem=rsem,
                device_id=dev(row, col), device_id_type=MESH,
            )

        def go():
            make().start()

        def done():
            make().wait_send()

        if cond is None:
            go()
        else:
            pl.when(cond)(go)
        if held is None:
            waits.append((cond, done, n))
        else:
            held.append((cond, done, n))

    def settle(sent):
        for cond, done, n in sent:
            if cond is None:
                done()
            else:
                pl.when(cond)(done)
            unused.append(n)
        unused.sort()
        sent.clear()

    def arrived(dst, rsem, row, col):
        pltpu.make_async_remote_copy(
            src_ref=dst, dst_ref=dst, send_sem=ssem.at[0], recv_sem=rsem,
            device_id=dev(row, col), device_id_type=MESH,
        ).wait_recv()

    loads = {}

    def load(name, n, src, dst):
        cp = pltpu.make_async_copy(src, dst, lsem.at[n])
        cp.start()
        loads[name] = cp

    for q in range(NQ):
        rows = pl.ds(q * qrows, qrows)
        load(("qr", q), 1 + q, qr_hbm.at[rows], racc.at[rows])
        if q == 0:
            load("g", 0, g_hbm, grow.at[z])
            load("ql", 5, ql_hbm, qlf)
    load("m", 6, m_hbm, mbuf)
    load("v", 7, v_hbm, vbuf)
    load("w", 8, w_hbm, wbuf)
    load("l", 9, l_hbm, lbuf)

    barrier = pltpu.get_barrier_semaphore()
    for row in (sib, opp, dia):
        pl.semaphore_signal(barrier, inc=1, device_id=dev(row, z), device_id_type=MESH)

    @pl.when(z > 0)
    def _():
        pl.semaphore_signal(barrier, inc=1, device_id=dev(i, z - 1), device_id_type=MESH)

    @pl.when(z < NDEV - 1)
    def _():
        pl.semaphore_signal(barrier, inc=1, device_id=dev(i, z + 1), device_id_type=MESH)

    def qr_cast(q):
        rows = pl.ds(q * qrows, qrows)
        loads[("qr", q)].wait()
        qrc[i, rows] = racc[rows].astype(BF16)

    qr_cast(0)
    inner = jnp.logical_and(z > 0, z < NDEV - 1)

    @pl.when(inner)
    def _():
        pl.semaphore_wait(barrier, 5)

    @pl.when(jnp.logical_not(inner))
    def _():
        pl.semaphore_wait(barrier, 4)

    def line_own(buf, rs, held=None):
        send(lambda: buf.at[z], lambda: buf.at[z], lambda: rs.at[z], i, z + 1, z < NDEV - 1, held)
        send(lambda: buf.at[z], lambda: buf.at[z], lambda: rs.at[z], i, z - 1, z > 0, held)

    def line_forward(buf, rs, s, held=None):
        right = jnp.logical_and(z >= s, z < NDEV - 1)
        left = jnp.logical_and(z + s < NDEV, z > 0)

        @pl.when(right)
        def _():
            arrived(buf.at[z - s], rs.at[z - s], i, z - 1)

        send(lambda: buf.at[z - s], lambda: buf.at[z - s], lambda: rs.at[z - s], i, z + 1, right, held)

        @pl.when(left)
        def _():
            arrived(buf.at[z + s], rs.at[z + s], i, z + 1)

        send(lambda: buf.at[z + s], lambda: buf.at[z + s], lambda: rs.at[z + s], i, z - 1, left, held)

    def line_last(buf, rs, s):
        @pl.when(jnp.logical_and(z >= s, z == NDEV - 1))
        def _():
            arrived(buf.at[z - s], rs.at[z - s], i, z - 1)

        @pl.when(jnp.logical_and(z + s < NDEV, z == 0))
        def _():
            arrived(buf.at[z + s], rs.at[z + s], i, z + 1)

    def qr_own(q):
        rows = pl.ds(q * qrows, qrows)
        for row in (opp, sib):
            send(lambda: qrc.at[i, rows], lambda: qrc.at[i, rows], lambda: r_qr.at[i, q], row, z, held=qr_waits)

    qr_own(0)
    loads["g"].wait()
    gbf[z] = grow[z].astype(BF16)
    line_own(gbf, r_gbf)
    loads["ql"].wait()
    qlr[z] = qlf[...].astype(BF16)
    qr_cast(1)
    line_own(qlr, r_qlr)
    for q in range(2, NQ):
        qr_cast(q)
        qr_own(q - 1)
    load("r", 10, r_hbm, racc)

    def qr_forward(q):
        rows = pl.ds(q * qrows, qrows)
        arrived(qrc.at[opp, rows], r_qr.at[opp, q], opp, z)
        send(lambda: qrc.at[opp, rows], lambda: qrc.at[opp, rows], lambda: r_qr.at[opp, q], sib, z, held=qr_waits)

    def h_add(k, q, first=False):
        rows = pl.ds(q * qrows, qrows)
        part = jnp.dot(gbf[k, :, rows], qrc[k, rows], preferred_element_type=F32)
        if first:
            hacc[...] = part
        else:
            hacc[...] += part

    qr_own(NQ - 1)

    line_forward(gbf, r_gbf, 1)
    line_forward(qlr, r_qlr, 1)
    qr_forward(0)
    line_forward(gbf, r_gbf, 2)
    line_forward(qlr, r_qlr, 2)
    line_own(grow, r_g32, line_waits)
    qr_forward(1)
    for s in range(1, NDEV):
        line_last(gbf, r_gbf, s)
        line_last(qlr, r_qlr, s)

    for row in (opp, dia, sib):
        send(lambda row=row: qlr.at[row], lambda: qlc.at[i], lambda: r_qlc.at[i], row, z)
    qlc[i] = qlr[i]

    for q in range(NQ):
        h_add(i, q, first=q == 0)
    for q in range(NQ):
        rows = pl.ds(q * qrows, qrows)
        arrived(qrc.at[sib, rows], r_qr.at[sib, q], sib, z)
        h_add(sib, q)
    qr_forward(2)
    for q in range(2):
        h_add(opp, q)
    for q in range(2):
        rows = pl.ds(q * qrows, qrows)
        arrived(qrc.at[dia, rows], r_qr.at[dia, q], sib, z)
        h_add(dia, q)
    h_add(opp, 2)
    qr_forward(3)
    h_add(opp, 3)
    for q in range(2, NQ):
        rows = pl.ds(q * qrows, qrows)
        arrived(qrc.at[dia, rows], r_qr.at[dia, q], sib, z)
        h_add(dia, q)

    def own_part(buf, rs, n):
        cols = pl.ds(n * hcols, hcols)
        for row in (opp, sib):
            send(lambda: buf.at[i, :, cols], lambda: buf.at[i, :, cols], lambda: rs.at[i, n], row, z)

    def forward_part(buf, rs, n):
        cols = pl.ds(n * hcols, hcols)
        arrived(buf.at[opp, :, cols], rs.at[opp, n], opp, z)
        send(lambda: buf.at[opp, :, cols], lambda: buf.at[opp, :, cols], lambda: rs.at[opp, n], sib, z)

    def rest_part(buf, rs, n):
        cols = pl.ds(n * hcols, hcols)
        arrived(buf.at[sib, :, cols], rs.at[sib, n], sib, z)
        arrived(buf.at[dia, :, cols], rs.at[dia, n], sib, z)

    hcol[i] = hacc[...].astype(BF16)
    for n in range(NH):
        own_part(hcol, r_h, n)

    half = pl.ds(pl.multiple_of(c * (tc // 2), tc // 2), tc // 2)
    other_half = pl.ds(pl.multiple_of((1 - c) * (tc // 2), tc // 2), tc // 2)
    send(lambda: qrc.at[1, half], lambda: qrx.at[half], lambda: r_qx.at[0], i, 1, z == 0, held=qr_waits)
    send(lambda: qrc.at[2, half], lambda: qrx.at[half], lambda: r_qx.at[0], i, 2, z == 3, held=qr_waits)

    early_waits = waits[:]
    waits.clear()

    line_forward(grow, r_g32, 1, line_waits)
    for row in (opp, dia, sib):
        arrived(qlc.at[row], r_qlc.at[row], row, z)
    loads["m"].wait()
    loads["v"].wait()

    for n in range(NH):
        cols = pl.ds(n * hcols, hcols)
        forward_part(hcol, r_h, n)
        rest_part(hcol, r_h, n)
        rotated = sum(
            lax.dot_general(qlc[k], hcol[k, :, cols], ROWS_T, preferred_element_type=F32) for k in range(NDEV)
        )
        hacc[:, cols] = rotated
        rotated = hacc[:, cols]
        new_first = BETA1 * mbuf[:, cols] + (1.0 - BETA1) * rotated
        new_second = BETA2 * vbuf[:, cols] + (1.0 - BETA2) * rotated * rotated
        mbuf[:, cols] = new_first
        vbuf[:, cols] = new_second
        direction = (new_first / BIAS_ONE) / (jnp.sqrt(new_second / BIAS_TWO) + EPS)
        ncol[i, :, cols] = direction.astype(BF16)
        own_part(ncol, r_n, n)
    def gj_part(src, slot, late):
        cols = pl.ds(early, tc - early) if late else pl.ds(0, early)
        n = slot + 2 * late
        return (lambda: src.at[:, cols]), (lambda: gj.at[slot, :, cols]), (lambda: r_gj.at[n])

    head = gparts[0]
    ahead = 1 - 2 * y

    def relay(station, came_row, came_col):
        @pl.when(z == station)
        def _():
            arrived(gi.at[opp, head], r_gi.at[opp, 0], came_row, came_col)

        send(lambda: gi.at[opp, head], lambda: gi.at[opp, head], lambda: r_gi.at[opp, 0], i, z + ahead, z == station)

    send(lambda: grow.at[opp, head], lambda: gi.at[i, head], lambda: r_gi.at[i, 0], opp, z, z == 2 - y)

    calm = y == z // 2
    dup = i == z
    send(*gj_part(grow.at[z], 1, False), opp, z)
    send(*gj_part(grow.at[z], 1, True), opp, z, jnp.logical_not(calm))
    send(lambda: grow.at[z], lambda: gj.at[0], lambda: r_gj.at[0], sib, z)

    def gi_send(b, valid, held=None):
        there = jnp.logical_and(valid, b != i)
        for n, rows in enumerate(gparts):
            cond = jnp.logical_and(there, jnp.logical_or(b != opp, z == 3 - 3 * y)) if n == 0 else there
            send(lambda: grow.at[b, rows], lambda: gi.at[i, rows], lambda: r_gi.at[i, n], b, z, cond, held)

    line_last(grow, r_g32, 1)
    gi_send(z - 1, z >= 1)
    gi_send(z + 1, z + 1 < NDEV)

    for n in range(NH):
        forward_part(ncol, r_n, n)
        rest_part(ncol, r_n, n)
        cols = pl.ds(n * hcols, hcols)
        kb[:, cols] = sum(
            jnp.dot(qlr[k], ncol[k, :, cols], preferred_element_type=F32) for k in range(NDEV)
        ).astype(BF16)

    settle(early_waits)

    def u_send(a, h, slot, col, cond):
        rows = pl.ds(h * urows, urows)
        send(lambda: ubuf.at[a, rows], lambda: urecv.at[slot, rows], lambda: r_u.at[slot, h], i, col, cond)

    def u_first(a, to_right):
        for h in range(NU):
            if to_right:
                u_send(a, h, a, z + 1, z == 0)
            else:
                u_send(a, h, NDEV if a == NDEV - 2 else a, z - 1, z == NDEV - 1)

    for piece, starts in ((3, ((3, True),)), (0, ((0, False),)), (2, ((2, True),)), (1, ((1, False),))):
        ubuf[piece] = lax.dot_general(kb[...], qrc[piece], COLS_T, preferred_element_type=F32)
        for a, to_right in starts:
            u_first(a, to_right)
    send(lambda: kb, lambda: kx, lambda: r_qx.at[2], i, 1, z == 0)
    send(lambda: kb, lambda: kx, lambda: r_qx.at[2], i, 2, z == 3)
    line_forward(grow, r_g32, 2, line_waits)

    relay(1 + y, opp, z)

    @pl.when(inner)
    def _():
        arrived(qrx.at[half], r_qx.at[0], i, 3 * (z // 2))

    send(lambda: qrx.at[half], lambda: qrx.at[half], lambda: r_qx.at[1], sib, z, inner)

    def u_at(a, h, station, to_right):
        rows = pl.ds(h * urows, urows)
        slot = NDEV if (not to_right and station == a) else a

        @pl.when(z == station)
        def _():
            arrived(urecv.at[slot, rows], r_u.at[slot, h], i, station - 1 if to_right else station + 1)
            ubuf[a, rows] += urecv[slot, rows]

        if station != a:
            nxt = station + 1 if to_right else station - 1
            nslot = NDEV if (not to_right and nxt == a) else a
            u_send(a, h, nslot, nxt, z == station)

    line_last(grow, r_g32, 2)
    gi_send(z - 2, z >= 2)
    gi_send(z + 2, z + 2 < NDEV)
    far = jnp.logical_or(jnp.logical_and(z == 0, i == 3), jnp.logical_and(z == 3, i == 0))

    def u_round(t):
        for h in range(NU):
            for a in (3, 2, 1):
                st = t - (3 - a)
                if 1 <= st <= a and a > 1:
                    u_at(a, h, st, True)
                    u_at(NDEV - 1 - a, h, NDEV - 1 - st, False)

    def gj_split(slot, ref, start=0, size=None):
        cols = pl.ds(start, size or tc)
        for t, term in enumerate(split3(ref[:, cols])):
            qrc[slot, pl.ds(t * tr, tr), cols] = term

    def gi_split(k, ref, n):
        rows = pl.ds(n * grows, grows)
        for t, term in enumerate(split3(ref[rows])):
            gis[k, t, rows] = term

    def right_add(blocks, n=None, start=0, size=None, first=False, unroll=1):
        begin, depth = (0, tr) if n is None else (n * grows, grows)
        cols = pl.ds(start, size or tc)

        def body(m, carry):
            rows = pl.ds(pl.multiple_of(m * tr, tr), tr)
            left, right = [], []
            for k, slot, turned in blocks:
                if turned is None:
                    a = [gis[k, t, pl.ds(begin, depth), rows].T for t in range(3)]
                else:
                    a = [git[turned, rows, pl.ds(t * tr + begin, depth)] for t in range(3)]
                b = [qrc[slot, pl.ds(t * tr + begin, depth), cols] for t in range(3)]
                left += [a[0], a[0], a[0], a[1], a[1], a[2]]
                right += [b[0], b[1], b[2], b[0], b[1], b[0]]
            left, right = jnp.concatenate(left, axis=1), jnp.concatenate(right, axis=0)
            share = (1.0 - BETA2) * jnp.dot(left, right, preferred_element_type=F32)
            old = racc[rows, cols]
            racc[rows, cols] = (BETA2 * old if first else old) + share
            return carry

        lax.fori_loop(0, tc // tr, body, 0, unroll=unroll)

    def gi_arrived(row, n, slot, turned=None):
        @pl.when(jnp.logical_not(dup))
        def _():
            if n == 1:
                arrived(gi.at[row, gparts[2]], r_gi.at[row, 2], row, z)
            else:
                arrived(gi.at[row, gparts[1]], r_gi.at[row, 1], row, z)
                if row is opp:
                    @pl.when(z == 3 * y)
                    def _():
                        arrived(gi.at[row, head], r_gi.at[row, 0], row, z)

                    @pl.when(z == 3 - 3 * y)
                    def _():
                        arrived(gi.at[row, head], r_gi.at[row, 0], i, z - ahead)
                else:
                    arrived(gi.at[row, head], r_gi.at[row, 0], row, z)
            gi_split(row, gi.at[row], n)

        @pl.when(dup)
        def _():
            gi_split(row, gj.at[slot], n)

        if turned is not None:
            for t in range(3):
                git[turned, :, pl.ds(t * tr + n * grows, grows)] = gis[row, t, pl.ds(n * grows, grows)].T

    def left_part(k, slot):
        pieces = [gis[k, t] for t in range(3)]
        other = [gis[z, t] for t in range(3)]
        total = None
        for t, u in ((0, 0), (0, 1), (1, 0), (1, 1), (0, 2), (2, 0)):
            d = lax.dot_general(pieces[t], other[u], COLS_T, preferred_element_type=F32)
            total = d if total is None else total + d
        lx[slot] = total

    settle(qr_waits)
    gj_split(0, grow.at[z])
    arrived(gj.at[0], r_gj.at[0], sib, z)
    gj_split(1, gj.at[0])
    loads["r"].wait()

    def chip_rows():
        for n in range(NG):
            gi_split(i, grow.at[i], n)
        right_add([(i, 0, None)], first=True)
        for n in range(NG):
            gi_arrived(sib, n, 0)
        right_add([(sib, 1, None)])

    pl.when(jnp.logical_not(far))(chip_rows)
    arrived(gj.at[1, :, pl.ds(0, early)], r_gj.at[1], opp, z)
    send(*gj_part(gj.at[1], 2, False), sib, z)
    relay(2 - y, i, z - ahead)
    gj_split(2, gj.at[1], 0, early)

    def gj_late_arrived():
        arrived(gj.at[1, :, pl.ds(early, tc - early)], r_gj.at[3], opp, z)

    u_round(1)
    line_last(grow, r_g32, 3)
    gi_send(z - 3, z >= 3, far_waits)
    gi_send(z + 3, z + 3 < NDEV, far_waits)
    send(*gj_part(grow.at[z], 1, True), opp, z, jnp.logical_and(calm, inner), held=late_waits)
    pl.when(calm)(gj_late_arrived)
    send(*gj_part(gj.at[1], 2, True), sib, z, calm)

    @pl.when(calm)
    def _():
        gj_split(2, gj.at[1], early, tc - early)

    arrived(gj.at[2, :, pl.ds(0, early)], r_gj.at[2], sib, z)
    gj_split(3, gj.at[2], 0, early)

    def gj_last_arrived():
        arrived(gj.at[2, :, pl.ds(early, tc - early)], r_gj.at[4], sib, z)
        gj_split(3, gj.at[2], early, tc - early)

    pl.when(calm)(gj_last_arrived)
    pl.when(far)(chip_rows)
    u_round(2)
    others = [(opp, 2, 0), (dia, 3, 1)]
    for n in range(NG - 1):
        gi_arrived(opp, n, 1, 0)
        gi_arrived(dia, n, 2, 1)
        right_add(others, n, 0, early)

    loads["w"].wait()
    loads["l"].wait()
    gi_arrived(dia, NG - 1, 2, 1)
    gi_arrived(opp, NG - 1, 1, 0)

    left_part(dia, 3)
    settle(far_waits)
    send(lambda: lx.at[3], lambda: lrecv.at[2], lambda: r_l.at[2], sib, z)
    left_part(opp, 2)
    arrived(lrecv.at[2], r_l.at[2], sib, z)
    send(*gj_part(grow.at[z], 1, True), opp, z, jnp.logical_and(calm, jnp.logical_not(inner)), held=late_waits)
    lx[2] += lrecv[2]
    send(lambda: lx.at[2], lambda: lrecv.at[1], lambda: r_l.at[1], opp, z, held=late_waits)
    left_part(sib, 1)
    send(lambda: lx.at[1], lambda: lrecv.at[0], lambda: r_l.at[0], sib, z, held=late_waits)
    left_part(i, 0)
    right_add(others, NG - 1, 0, early, unroll=2)
    pl.when(jnp.logical_not(calm))(gj_late_arrived)
    send(*gj_part(gj.at[1], 2, True), sib, z, jnp.logical_not(calm), held=late_waits)

    @pl.when(jnp.logical_not(calm))
    def _():
        gj_split(2, gj.at[1], early, tc - early)

    @pl.when(inner)
    def _():
        arrived(qrx.at[other_half], r_qx.at[1], sib, z)
        arrived(kx, r_qx.at[2], i, 3 * (z // 2))
        ubuf[z] += lax.dot_general(kx[...], qrx[...], COLS_T, preferred_element_type=F32)

    pl.when(jnp.logical_not(calm))(gj_last_arrived)
    right_add(others, None, early, tc - early, unroll=2)
    u_round(3)
    wbuf[...] = wbuf[...] - LR * ubuf[z]
    settle(waits)
    settle(line_waits)
    arrived(lrecv.at[0], r_l.at[0], sib, z)
    left_sum = lx[0] + lrecv[0]
    arrived(lrecv.at[1], r_l.at[1], opp, z)
    left_sum += lrecv[1]
    lbuf[...] = BETA2 * lbuf[...] + (1.0 - BETA2) * left_sum

    settle(waits)
    settle(late_waits)
    assert most[0] == NSEND, most[0]


def write_out(*refs):
    ins, outs, sem = refs[:5], refs[5:10], refs[10]
    copies = []
    for a, b in zip(ins, outs):
        step = a.shape[0] // 4
        for n in range(4):
            rows = pl.ds(n * step, step)
            copies.append(pltpu.make_async_copy(a.at[rows], b.at[rows], sem.at[len(copies)]))
    for cp in copies:
        cp.start()
    for cp in copies:
        cp.wait()


def solution(mesh):
    tile_spec = P(("layer", "row"), "col")

    def local_step(weight, grad_in, mom_first, mom_second, stat_left, stat_right, basis_left, basis_right):
        tr, tc = grad_in.shape
        tl = stat_left.shape[0]
        dma = pltpu.SemaphoreType.DMA
        scratch = [
            pltpu.VMEM((4, tr, tc), F32),
            pltpu.VMEM((4, tr, tc), BF16),
            pltpu.VMEM((4, tr, tc), F32),
            pltpu.VMEM((3, tr, tc), F32),
            pltpu.VMEM((4, tc, tc), BF16),
            pltpu.VMEM((4, tr, tc), BF16),
            pltpu.VMEM((4, tr, tc), BF16),
            pltpu.VMEM((4, 3, tr, tc), BF16),
            pltpu.VMEM((4, tr, tc), F32),
            pltpu.VMEM((5, tr, tc), F32),
            pltpu.VMEM((4, tl, tl), BF16),
            pltpu.VMEM((4, tl, tl), BF16),
            pltpu.VMEM((tr, tc), F32),
            pltpu.VMEM((tr, tc), BF16),
            pltpu.VMEM((tc, tc), BF16),
            pltpu.VMEM((tr, tc), BF16),
            pltpu.VMEM((tl, tl), F32),
            pltpu.VMEM((4, tl, tl), F32),
            pltpu.VMEM((3, tl, tl), F32),
            pltpu.VMEM((2, tc, 3 * tr), BF16),
            dma((NSEND,)),
            dma((11,)),
            dma((4,)), dma((4,)), dma((4,)),
            dma((4, NQ)), dma((4,)),
            dma((4, NH)), dma((4, NH)),
            dma((5,)), dma((4, 3)),
            dma((5, NU)), dma((3,)), dma((3,)),
        ]
        any_spec = pl.BlockSpec(memory_space=pl.ANY)
        vmem_spec = pl.BlockSpec(memory_space=pltpu.VMEM)
        outs = [weight, mom_first, mom_second, stat_left, stat_right]
        results = pl.pallas_call(
            kernel,
            name="soap_step",
            out_shape=[pltpu.VMEM(o.shape, o.dtype) for o in outs],
            in_specs=[any_spec] * 8,
            out_specs=[vmem_spec] * 5,
            scratch_shapes=scratch,
            compiler_params=pltpu.CompilerParams(
                collective_id=0, has_side_effects=True, vmem_limit_bytes=VMEM_BYTES,
            ),
        )(weight, grad_in, mom_first, mom_second, stat_left, stat_right, basis_left, basis_right)
        results = [pltpu.with_memory_space_constraint(r, pltpu.VMEM) for r in results]
        return pl.pallas_call(
            write_out,
            name="write_out",
            out_shape=[jax.ShapeDtypeStruct(o.shape, o.dtype) for o in outs],
            in_specs=[vmem_spec] * 5,
            out_specs=[any_spec] * 5,
            scratch_shapes=[dma((20,))],
            compiler_params=pltpu.CompilerParams(vmem_limit_bytes=2**20),
        )(*results)

    return jax.shard_map(local_step, mesh=mesh, in_specs=(tile_spec,) * 8, out_specs=(tile_spec,) * 5, check_vma=False)
```

```python
import jax
import jax.numpy as jnp
from jax import lax
from jax.experimental import pallas as pl
from jax.experimental.pallas import tpu as pltpu
from jax.sharding import PartitionSpec as P

BETA1 = 0.9
BETA2 = 0.9
EPS = 1e-8
LR = 0.1
STEP = 10
BIAS_ONE = 1.0 - BETA1 ** STEP
BIAS_TWO = 1.0 - BETA2 ** STEP

MESH = pl.DeviceIdType.MESH
F32 = jnp.float32
BF16 = jnp.bfloat16
NQ = 4
NH = 2
NU = 2
NG = 2
NDEV = 4
NSEND = 64
VMEM_BYTES = 56 * 2**20

ROWS_T = (((0,), (0,)), ((), ()))
COLS_T = (((1,), (1,)), ((), ()))


def split3(x):
    a0 = x.astype(BF16)
    r = x - a0.astype(F32)
    a1 = r.astype(BF16)
    a2 = (r - a1.astype(F32)).astype(BF16)
    return a0, a1, a2


def kernel(
    w_hbm, g_hbm, m_hbm, v_hbm, l_hbm, r_hbm, ql_hbm, qr_hbm,
    wbuf, mbuf, vbuf, lbuf, racc,
    grow, gbf, gi, gj, qrc, hcol, ncol, gis, ubuf, urecv,
    qlr, qlc, hacc, kb, qrx, kx, qlf, lx, lrecv, git,
    ssem, lsem, r_gbf, r_qlr, r_g32, r_qr, r_qlc, r_h, r_n, r_gj, r_gi, r_u, r_qx, r_l,
):
    lay = lax.axis_index("layer")
    z = lax.axis_index("col")
    i = lax.axis_index("row")
    y, c = i // 2, i % 2
    sib = 2 * y + (1 - c)
    opp = 2 * (1 - y) + c
    dia = 2 * (1 - y) + (1 - c)
    tr, tc = grow.shape[1], grow.shape[2]
    qrows = tc // NQ
    hcols = tc // NH
    urows = tr // NU
    grows = tr // NG
    head_rows = 3 * grows // 4
    gparts = (pl.ds(0, head_rows), pl.ds(head_rows, grows - head_rows), pl.ds(grows, grows))
    early = tc - tc // 4

    waits, qr_waits, late_waits, line_waits, far_waits = [], [], [], [], []
    unused, most = list(range(NSEND)), [0]

    def dev(row, col):
        return (lay, col, row)

    def send(src, dst, rsem, row, col, cond=None, held=None):
        src, dst, rsem = src(), dst(), rsem()
        n = unused.pop(0)
        most[0] = max(most[0], n + 1)

        def make():
            return pltpu.make_async_remote_copy(
                src_ref=src, dst_ref=dst, send_sem=ssem.at[n], recv_sem=rsem,
                device_id=dev(row, col), device_id_type=MESH,
            )

        def go():
            make().start()

        def done():
            make().wait_send()

        if cond is None:
            go()
        else:
            pl.when(cond)(go)
        if held is None:
            waits.append((cond, done, n))
        else:
            held.append((cond, done, n))

    def settle(sent):
        for cond, done, n in sent:
            if cond is None:
                done()
            else:
                pl.when(cond)(done)
            unused.append(n)
        unused.sort()
        sent.clear()

    def arrived(dst, rsem, row, col):
        pltpu.make_async_remote_copy(
            src_ref=dst, dst_ref=dst, send_sem=ssem.at[0], recv_sem=rsem,
            device_id=dev(row, col), device_id_type=MESH,
        ).wait_recv()

    loads = {}

    def load(name, n, src, dst):
        cp = pltpu.make_async_copy(src, dst, lsem.at[n])
        cp.start()
        loads[name] = cp

    for q in range(NQ):
        rows = pl.ds(q * qrows, qrows)
        load(("qr", q), 1 + q, qr_hbm.at[rows], racc.at[rows])
        if q == 0:
            load("g", 0, g_hbm, grow.at[z])
            load("ql", 5, ql_hbm, qlf)
    load("m", 6, m_hbm, mbuf)
    load("v", 7, v_hbm, vbuf)
    load("w", 8, w_hbm, wbuf)
    load("l", 9, l_hbm, lbuf)

    barrier = pltpu.get_barrier_semaphore()
    for row in (sib, opp, dia):
        pl.semaphore_signal(barrier, inc=1, device_id=dev(row, z), device_id_type=MESH)

    @pl.when(z > 0)
    def _():
        pl.semaphore_signal(barrier, inc=1, device_id=dev(i, z - 1), device_id_type=MESH)

    @pl.when(z < NDEV - 1)
    def _():
        pl.semaphore_signal(barrier, inc=1, device_id=dev(i, z + 1), device_id_type=MESH)

    def qr_cast(q):
        rows = pl.ds(q * qrows, qrows)
        loads[("qr", q)].wait()
        qrc[i, rows] = racc[rows].astype(BF16)

    qr_cast(0)
    inner = jnp.logical_and(z > 0, z < NDEV - 1)

    @pl.when(inner)
    def _():
        pl.semaphore_wait(barrier, 5)

    @pl.when(jnp.logical_not(inner))
    def _():
        pl.semaphore_wait(barrier, 4)

    def line_own(buf, rs, held=None):
        send(lambda: buf.at[z], lambda: buf.at[z], lambda: rs.at[z], i, z + 1, z < NDEV - 1, held)
        send(lambda: buf.at[z], lambda: buf.at[z], lambda: rs.at[z], i, z - 1, z > 0, held)

    def line_forward(buf, rs, s, held=None):
        right = jnp.logical_and(z >= s, z < NDEV - 1)
        left = jnp.logical_and(z + s < NDEV, z > 0)

        @pl.when(right)
        def _():
            arrived(buf.at[z - s], rs.at[z - s], i, z - 1)

        send(lambda: buf.at[z - s], lambda: buf.at[z - s], lambda: rs.at[z - s], i, z + 1, right, held)

        @pl.when(left)
        def _():
            arrived(buf.at[z + s], rs.at[z + s], i, z + 1)

        send(lambda: buf.at[z + s], lambda: buf.at[z + s], lambda: rs.at[z + s], i, z - 1, left, held)

    def line_last(buf, rs, s):
        @pl.when(jnp.logical_and(z >= s, z == NDEV - 1))
        def _():
            arrived(buf.at[z - s], rs.at[z - s], i, z - 1)

        @pl.when(jnp.logical_and(z + s < NDEV, z == 0))
        def _():
            arrived(buf.at[z + s], rs.at[z + s], i, z + 1)

    def qr_own(q):
        rows = pl.ds(q * qrows, qrows)
        for row in (opp, sib):
            send(lambda: qrc.at[i, rows], lambda: qrc.at[i, rows], lambda: r_qr.at[i, q], row, z, held=qr_waits)

    qr_own(0)
    loads["g"].wait()
    gbf[z] = grow[z].astype(BF16)
    line_own(gbf, r_gbf)
    loads["ql"].wait()
    qlr[z] = qlf[...].astype(BF16)
    qr_cast(1)
    line_own(qlr, r_qlr)
    for q in range(2, NQ):
        qr_cast(q)
        qr_own(q - 1)
    load("r", 10, r_hbm, racc)

    def qr_forward(q):
        rows = pl.ds(q * qrows, qrows)
        arrived(qrc.at[opp, rows], r_qr.at[opp, q], opp, z)
        send(lambda: qrc.at[opp, rows], lambda: qrc.at[opp, rows], lambda: r_qr.at[opp, q], sib, z, held=qr_waits)

    def h_add(k, q, first=False):
        rows = pl.ds(q * qrows, qrows)
        part = jnp.dot(gbf[k, :, rows], qrc[k, rows], preferred_element_type=F32)
        if first:
            hacc[...] = part
        else:
            hacc[...] += part

    qr_own(NQ - 1)

    line_forward(gbf, r_gbf, 1)
    line_forward(qlr, r_qlr, 1)
    qr_forward(0)
    line_forward(gbf, r_gbf, 2)
    line_forward(qlr, r_qlr, 2)
    line_own(grow, r_g32, line_waits)
    qr_forward(1)
    for s in range(1, NDEV):
        line_last(gbf, r_gbf, s)
        line_last(qlr, r_qlr, s)

    for row in (opp, dia, sib):
        send(lambda row=row: qlr.at[row], lambda: qlc.at[i], lambda: r_qlc.at[i], row, z)
    qlc[i] = qlr[i]

    for q in range(NQ):
        h_add(i, q, first=q == 0)
    for q in range(NQ):
        rows = pl.ds(q * qrows, qrows)
        arrived(qrc.at[sib, rows], r_qr.at[sib, q], sib, z)
        h_add(sib, q)
    qr_forward(2)
    for q in range(2):
        h_add(opp, q)
    for q in range(2):
        rows = pl.ds(q * qrows, qrows)
        arrived(qrc.at[dia, rows], r_qr.at[dia, q], sib, z)
        h_add(dia, q)
    h_add(opp, 2)
    qr_forward(3)
    h_add(opp, 3)
    for q in range(2, NQ):
        rows = pl.ds(q * qrows, qrows)
        arrived(qrc.at[dia, rows], r_qr.at[dia, q], sib, z)
        h_add(dia, q)

    def own_part(buf, rs, n):
        cols = pl.ds(n * hcols, hcols)
        for row in (opp, sib):
            send(lambda: buf.at[i, :, cols], lambda: buf.at[i, :, cols], lambda: rs.at[i, n], row, z)

    def forward_part(buf, rs, n):
        cols = pl.ds(n * hcols, hcols)
        arrived(buf.at[opp, :, cols], rs.at[opp, n], opp, z)
        send(lambda: buf.at[opp, :, cols], lambda: buf.at[opp, :, cols], lambda: rs.at[opp, n], sib, z)

    def rest_part(buf, rs, n):
        cols = pl.ds(n * hcols, hcols)
        arrived(buf.at[sib, :, cols], rs.at[sib, n], sib, z)
        arrived(buf.at[dia, :, cols], rs.at[dia, n], sib, z)

    hcol[i] = hacc[...].astype(BF16)
    for n in range(NH):
        own_part(hcol, r_h, n)

    half = pl.ds(pl.multiple_of(c * (tc // 2), tc // 2), tc // 2)
    other_half = pl.ds(pl.multiple_of((1 - c) * (tc // 2), tc // 2), tc // 2)
    send(lambda: qrc.at[1, half], lambda: qrx.at[half], lambda: r_qx.at[0], i, 1, z == 0, held=qr_waits)
    send(lambda: qrc.at[2, half], lambda: qrx.at[half], lambda: r_qx.at[0], i, 2, z == 3, held=qr_waits)

    early_waits = waits[:]
    waits.clear()

    line_forward(grow, r_g32, 1, line_waits)
    for row in (opp, dia, sib):
        arrived(qlc.at[row], r_qlc.at[row], row, z)
    loads["m"].wait()
    loads["v"].wait()

    for n in range(NH):
        cols = pl.ds(n * hcols, hcols)
        forward_part(hcol, r_h, n)
        rest_part(hcol, r_h, n)
        rotated = sum(
            lax.dot_general(qlc[k], hcol[k, :, cols], ROWS_T, preferred_element_type=F32) for k in range(NDEV)
        )
        hacc[:, cols] = rotated
        rotated = hacc[:, cols]
        new_first = BETA1 * mbuf[:, cols] + (1.0 - BETA1) * rotated
        new_second = BETA2 * vbuf[:, cols] + (1.0 - BETA2) * rotated * rotated
        mbuf[:, cols] = new_first
        vbuf[:, cols] = new_second
        direction = (new_first / BIAS_ONE) / (jnp.sqrt(new_second / BIAS_TWO) + EPS)
        ncol[i, :, cols] = direction.astype(BF16)
        own_part(ncol, r_n, n)
    def gj_part(src, slot, late):
        cols = pl.ds(early, tc - early) if late else pl.ds(0, early)
        n = slot + 2 * late
        return (lambda: src.at[:, cols]), (lambda: gj.at[slot, :, cols]), (lambda: r_gj.at[n])

    head = gparts[0]
    ahead = 1 - 2 * y

    def relay(station, came_row, came_col):
        @pl.when(z == station)
        def _():
            arrived(gi.at[opp, head], r_gi.at[opp, 0], came_row, came_col)

        send(lambda: gi.at[opp, head], lambda: gi.at[opp, head], lambda: r_gi.at[opp, 0], i, z + ahead, z == station)

    send(lambda: grow.at[opp, head], lambda: gi.at[i, head], lambda: r_gi.at[i, 0], opp, z, z == 2 - y)

    calm = y == z // 2
    dup = i == z
    send(*gj_part(grow.at[z], 1, False), opp, z)
    send(*gj_part(grow.at[z], 1, True), opp, z, jnp.logical_not(calm))
    send(lambda: grow.at[z], lambda: gj.at[0], lambda: r_gj.at[0], sib, z)

    def gi_send(b, valid, held=None):
        there = jnp.logical_and(valid, b != i)
        for n, rows in enumerate(gparts):
            cond = jnp.logical_and(there, jnp.logical_or(b != opp, z == 3 - 3 * y)) if n == 0 else there
            send(lambda: grow.at[b, rows], lambda: gi.at[i, rows], lambda: r_gi.at[i, n], b, z, cond, held)

    line_last(grow, r_g32, 1)
    gi_send(z - 1, z >= 1)
    gi_send(z + 1, z + 1 < NDEV)

    for n in range(NH):
        forward_part(ncol, r_n, n)
        rest_part(ncol, r_n, n)
        cols = pl.ds(n * hcols, hcols)
        kb[:, cols] = sum(
            jnp.dot(qlr[k], ncol[k, :, cols], preferred_element_type=F32) for k in range(NDEV)
        ).astype(BF16)

    settle(early_waits)

    def u_send(a, h, slot, col, cond):
        rows = pl.ds(h * urows, urows)
        send(lambda: ubuf.at[a, rows], lambda: urecv.at[slot, rows], lambda: r_u.at[slot, h], i, col, cond)

    def u_first(a, to_right):
        for h in range(NU):
            if to_right:
                u_send(a, h, a, z + 1, z == 0)
            else:
                u_send(a, h, NDEV if a == NDEV - 2 else a, z - 1, z == NDEV - 1)

    for piece, starts in ((3, ((3, True),)), (0, ((0, False),)), (2, ((2, True),)), (1, ((1, False),))):
        ubuf[piece] = lax.dot_general(kb[...], qrc[piece], COLS_T, preferred_element_type=F32)
        for a, to_right in starts:
            u_first(a, to_right)
    send(lambda: kb, lambda: kx, lambda: r_qx.at[2], i, 1, z == 0)
    send(lambda: kb, lambda: kx, lambda: r_qx.at[2], i, 2, z == 3)
    line_forward(grow, r_g32, 2, line_waits)

    relay(1 + y, opp, z)

    @pl.when(inner)
    def _():
        arrived(qrx.at[half], r_qx.at[0], i, 3 * (z // 2))

    send(lambda: qrx.at[half], lambda: qrx.at[half], lambda: r_qx.at[1], sib, z, inner)

    def u_at(a, h, station, to_right):
        rows = pl.ds(h * urows, urows)
        slot = NDEV if (not to_right and station == a) else a

        @pl.when(z == station)
        def _():
            arrived(urecv.at[slot, rows], r_u.at[slot, h], i, station - 1 if to_right else station + 1)
            ubuf[a, rows] += urecv[slot, rows]

        if station != a:
            nxt = station + 1 if to_right else station - 1
            nslot = NDEV if (not to_right and nxt == a) else a
            u_send(a, h, nslot, nxt, z == station)

    line_last(grow, r_g32, 2)
    gi_send(z - 2, z >= 2)
    gi_send(z + 2, z + 2 < NDEV)
    far = jnp.logical_or(jnp.logical_and(z == 0, i == 3), jnp.logical_and(z == 3, i == 0))

    def u_round(t):
        for h in range(NU):
            for a in (3, 2, 1):
                st = t - (3 - a)
                if 1 <= st <= a and a > 1:
                    u_at(a, h, st, True)
                    u_at(NDEV - 1 - a, h, NDEV - 1 - st, False)

    def gj_split(slot, ref, start=0, size=None):
        cols = pl.ds(start, size or tc)
        for t, term in enumerate(split3(ref[:, cols])):
            qrc[slot, pl.ds(t * tr, tr), cols] = term

    def gi_split(k, ref, n):
        rows = pl.ds(n * grows, grows)
        for t, term in enumerate(split3(ref[rows])):
            gis[k, t, rows] = term

    def right_add(blocks, n=None, start=0, size=None, first=False, unroll=1):
        begin, depth = (0, tr) if n is None else (n * grows, grows)
        cols = pl.ds(start, size or tc)

        def body(m, carry):
            rows = pl.ds(pl.multiple_of(m * tr, tr), tr)
            left, right = [], []
            for k, slot, turned in blocks:
                if turned is None:
                    a = [gis[k, t, pl.ds(begin, depth), rows].T for t in range(3)]
                else:
                    a = [git[turned, rows, pl.ds(t * tr + begin, depth)] for t in range(3)]
                b = [qrc[slot, pl.ds(t * tr + begin, depth), cols] for t in range(3)]
                left += [a[0], a[0], a[0], a[1], a[1], a[2]]
                right += [b[0], b[1], b[2], b[0], b[1], b[0]]
            left, right = jnp.concatenate(left, axis=1), jnp.concatenate(right, axis=0)
            share = (1.0 - BETA2) * jnp.dot(left, right, preferred_element_type=F32)
            old = racc[rows, cols]
            racc[rows, cols] = (BETA2 * old if first else old) + share
            return carry

        lax.fori_loop(0, tc // tr, body, 0, unroll=unroll)

    def gi_arrived(row, n, slot, turned=None):
        @pl.when(jnp.logical_not(dup))
        def _():
            if n == 1:
                arrived(gi.at[row, gparts[2]], r_gi.at[row, 2], row, z)
            else:
                arrived(gi.at[row, gparts[1]], r_gi.at[row, 1], row, z)
                if row is opp:
                    @pl.when(z == 3 * y)
                    def _():
                        arrived(gi.at[row, head], r_gi.at[row, 0], row, z)

                    @pl.when(z == 3 - 3 * y)
                    def _():
                        arrived(gi.at[row, head], r_gi.at[row, 0], i, z - ahead)
                else:
                    arrived(gi.at[row, head], r_gi.at[row, 0], row, z)
            gi_split(row, gi.at[row], n)

        @pl.when(dup)
        def _():
            gi_split(row, gj.at[slot], n)

        if turned is not None:
            for t in range(3):
                git[turned, :, pl.ds(t * tr + n * grows, grows)] = gis[row, t, pl.ds(n * grows, grows)].T

    def left_part(k, slot):
        pieces = [gis[k, t] for t in range(3)]
        other = [gis[z, t] for t in range(3)]
        total = None
        for t, u in ((0, 0), (0, 1), (1, 0), (1, 1), (0, 2), (2, 0)):
            d = lax.dot_general(pieces[t], other[u], COLS_T, preferred_element_type=F32)
            total = d if total is None else total + d
        lx[slot] = total

    settle(qr_waits)
    gj_split(0, grow.at[z])
    arrived(gj.at[0], r_gj.at[0], sib, z)
    gj_split(1, gj.at[0])
    loads["r"].wait()

    def chip_rows():
        for n in range(NG):
            gi_split(i, grow.at[i], n)
        right_add([(i, 0, None)], first=True)
        for n in range(NG):
            gi_arrived(sib, n, 0)
        right_add([(sib, 1, None)])

    pl.when(jnp.logical_not(far))(chip_rows)
    relay(2 - y, i, z - ahead)
    u_round(1)
    arrived(gj.at[1, :, pl.ds(0, early)], r_gj.at[1], opp, z)
    send(*gj_part(gj.at[1], 2, False), sib, z)
    gj_split(2, gj.at[1], 0, early)

    def gj_late_arrived():
        arrived(gj.at[1, :, pl.ds(early, tc - early)], r_gj.at[3], opp, z)

    line_last(grow, r_g32, 3)
    gi_send(z - 3, z >= 3, far_waits)
    gi_send(z + 3, z + 3 < NDEV, far_waits)
    send(*gj_part(grow.at[z], 1, True), opp, z, jnp.logical_and(calm, inner), held=late_waits)
    pl.when(calm)(gj_late_arrived)
    send(*gj_part(gj.at[1], 2, True), sib, z, calm)

    @pl.when(calm)
    def _():
        gj_split(2, gj.at[1], early, tc - early)

    arrived(gj.at[2, :, pl.ds(0, early)], r_gj.at[2], sib, z)
    gj_split(3, gj.at[2], 0, early)

    def gj_last_arrived():
        arrived(gj.at[2, :, pl.ds(early, tc - early)], r_gj.at[4], sib, z)
        gj_split(3, gj.at[2], early, tc - early)

    pl.when(calm)(gj_last_arrived)
    pl.when(far)(chip_rows)
    u_round(2)
    others = [(opp, 2, 0), (dia, 3, 1)]
    for n in range(NG - 1):
        gi_arrived(opp, n, 1, 0)
        gi_arrived(dia, n, 2, 1)
        right_add(others, n, 0, early)

    loads["w"].wait()
    loads["l"].wait()
    gi_arrived(dia, NG - 1, 2, 1)
    gi_arrived(opp, NG - 1, 1, 0)

    left_part(dia, 3)
    settle(far_waits)
    send(lambda: lx.at[3], lambda: lrecv.at[2], lambda: r_l.at[2], sib, z)
    left_part(opp, 2)
    arrived(lrecv.at[2], r_l.at[2], sib, z)
    send(*gj_part(grow.at[z], 1, True), opp, z, jnp.logical_and(calm, jnp.logical_not(inner)), held=late_waits)
    lx[2] += lrecv[2]
    send(lambda: lx.at[2], lambda: lrecv.at[1], lambda: r_l.at[1], opp, z, held=late_waits)
    left_part(sib, 1)
    send(lambda: lx.at[1], lambda: lrecv.at[0], lambda: r_l.at[0], sib, z, held=late_waits)
    left_part(i, 0)
    right_add(others, NG - 1, 0, early)
    pl.when(jnp.logical_not(calm))(gj_late_arrived)
    send(*gj_part(gj.at[1], 2, True), sib, z, jnp.logical_not(calm), held=late_waits)

    @pl.when(jnp.logical_not(calm))
    def _():
        gj_split(2, gj.at[1], early, tc - early)

    @pl.when(inner)
    def _():
        arrived(qrx.at[other_half], r_qx.at[1], sib, z)
        arrived(kx, r_qx.at[2], i, 3 * (z // 2))
        ubuf[z] += lax.dot_general(kx[...], qrx[...], COLS_T, preferred_element_type=F32)

    pl.when(jnp.logical_not(calm))(gj_last_arrived)
    right_add(others, None, early, tc - early, unroll=2)
    u_round(3)
    wbuf[...] = wbuf[...] - LR * ubuf[z]
    settle(waits)
    settle(line_waits)
    arrived(lrecv.at[0], r_l.at[0], sib, z)
    left_sum = lx[0] + lrecv[0]
    arrived(lrecv.at[1], r_l.at[1], opp, z)
    left_sum += lrecv[1]
    lbuf[...] = BETA2 * lbuf[...] + (1.0 - BETA2) * left_sum

    settle(waits)
    settle(late_waits)
    assert most[0] == NSEND, most[0]


def write_out(*refs):
    ins, outs, sem = refs[:5], refs[5:10], refs[10]
    copies = []
    for a, b in zip(ins, outs):
        step = a.shape[0] // 4
        for n in range(4):
            rows = pl.ds(n * step, step)
            copies.append(pltpu.make_async_copy(a.at[rows], b.at[rows], sem.at[len(copies)]))
    for cp in copies:
        cp.start()
    for cp in copies:
        cp.wait()


def solution(mesh):
    tile_spec = P(("layer", "row"), "col")

    def local_step(weight, grad_in, mom_first, mom_second, stat_left, stat_right, basis_left, basis_right):
        tr, tc = grad_in.shape
        tl = stat_left.shape[0]
        dma = pltpu.SemaphoreType.DMA
        scratch = [
            pltpu.VMEM((4, tr, tc), F32),
            pltpu.VMEM((4, tr, tc), BF16),
            pltpu.VMEM((4, tr, tc), F32),
            pltpu.VMEM((3, tr, tc), F32),
            pltpu.VMEM((4, tc, tc), BF16),
            pltpu.VMEM((4, tr, tc), BF16),
            pltpu.VMEM((4, tr, tc), BF16),
            pltpu.VMEM((4, 3, tr, tc), BF16),
            pltpu.VMEM((4, tr, tc), F32),
            pltpu.VMEM((5, tr, tc), F32),
            pltpu.VMEM((4, tl, tl), BF16),
            pltpu.VMEM((4, tl, tl), BF16),
            pltpu.VMEM((tr, tc), F32),
            pltpu.VMEM((tr, tc), BF16),
            pltpu.VMEM((tc, tc), BF16),
            pltpu.VMEM((tr, tc), BF16),
            pltpu.VMEM((tl, tl), F32),
            pltpu.VMEM((4, tl, tl), F32),
            pltpu.VMEM((3, tl, tl), F32),
            pltpu.VMEM((2, tc, 3 * tr), BF16),
            dma((NSEND,)),
            dma((11,)),
            dma((4,)), dma((4,)), dma((4,)),
            dma((4, NQ)), dma((4,)),
            dma((4, NH)), dma((4, NH)),
            dma((5,)), dma((4, 3)),
            dma((5, NU)), dma((3,)), dma((3,)),
        ]
        any_spec = pl.BlockSpec(memory_space=pl.ANY)
        vmem_spec = pl.BlockSpec(memory_space=pltpu.VMEM)
        outs = [weight, mom_first, mom_second, stat_left, stat_right]
        results = pl.pallas_call(
            kernel,
            name="soap_step",
            out_shape=[pltpu.VMEM(o.shape, o.dtype) for o in outs],
            in_specs=[any_spec] * 8,
            out_specs=[vmem_spec] * 5,
            scratch_shapes=scratch,
            compiler_params=pltpu.CompilerParams(
                collective_id=0, has_side_effects=True, vmem_limit_bytes=VMEM_BYTES,
            ),
        )(weight, grad_in, mom_first, mom_second, stat_left, stat_right, basis_left, basis_right)
        results = [pltpu.with_memory_space_constraint(r, pltpu.VMEM) for r in results]
        return pl.pallas_call(
            write_out,
            name="write_out",
            out_shape=[jax.ShapeDtypeStruct(o.shape, o.dtype) for o in outs],
            in_specs=[vmem_spec] * 5,
            out_specs=[any_spec] * 5,
            scratch_shapes=[dma((20,))],
            compiler_params=pltpu.CompilerParams(vmem_limit_bytes=2**20),
        )(*results)

    return jax.shard_map(local_step, mesh=mesh, in_specs=(tile_spec,) * 8, out_specs=(tile_spec,) * 5, check_vma=False)
```

```python
import jax
import jax.numpy as jnp
from jax import lax
from jax.experimental import pallas as pl
from jax.experimental.pallas import tpu as pltpu
from jax.sharding import PartitionSpec as P

BETA1 = 0.9
BETA2 = 0.9
EPS = 1e-8
LR = 0.1
STEP = 10
BIAS_ONE = 1.0 - BETA1 ** STEP
BIAS_TWO = 1.0 - BETA2 ** STEP

MESH = pl.DeviceIdType.MESH
F32 = jnp.float32
BF16 = jnp.bfloat16
NQ = 4
NH = 2
NU = 2
NG = 2
NDEV = 4
NSEND = 64
VMEM_BYTES = 56 * 2**20

ROWS_T = (((0,), (0,)), ((), ()))
COLS_T = (((1,), (1,)), ((), ()))


def split3(x):
    a0 = x.astype(BF16)
    r = x - a0.astype(F32)
    a1 = r.astype(BF16)
    a2 = (r - a1.astype(F32)).astype(BF16)
    return a0, a1, a2


def kernel(
    w_hbm, g_hbm, m_hbm, v_hbm, l_hbm, r_hbm, ql_hbm, qr_hbm,
    wbuf, mbuf, vbuf, lbuf, racc,
    grow, gbf, gi, gj, qrc, hcol, ncol, gis, ubuf, urecv,
    qlr, qlc, hacc, kb, qrx, kx, qlf, lx, lrecv, git,
    ssem, lsem, r_gbf, r_qlr, r_g32, r_qr, r_qlc, r_h, r_n, r_gj, r_gi, r_u, r_qx, r_l,
):
    lay = lax.axis_index("layer")
    z = lax.axis_index("col")
    i = lax.axis_index("row")
    y, c = i // 2, i % 2
    sib = 2 * y + (1 - c)
    opp = 2 * (1 - y) + c
    dia = 2 * (1 - y) + (1 - c)
    tr, tc = grow.shape[1], grow.shape[2]
    qrows = tc // NQ
    hcols = tc // NH
    urows = tr // NU
    grows = tr // NG
    head_rows = 3 * grows // 4
    gparts = (pl.ds(0, head_rows), pl.ds(head_rows, grows - head_rows), pl.ds(grows, grows))
    early = tc - tc // 4

    waits, qr_waits, late_waits, line_waits, far_waits = [], [], [], [], []
    unused, most = list(range(NSEND)), [0]

    def dev(row, col):
        return (lay, col, row)

    def send(src, dst, rsem, row, col, cond=None, held=None):
        src, dst, rsem = src(), dst(), rsem()
        n = unused.pop(0)
        most[0] = max(most[0], n + 1)

        def make():
            return pltpu.make_async_remote_copy(
                src_ref=src, dst_ref=dst, send_sem=ssem.at[n], recv_sem=rsem,
                device_id=dev(row, col), device_id_type=MESH,
            )

        def go():
            make().start()

        def done():
            make().wait_send()

        if cond is None:
            go()
        else:
            pl.when(cond)(go)
        if held is None:
            waits.append((cond, done, n))
        else:
            held.append((cond, done, n))

    def settle(sent):
        for cond, done, n in sent:
            if cond is None:
                done()
            else:
                pl.when(cond)(done)
            unused.append(n)
        unused.sort()
        sent.clear()

    def arrived(dst, rsem, row, col):
        pltpu.make_async_remote_copy(
            src_ref=dst, dst_ref=dst, send_sem=ssem.at[0], recv_sem=rsem,
            device_id=dev(row, col), device_id_type=MESH,
        ).wait_recv()

    loads = {}

    def load(name, n, src, dst):
        cp = pltpu.make_async_copy(src, dst, lsem.at[n])
        cp.start()
        loads[name] = cp

    for q in range(NQ):
        rows = pl.ds(q * qrows, qrows)
        load(("qr", q), 1 + q, qr_hbm.at[rows], racc.at[rows])
        if q == 0:
            load("g", 0, g_hbm, grow.at[z])
            load("ql", 5, ql_hbm, qlf)
    load("m", 6, m_hbm, mbuf)
    load("v", 7, v_hbm, vbuf)
    load("w", 8, w_hbm, wbuf)
    load("l", 9, l_hbm, lbuf)

    barrier = pltpu.get_barrier_semaphore()
    for row in (sib, opp, dia):
        pl.semaphore_signal(barrier, inc=1, device_id=dev(row, z), device_id_type=MESH)

    @pl.when(z > 0)
    def _():
        pl.semaphore_signal(barrier, inc=1, device_id=dev(i, z - 1), device_id_type=MESH)

    @pl.when(z < NDEV - 1)
    def _():
        pl.semaphore_signal(barrier, inc=1, device_id=dev(i, z + 1), device_id_type=MESH)

    def qr_cast(q):
        rows = pl.ds(q * qrows, qrows)
        loads[("qr", q)].wait()
        qrc[i, rows] = racc[rows].astype(BF16)

    qr_cast(0)
    inner = jnp.logical_and(z > 0, z < NDEV - 1)

    @pl.when(inner)
    def _():
        pl.semaphore_wait(barrier, 5)

    @pl.when(jnp.logical_not(inner))
    def _():
        pl.semaphore_wait(barrier, 4)

    def line_own(buf, rs, held=None):
        send(lambda: buf.at[z], lambda: buf.at[z], lambda: rs.at[z], i, z + 1, z < NDEV - 1, held)
        send(lambda: buf.at[z], lambda: buf.at[z], lambda: rs.at[z], i, z - 1, z > 0, held)

    def line_forward(buf, rs, s, held=None):
        right = jnp.logical_and(z >= s, z < NDEV - 1)
        left = jnp.logical_and(z + s < NDEV, z > 0)

        @pl.when(right)
        def _():
            arrived(buf.at[z - s], rs.at[z - s], i, z - 1)

        send(lambda: buf.at[z - s], lambda: buf.at[z - s], lambda: rs.at[z - s], i, z + 1, right, held)

        @pl.when(left)
        def _():
            arrived(buf.at[z + s], rs.at[z + s], i, z + 1)

        send(lambda: buf.at[z + s], lambda: buf.at[z + s], lambda: rs.at[z + s], i, z - 1, left, held)

    def line_last(buf, rs, s):
        @pl.when(jnp.logical_and(z >= s, z == NDEV - 1))
        def _():
            arrived(buf.at[z - s], rs.at[z - s], i, z - 1)

        @pl.when(jnp.logical_and(z + s < NDEV, z == 0))
        def _():
            arrived(buf.at[z + s], rs.at[z + s], i, z + 1)

    def qr_own(q):
        rows = pl.ds(q * qrows, qrows)
        for row in (opp, sib):
            send(lambda: qrc.at[i, rows], lambda: qrc.at[i, rows], lambda: r_qr.at[i, q], row, z, held=qr_waits)

    qr_own(0)
    loads["g"].wait()
    gbf[z] = grow[z].astype(BF16)
    line_own(gbf, r_gbf)
    loads["ql"].wait()
    qlr[z] = qlf[...].astype(BF16)
    qr_cast(1)
    line_own(qlr, r_qlr)
    for q in range(2, NQ):
        qr_cast(q)
        qr_own(q - 1)
    load("r", 10, r_hbm, racc)

    def qr_forward(q):
        rows = pl.ds(q * qrows, qrows)
        arrived(qrc.at[opp, rows], r_qr.at[opp, q], opp, z)
        send(lambda: qrc.at[opp, rows], lambda: qrc.at[opp, rows], lambda: r_qr.at[opp, q], sib, z, held=qr_waits)

    def h_add(k, q, first=False):
        rows = pl.ds(q * qrows, qrows)
        part = jnp.dot(gbf[k, :, rows], qrc[k, rows], preferred_element_type=F32)
        if first:
            hacc[...] = part
        else:
            hacc[...] += part

    qr_own(NQ - 1)

    line_forward(gbf, r_gbf, 1)
    line_forward(qlr, r_qlr, 1)
    qr_forward(0)
    line_forward(gbf, r_gbf, 2)
    line_forward(qlr, r_qlr, 2)
    line_own(grow, r_g32, line_waits)
    qr_forward(1)
    for s in range(1, NDEV):
        line_last(gbf, r_gbf, s)
        line_last(qlr, r_qlr, s)

    for row in (opp, dia, sib):
        send(lambda row=row: qlr.at[row], lambda: qlc.at[i], lambda: r_qlc.at[i], row, z)
    qlc[i] = qlr[i]

    for q in range(NQ):
        h_add(i, q, first=q == 0)
    for q in range(NQ):
        rows = pl.ds(q * qrows, qrows)
        arrived(qrc.at[sib, rows], r_qr.at[sib, q], sib, z)
        h_add(sib, q)
    qr_forward(2)
    for q in range(2):
        h_add(opp, q)
    for q in range(2):
        rows = pl.ds(q * qrows, qrows)
        arrived(qrc.at[dia, rows], r_qr.at[dia, q], sib, z)
        h_add(dia, q)
    h_add(opp, 2)
    qr_forward(3)
    h_add(opp, 3)
    for q in range(2, NQ):
        rows = pl.ds(q * qrows, qrows)
        arrived(qrc.at[dia, rows], r_qr.at[dia, q], sib, z)
        h_add(dia, q)

    def own_part(buf, rs, n):
        cols = pl.ds(n * hcols, hcols)
        for row in (opp, sib):
            send(lambda: buf.at[i, :, cols], lambda: buf.at[i, :, cols], lambda: rs.at[i, n], row, z)

    def forward_part(buf, rs, n):
        cols = pl.ds(n * hcols, hcols)
        arrived(buf.at[opp, :, cols], rs.at[opp, n], opp, z)
        send(lambda: buf.at[opp, :, cols], lambda: buf.at[opp, :, cols], lambda: rs.at[opp, n], sib, z)

    def rest_part(buf, rs, n):
        cols = pl.ds(n * hcols, hcols)
        arrived(buf.at[sib, :, cols], rs.at[sib, n], sib, z)
        arrived(buf.at[dia, :, cols], rs.at[dia, n], sib, z)

    hcol[i] = hacc[...].astype(BF16)
    for n in range(NH):
        own_part(hcol, r_h, n)

    half = pl.ds(pl.multiple_of(c * (tc // 2), tc // 2), tc // 2)
    other_half = pl.ds(pl.multiple_of((1 - c) * (tc // 2), tc // 2), tc // 2)
    send(lambda: qrc.at[1, half], lambda: qrx.at[half], lambda: r_qx.at[0], i, 1, z == 0, held=qr_waits)
    send(lambda: qrc.at[2, half], lambda: qrx.at[half], lambda: r_qx.at[0], i, 2, z == 3, held=qr_waits)

    early_waits = waits[:]
    waits.clear()

    line_forward(grow, r_g32, 1, line_waits)
    for row in (opp, dia, sib):
        arrived(qlc.at[row], r_qlc.at[row], row, z)
    loads["m"].wait()
    loads["v"].wait()

    for n in range(NH):
        cols = pl.ds(n * hcols, hcols)
        forward_part(hcol, r_h, n)
        rest_part(hcol, r_h, n)
        rotated = sum(
            lax.dot_general(qlc[k], hcol[k, :, cols], ROWS_T, preferred_element_type=F32) for k in range(NDEV)
        )
        hacc[:, cols] = rotated
        rotated = hacc[:, cols]
        new_first = BETA1 * mbuf[:, cols] + (1.0 - BETA1) * rotated
        new_second = BETA2 * vbuf[:, cols] + (1.0 - BETA2) * rotated * rotated
        mbuf[:, cols] = new_first
        vbuf[:, cols] = new_second
        direction = (new_first / BIAS_ONE) / (jnp.sqrt(new_second / BIAS_TWO) + EPS)
        ncol[i, :, cols] = direction.astype(BF16)
        own_part(ncol, r_n, n)
    def gj_part(src, slot, late):
        cols = pl.ds(early, tc - early) if late else pl.ds(0, early)
        n = slot + 2 * late
        return (lambda: src.at[:, cols]), (lambda: gj.at[slot, :, cols]), (lambda: r_gj.at[n])

    head = gparts[0]
    ahead = 1 - 2 * y

    def relay(station, came_row, came_col):
        @pl.when(z == station)
        def _():
            arrived(gi.at[opp, head], r_gi.at[opp, 0], came_row, came_col)

        send(lambda: gi.at[opp, head], lambda: gi.at[opp, head], lambda: r_gi.at[opp, 0], i, z + ahead, z == station)

    send(lambda: grow.at[opp, head], lambda: gi.at[i, head], lambda: r_gi.at[i, 0], opp, z, z == 2 - y)

    calm = y == z // 2
    dup = i == z
    send(*gj_part(grow.at[z], 1, False), opp, z)
    send(*gj_part(grow.at[z], 1, True), opp, z, jnp.logical_not(calm))
    send(lambda: grow.at[z], lambda: gj.at[0], lambda: r_gj.at[0], sib, z)

    def gi_send(b, valid, held=None):
        there = jnp.logical_and(valid, b != i)
        for n, rows in enumerate(gparts):
            cond = jnp.logical_and(there, jnp.logical_or(b != opp, z == 3 - 3 * y)) if n == 0 else there
            send(lambda: grow.at[b, rows], lambda: gi.at[i, rows], lambda: r_gi.at[i, n], b, z, cond, held)

    line_last(grow, r_g32, 1)
    gi_send(z - 1, z >= 1)
    gi_send(z + 1, z + 1 < NDEV)

    for n in range(NH):
        forward_part(ncol, r_n, n)
        rest_part(ncol, r_n, n)
        cols = pl.ds(n * hcols, hcols)
        kb[:, cols] = sum(
            jnp.dot(qlr[k], ncol[k, :, cols], preferred_element_type=F32) for k in range(NDEV)
        ).astype(BF16)

    settle(early_waits)

    def u_send(a, h, slot, col, cond):
        rows = pl.ds(h * urows, urows)
        send(lambda: ubuf.at[a, rows], lambda: urecv.at[slot, rows], lambda: r_u.at[slot, h], i, col, cond)

    def u_first(a, to_right):
        for h in range(NU):
            if to_right:
                u_send(a, h, a, z + 1, z == 0)
            else:
                u_send(a, h, NDEV if a == NDEV - 2 else a, z - 1, z == NDEV - 1)

    for piece, starts in ((3, ((3, True),)), (0, ((0, False),)), (2, ((2, True),)), (1, ((1, False),))):
        ubuf[piece] = lax.dot_general(kb[...], qrc[piece], COLS_T, preferred_element_type=F32)
        for a, to_right in starts:
            u_first(a, to_right)
    send(lambda: kb, lambda: kx, lambda: r_qx.at[2], i, 1, z == 0)
    send(lambda: kb, lambda: kx, lambda: r_qx.at[2], i, 2, z == 3)
    line_forward(grow, r_g32, 2, line_waits)

    relay(1 + y, opp, z)

    @pl.when(inner)
    def _():
        arrived(qrx.at[half], r_qx.at[0], i, 3 * (z // 2))

    send(lambda: qrx.at[half], lambda: qrx.at[half], lambda: r_qx.at[1], sib, z, inner)

    def u_at(a, h, station, to_right):
        rows = pl.ds(h * urows, urows)
        slot = NDEV if (not to_right and station == a) else a

        @pl.when(z == station)
        def _():
            arrived(urecv.at[slot, rows], r_u.at[slot, h], i, station - 1 if to_right else station + 1)
            ubuf[a, rows] += urecv[slot, rows]

        if station != a:
            nxt = station + 1 if to_right else station - 1
            nslot = NDEV if (not to_right and nxt == a) else a
            u_send(a, h, nslot, nxt, z == station)

    line_last(grow, r_g32, 2)
    gi_send(z - 2, z >= 2)
    gi_send(z + 2, z + 2 < NDEV)
    far = jnp.logical_or(jnp.logical_and(z == 0, i == 3), jnp.logical_and(z == 3, i == 0))

    def u_round(t):
        for h in range(NU):
            for a in (3, 2, 1):
                st = t - (3 - a)
                if 1 <= st <= a and a > 1:
                    u_at(a, h, st, True)
                    u_at(NDEV - 1 - a, h, NDEV - 1 - st, False)

    def gj_split(slot, ref, start=0, size=None):
        cols = pl.ds(start, size or tc)
        for t, term in enumerate(split3(ref[:, cols])):
            qrc[slot, pl.ds(t * tr, tr), cols] = term

    def gi_split(k, ref, n):
        rows = pl.ds(n * grows, grows)
        for t, term in enumerate(split3(ref[rows])):
            gis[k, t, rows] = term

    def right_add(blocks, n=None, start=0, size=None, first=False, unroll=1):
        begin, depth = (0, tr) if n is None else (n * grows, grows)
        cols = pl.ds(start, size or tc)

        def body(m, carry):
            rows = pl.ds(pl.multiple_of(m * tr, tr), tr)
            left, right = [], []
            for k, slot, turned in blocks:
                if turned is None:
                    a = [gis[k, t, pl.ds(begin, depth), rows].T for t in range(3)]
                else:
                    a = [git[turned, rows, pl.ds(t * tr + begin, depth)] for t in range(3)]
                b = [qrc[slot, pl.ds(t * tr + begin, depth), cols] for t in range(3)]
                left += [a[0], a[0], a[0], a[1], a[1], a[2]]
                right += [b[0], b[1], b[2], b[0], b[1], b[0]]
            left, right = jnp.concatenate(left, axis=1), jnp.concatenate(right, axis=0)
            share = (1.0 - BETA2) * jnp.dot(left, right, preferred_element_type=F32)
            old = racc[rows, cols]
            racc[rows, cols] = (BETA2 * old if first else old) + share
            return carry

        lax.fori_loop(0, tc // tr, body, 0, unroll=unroll)

    def gi_arrived(row, n, slot, turned=None):
        @pl.when(jnp.logical_not(dup))
        def _():
            if n == 1:
                arrived(gi.at[row, gparts[2]], r_gi.at[row, 2], row, z)
            else:
                arrived(gi.at[row, gparts[1]], r_gi.at[row, 1], row, z)
                if row is opp:
                    @pl.when(z == 3 * y)
                    def _():
                        arrived(gi.at[row, head], r_gi.at[row, 0], row, z)

                    @pl.when(z == 3 - 3 * y)
                    def _():
                        arrived(gi.at[row, head], r_gi.at[row, 0], i, z - ahead)
                else:
                    arrived(gi.at[row, head], r_gi.at[row, 0], row, z)
            gi_split(row, gi.at[row], n)

        @pl.when(dup)
        def _():
            gi_split(row, gj.at[slot], n)

        if turned is not None:
            for t in range(3):
                git[turned, :, pl.ds(t * tr + n * grows, grows)] = gis[row, t, pl.ds(n * grows, grows)].T

    def left_part(k, slot):
        pieces = [gis[k, t] for t in range(3)]
        other = [gis[z, t] for t in range(3)]
        d0, d1, d2 = [
            lax.dot_general(jnp.concatenate(pieces[:3 - u], axis=0), other[u], COLS_T, preferred_element_type=F32)
            for u in range(3)
        ]
        total = ((d0[:tr] + d0[tr:2 * tr]) + (d1[:tr] + d1[tr:])) + (d0[2 * tr:] + d2)
        lx[slot] = total

    settle(qr_waits)
    gj_split(0, grow.at[z])
    arrived(gj.at[0], r_gj.at[0], sib, z)
    gj_split(1, gj.at[0])
    loads["r"].wait()

    def chip_rows():
        for n in range(NG):
            gi_split(i, grow.at[i], n)
        right_add([(i, 0, None)], first=True)
        for n in range(NG):
            gi_arrived(sib, n, 0)
        right_add([(sib, 1, None)])

    pl.when(jnp.logical_not(far))(chip_rows)
    relay(2 - y, i, z - ahead)
    u_round(1)
    arrived(gj.at[1, :, pl.ds(0, early)], r_gj.at[1], opp, z)
    send(*gj_part(gj.at[1], 2, False), sib, z)
    gj_split(2, gj.at[1], 0, early)

    def gj_late_arrived():
        arrived(gj.at[1, :, pl.ds(early, tc - early)], r_gj.at[3], opp, z)

    line_last(grow, r_g32, 3)
    gi_send(z - 3, z >= 3, far_waits)
    gi_send(z + 3, z + 3 < NDEV, far_waits)
    send(*gj_part(grow.at[z], 1, True), opp, z, jnp.logical_and(calm, inner), held=late_waits)
    pl.when(calm)(gj_late_arrived)
    send(*gj_part(gj.at[1], 2, True), sib, z, calm)

    @pl.when(calm)
    def _():
        gj_split(2, gj.at[1], early, tc - early)

    arrived(gj.at[2, :, pl.ds(0, early)], r_gj.at[2], sib, z)
    gj_split(3, gj.at[2], 0, early)

    def gj_last_arrived():
        arrived(gj.at[2, :, pl.ds(early, tc - early)], r_gj.at[4], sib, z)
        gj_split(3, gj.at[2], early, tc - early)

    pl.when(calm)(gj_last_arrived)
    pl.when(far)(chip_rows)
    u_round(2)
    others = [(opp, 2, 0), (dia, 3, 1)]
    for n in range(NG - 1):
        gi_arrived(opp, n, 1, 0)
        gi_arrived(dia, n, 2, 1)
        right_add(others, n, 0, early)

    loads["w"].wait()
    loads["l"].wait()
    gi_arrived(dia, NG - 1, 2, 1)
    gi_arrived(opp, NG - 1, 1, 0)

    left_part(dia, 3)
    settle(far_waits)
    send(lambda: lx.at[3], lambda: lrecv.at[2], lambda: r_l.at[2], sib, z)
    left_part(opp, 2)
    arrived(lrecv.at[2], r_l.at[2], sib, z)
    send(*gj_part(grow.at[z], 1, True), opp, z, jnp.logical_and(calm, jnp.logical_not(inner)), held=late_waits)
    lx[2] += lrecv[2]
    send(lambda: lx.at[2], lambda: lrecv.at[1], lambda: r_l.at[1], opp, z, held=late_waits)
    left_part(sib, 1)
    send(lambda: lx.at[1], lambda: lrecv.at[0], lambda: r_l.at[0], sib, z, held=late_waits)
    left_part(i, 0)
    right_add(others, NG - 1, 0, early)
    pl.when(jnp.logical_not(calm))(gj_late_arrived)
    send(*gj_part(gj.at[1], 2, True), sib, z, jnp.logical_not(calm), held=late_waits)

    @pl.when(jnp.logical_not(calm))
    def _():
        gj_split(2, gj.at[1], early, tc - early)

    @pl.when(inner)
    def _():
        arrived(qrx.at[other_half], r_qx.at[1], sib, z)
        arrived(kx, r_qx.at[2], i, 3 * (z // 2))
        ubuf[z] += lax.dot_general(kx[...], qrx[...], COLS_T, preferred_element_type=F32)

    pl.when(jnp.logical_not(calm))(gj_last_arrived)
    right_add(others, None, early, tc - early, unroll=2)
    u_round(3)
    wbuf[...] = wbuf[...] - LR * ubuf[z]
    settle(waits)
    settle(line_waits)
    arrived(lrecv.at[0], r_l.at[0], sib, z)
    left_sum = lx[0] + lrecv[0]
    arrived(lrecv.at[1], r_l.at[1], opp, z)
    left_sum += lrecv[1]
    lbuf[...] = BETA2 * lbuf[...] + (1.0 - BETA2) * left_sum

    settle(waits)
    settle(late_waits)
    assert most[0] == NSEND, most[0]


def write_out(*refs):
    ins, outs, sem = refs[:5], refs[5:10], refs[10]
    copies = []
    for a, b in zip(ins, outs):
        step = a.shape[0] // 4
        for n in range(4):
            rows = pl.ds(n * step, step)
            copies.append(pltpu.make_async_copy(a.at[rows], b.at[rows], sem.at[len(copies)]))
    for cp in copies:
        cp.start()
    for cp in copies:
        cp.wait()


def solution(mesh):
    tile_spec = P(("layer", "row"), "col")

    def local_step(weight, grad_in, mom_first, mom_second, stat_left, stat_right, basis_left, basis_right):
        tr, tc = grad_in.shape
        tl = stat_left.shape[0]
        dma = pltpu.SemaphoreType.DMA
        scratch = [
            pltpu.VMEM((4, tr, tc), F32),
            pltpu.VMEM((4, tr, tc), BF16),
            pltpu.VMEM((4, tr, tc), F32),
            pltpu.VMEM((3, tr, tc), F32),
            pltpu.VMEM((4, tc, tc), BF16),
            pltpu.VMEM((4, tr, tc), BF16),
            pltpu.VMEM((4, tr, tc), BF16),
            pltpu.VMEM((4, 3, tr, tc), BF16),
            pltpu.VMEM((4, tr, tc), F32),
            pltpu.VMEM((5, tr, tc), F32),
            pltpu.VMEM((4, tl, tl), BF16),
            pltpu.VMEM((4, tl, tl), BF16),
            pltpu.VMEM((tr, tc), F32),
            pltpu.VMEM((tr, tc), BF16),
            pltpu.VMEM((tc, tc), BF16),
            pltpu.VMEM((tr, tc), BF16),
            pltpu.VMEM((tl, tl), F32),
            pltpu.VMEM((4, tl, tl), F32),
            pltpu.VMEM((3, tl, tl), F32),
            pltpu.VMEM((2, tc, 3 * tr), BF16),
            dma((NSEND,)),
            dma((11,)),
            dma((4,)), dma((4,)), dma((4,)),
            dma((4, NQ)), dma((4,)),
            dma((4, NH)), dma((4, NH)),
            dma((5,)), dma((4, 3)),
            dma((5, NU)), dma((3,)), dma((3,)),
        ]
        any_spec = pl.BlockSpec(memory_space=pl.ANY)
        vmem_spec = pl.BlockSpec(memory_space=pltpu.VMEM)
        outs = [weight, mom_first, mom_second, stat_left, stat_right]
        results = pl.pallas_call(
            kernel,
            name="soap_step",
            out_shape=[pltpu.VMEM(o.shape, o.dtype) for o in outs],
            in_specs=[any_spec] * 8,
            out_specs=[vmem_spec] * 5,
            scratch_shapes=scratch,
            compiler_params=pltpu.CompilerParams(
                collective_id=0, has_side_effects=True, vmem_limit_bytes=VMEM_BYTES,
            ),
        )(weight, grad_in, mom_first, mom_second, stat_left, stat_right, basis_left, basis_right)
        results = [pltpu.with_memory_space_constraint(r, pltpu.VMEM) for r in results]
        return pl.pallas_call(
            write_out,
            name="write_out",
            out_shape=[jax.ShapeDtypeStruct(o.shape, o.dtype) for o in outs],
            in_specs=[vmem_spec] * 5,
            out_specs=[any_spec] * 5,
            scratch_shapes=[dma((20,))],
            compiler_params=pltpu.CompilerParams(vmem_limit_bytes=2**20),
        )(*results)

    return jax.shard_map(local_step, mesh=mesh, in_specs=(tile_spec,) * 8, out_specs=(tile_spec,) * 5, check_vma=False)
```
